256 devices in a mesh: fsdp: 128 (over z, x, y), dp: 2 (over core).
Axes of the slice: x: 4, y: 4, z: 8, core: 2. Of those that a mesh axis runs over, the one named last changes fastest.
Arguments:
- gradients: bfloat16 [2, 512, 256, 256], P('dp', 'fsdp'), may hold values from -6 to 6
- first_moment: float32 [768, 256, 256], P('fsdp'), may hold values from -4 to 4
- second_moment: float32 [768, 256, 256], P('fsdp'), may hold values from 0.05 to 2
- left_basis: float32 [768, 256, 256], P('fsdp'), may hold values from -1 to 1, as said below
- right_basis: float32 [768, 256, 256], P('fsdp'), may hold values from -1 to 1, as said below
- shard_starts: int32 [128], replicated, may hold values from 0 to 384, as said below
- block_owners: int32 [384], replicated, may hold values from 0 to 127, as said below
Outputs:
- direction: float32 [512, 256, 256], P('fsdp')
- first_new: float32 [768, 256, 256], P('fsdp')
- second_new: float32 [768, 256, 256], P('fsdp')
The draws below stay inside these ranges and needn't reach their ends.
Inputs may be any that keep to these rules, and one draw needn't show every extreme that they name: Starts never fall and shard_starts[0] = 0; a device holds at most 4 blocks, some device exactly 4 and some none. `block_owners`: never falls; a device owns at most 6 blocks, some device exactly 6 and some none; a block's owner differs from its holder by at most 2 fsdp indices, by exactly 2 for some block in each direction. `left_basis`: each matrix is orthogonal up to float32 rounding. `right_basis`: each matrix is orthogonal up to float32 rounding.
All inputs are finite; a program needn't handle non-finite values.
Results may differ from the reference program's by a relative error of at most 0.0014.
Values may be sent and summed in bfloat16 or wider, within the bound.
A program may use at most 64 MiB of HBM per device.

```python
import math
import jax
import jax.numpy as jnp
import numpy as np
from jax import lax

BS = 256
SLOTS = 4
OWN = 6
STEP = 10
NBLK = 384
N_FSDP = 128
N_DP = 2


holder_table = np.array([[4, 4, 2, 2], [4, 3, 3, 2], [4, 4, 3, 1], [4, 4, 4, 0], [4, 3, 4, 1], [4, 2, 2, 4]], dtype=np.int32)


owner_table = np.array([[6, 2, 2, 2], [6, 3, 2, 1], [6, 4, 1, 1], [6, 6, 0, 0], [6, 3, 3, 0], [6, 4, 2, 0], [6, 5, 1, 0], [6, 1, 2, 3]], dtype=np.int32)


edge_holder_table = np.array([[4, 2], [3, 3], [2, 4]], dtype=np.int32)


edge_owner_table = np.array([[3, 3], [4, 2], [2, 4], [6, 0], [0, 6]], dtype=np.int32)


def group_counts(key):
    inner = N_FSDP // 4 - 1
    middle = N_FSDP // 8 - 1
    base = jax.random.fold_in(key, 7)
    parts = jax.random.split(base, 8)
    hold_pick = jax.random.randint(parts[0], (inner,), 0, holder_table.shape[0])
    own_pick = jax.random.randint(parts[1], (inner,), 0, owner_table.shape[0])
    hold_rows = jnp.asarray(holder_table)[hold_pick]
    own_rows = jnp.asarray(owner_table)[own_pick]
    hold_keys = jax.random.split(parts[2], inner)
    own_keys = jax.random.split(parts[3], inner)
    hold_rows = jax.vmap(lambda kk, row: jax.random.permutation(kk, row))(hold_keys, hold_rows)
    own_rows = jax.vmap(lambda kk, row: jax.random.permutation(kk, row))(own_keys, own_rows)
    first_rank = jax.random.randint(parts[4], (), 0, inner - 1)
    first_group = first_rank + (first_rank >= middle).astype(jnp.int32)
    second_rank = (first_rank + 1 + jax.random.randint(parts[5], (), 0, inner - 2)) % (inner - 1)
    second_group = second_rank + (second_rank >= middle).astype(jnp.int32)
    group_ids = jnp.arange(inner)[:, None]
    hold_rows = jnp.where(group_ids == first_group, jnp.array([[4, 4, 4, 0]], jnp.int32), hold_rows)
    own_rows = jnp.where(group_ids == first_group, jnp.array([[0, 0, 6, 6]], jnp.int32), own_rows)
    hold_rows = jnp.where(group_ids == second_group, jnp.array([[0, 4, 4, 4]], jnp.int32), hold_rows)
    own_rows = jnp.where(group_ids == second_group, jnp.array([[6, 6, 0, 0]], jnp.int32), own_rows)
    hold_rows = jnp.where(group_ids == middle, jnp.array([[4, 4, 4, 0]], jnp.int32), hold_rows)
    own_rows = jnp.where(group_ids == middle, jnp.array([[0, 2, 6, 4]], jnp.int32), own_rows)
    edge_keys = jax.random.split(parts[6], 2)
    owner_keys = jax.random.split(parts[7], 2)
    edge_hold = [jnp.asarray(edge_holder_table)[jax.random.randint(edge_keys[side], (), 0, edge_holder_table.shape[0])] for side in range(2)]
    edge_own = [jnp.asarray(edge_owner_table)[jax.random.randint(owner_keys[side], (), 0, edge_owner_table.shape[0])] for side in range(2)]
    hold_counts = jnp.concatenate([edge_hold[0], hold_rows.reshape(-1), edge_hold[1]]).astype(jnp.int32)
    own_counts = jnp.concatenate([edge_own[0], own_rows.reshape(-1), edge_own[1]]).astype(jnp.int32)
    return (hold_counts, own_counts)


def draw_shard_starts(key, part):
    hold_counts, own_counts = group_counts(key)
    return (jnp.cumsum(hold_counts) - hold_counts).astype(jnp.int32)


def draw_block_owners(key, part):
    hold_counts, own_counts = group_counts(key)
    return jnp.repeat(jnp.arange(N_FSDP, dtype=jnp.int32), own_counts, total_repeat_length=NBLK).astype(jnp.int32)


def orthogonal(key, spread):
    random_part = jax.random.normal(key, (N_FSDP * OWN, BS, BS), jnp.float32) * (spread / BS ** 0.5)
    skew_part = random_part - jnp.swapaxes(random_part, 1, 2)
    identity = jnp.broadcast_to(jnp.eye(BS, dtype=jnp.float32), skew_part.shape)
    return jnp.linalg.solve(identity - skew_part, identity + skew_part)


def draw_left_basis(key, part):
    return orthogonal(jax.random.fold_in(key, 11), 0.8)


def draw_right_basis(key, part):
    return orthogonal(jax.random.fold_in(key, 13), 0.8)


def shard_levels(key, shape, cuts, smallest, high):
    def one(axis_at, blocks):
        heights = jax.random.uniform(jax.random.fold_in(jax.random.fold_in(key, 6), axis_at), (blocks,), jnp.float32, smallest / len(cuts), high / len(cuts))
        return jnp.repeat(jnp.exp(heights), shape[axis_at] // blocks).reshape((-1,) + (1,) * (len(shape) - axis_at - 1))

    level = one(*cuts[0])
    for cut in cuts[1:]:
        level = level * one(*cut)
    return level


def gaussian(own_key, dims, scale, reach, shards=(), kind=jnp.bfloat16):
    gain = shard_levels(own_key, dims, shards, -0.22, 0.18) if shards else 1.0
    result = jax.random.normal(own_key, dims, jnp.float32) * scale * gain
    return jnp.minimum(jnp.maximum(result, -reach), reach).astype(kind)


def setup_inputs(seed: int = 0) -> dict:
    streams_of = jax.random.split(jax.random.key(seed), 8)
    return {
        "gradients": gaussian(streams_of[0], (N_DP, N_FSDP * SLOTS, BS, BS), 1.0, 6.0, ((0, 2), (1, 128))),
        "first_moment": gaussian(streams_of[1], (N_FSDP * OWN, BS, BS), 0.5, 4.0, ((0, 128),), jnp.float32),
        "second_moment": jnp.clip(jnp.exp(math.log(2.0) - 3.6888794 * jax.random.uniform(streams_of[2], (N_FSDP * OWN, BS, BS), jnp.float32) ** shard_levels(streams_of[2], (N_FSDP * OWN, BS, BS), ((0, 128),), -0.2, 0.2)), 0.05, 2.0),
        "left_basis": draw_left_basis(jax.random.fold_in(streams_of[7], 71), 0),
        "right_basis": draw_right_basis(jax.random.fold_in(streams_of[7], 71), 0),
        "shard_starts": draw_shard_starts(jax.random.fold_in(streams_of[7], 71), 0),
        "block_owners": draw_block_owners(jax.random.fold_in(streams_of[7], 71), 0),
    }


beta_one = 0.9
beta_two = 0.95
epsilon = 1e-08

def soap_blocks(gradient, moment_one, moment_two, left_basis, right_basis):
    highest = lax.Precision.HIGHEST
    moment_new = beta_one * moment_one + (1.0 - beta_one) * gradient
    turned = jnp.einsum('jad,jde->jae', jnp.einsum('jba,jbd->jad', left_basis, gradient, precision=highest), right_basis, precision=highest)
    turned_moment = jnp.einsum('jad,jde->jae', jnp.einsum('jba,jbd->jad', left_basis, moment_new, precision=highest), right_basis, precision=highest)
    second_next = beta_two * moment_two + (1.0 - beta_two) * turned * turned
    bias_one = 1.0 - beta_one ** STEP
    bias_two = 1.0 - beta_two ** STEP
    scaled = turned_moment / bias_one / (jnp.sqrt(second_next / bias_two) + epsilon)
    update = jnp.einsum('jad,jed->jae', jnp.einsum('jab,jbd->jad', left_basis, scaled, precision=highest), right_basis, precision=highest)
    return (moment_new, second_next, update)

def reference(gradients, first_moment, second_moment, left_basis, right_basis, shard_starts, block_owners):
    block_ids = jnp.arange(NBLK, dtype=jnp.int32)
    holder = (jnp.searchsorted(shard_starts, block_ids, side='right') - 1).astype(jnp.int32)
    hold_row = (holder * SLOTS + block_ids - shard_starts[holder]).astype(jnp.int32)
    first_owned = jnp.searchsorted(block_owners, block_owners, side='left').astype(jnp.int32)
    own_row = (block_owners * OWN + block_ids - first_owned).astype(jnp.int32)
    summed = lax.optimization_barrier(jnp.sum(gradients.astype(jnp.float32), axis=0)).astype(jnp.bfloat16)
    gradient = summed[hold_row].astype(jnp.float32)
    moment_new, second_next, update = soap_blocks(gradient, first_moment[own_row], second_moment[own_row], left_basis[own_row], right_basis[own_row])
    blank_hold = jnp.zeros((N_FSDP * SLOTS, BS, BS), jnp.float32)
    blank_own = jnp.zeros((N_FSDP * OWN, BS, BS), jnp.float32)
    direction = blank_hold.at[hold_row].set(update)
    first_new = blank_own.at[own_row].set(moment_new)
    second_new = blank_own.at[own_row].set(second_next)
    return (direction, first_new, second_new)
```

```python
import functools

import jax
import jax.numpy as jnp
from jax import lax
from jax.experimental import pallas as pl
from jax.experimental.pallas import tpu as pltpu
from jax.sharding import PartitionSpec as P

STEP = 10
BETA_ONE = 0.9
BETA_TWO = 0.95
EPSILON = 1e-08
TOP = 32766.0
MESH = pl.DeviceIdType.MESH
F32 = jnp.float32
BF16 = jnp.bfloat16
I16 = jnp.int16


def neighbours(devices):
    me = lax.axis_index("fsdp")
    core = lax.axis_index("dp")
    right = {"fsdp": lax.rem(me + 1, devices)}
    left = {"fsdp": lax.rem(me + devices - 1, devices)}
    twin = {"dp": 1 - core}
    return core, right, left, twin


def greet(peers):
    barrier = pltpu.get_barrier_semaphore()
    for peer in peers:
        pl.semaphore_signal(barrier, inc=1, device_id=peer, device_id_type=MESH)
    pl.semaphore_wait(barrier, len(peers))


def push(src, dst, send_sem, recv_sem, peer):
    return pltpu.make_async_remote_copy(
        src_ref=src,
        dst_ref=dst,
        send_sem=send_sem,
        recv_sem=recv_sem,
        device_id=peer,
        device_id_type=MESH,
    )


def gather_kernel(devices, grad, out, mine, theirs, other, load_sem, twin_sem, ring_send, ring_recv, hand_send, hand_recv):
    core, right, left, twin = neighbours(devices)
    slots = grad.shape[1]
    half = grad.shape[2] // 2
    rows = pl.ds(pl.multiple_of(core * half, half), half)
    other_rows = pl.ds(pl.multiple_of((1 - core) * half, half), half)
    load_other = pltpu.make_async_copy(grad.at[0, :, other_rows], other, load_sem.at[0])
    load_mine = pltpu.make_async_copy(grad.at[0, :, rows], mine, load_sem.at[1])
    load_other.start()
    load_mine.start()
    greet((twin, right, left))
    load_other.wait()
    swap = push(other, theirs, twin_sem.at[0], twin_sem.at[1], twin)
    swap.start()
    load_mine.wait()
    swap.wait_recv()
    for s in range(slots):
        out[2, s, rows] = (mine[s].astype(F32) + theirs[s].astype(F32)).astype(BF16)

    def part(k, s):
        return out.at[k, s, rows]

    def ring(src_k, dst_k, s, peer):
        return push(part(src_k, s), part(dst_k, s), ring_send.at[dst_k, s], ring_recv.at[dst_k, s], peer)

    def hand(k, s):
        return push(part(k, s), part(k, s), hand_send.at[k, s], hand_recv.at[k, s], twin)

    copies = []
    for s in range(slots):
        for copy in (ring(2, 1, s, right), ring(2, 3, s, left), hand(2, s)):
            copy.start()
            copies.append(copy)
    relays = []
    for s in range(slots):
        for near, far, peer in ((1, 0, right), (3, 4, left)):
            ring(2, near, s, peer).wait_recv()
            relay = ring(near, far, s, peer)
            relay.start()
            pass_on = hand(near, s)
            pass_on.start()
            copies += [relay, pass_on]
            relays.append((far, s, relay))
    for far, s, relay in relays:
        relay.wait_recv()
        pass_on = hand(far, s)
        pass_on.start()
        copies.append(pass_on)
    swap.wait_send()
    for copy in copies:
        copy.wait_send()
    for k in range(5):
        for s in range(slots):
            hand(k, s).wait_recv()


def split(x):
    high = x.astype(BF16)
    return high, (x - high.astype(F32)).astype(BF16)


def dot(a, b, dims):
    return lax.dot_general(a, b, (dims, ((), ())), preferred_element_type=F32)


def dot_three(a, b, dims):
    return dot(a[0], b[0], dims) + (dot(a[0], b[1], dims) + dot(a[1], b[0], dims))


NN = ((1,), (0,))
TN = ((0,), (0,))
NT = ((1,), (1,))


def step_kernel(devices, starts, owners, gathered, moment, second, left, right, first_out, second_out, codes, scales, table):
    j = pl.program_id(0)
    me = lax.axis_index("fsdp")
    core = lax.axis_index("dp")
    blocks = owners.shape[0]
    slots = gathered.shape[0] // 5
    half = left.shape[1] // 2

    def start_of(device):
        value = starts[jnp.clip(device, 0, devices - 1)]
        return jnp.where(device < 0, -1, jnp.where(device >= devices, blocks, value))

    @pl.when(j == 0)
    def _():
        codes[...] = jnp.zeros(codes.shape, codes.dtype)
        scales[...] = jnp.zeros(scales.shape, scales.dtype)
        base = jnp.maximum(start_of(me - 2), 0)
        below = jnp.int32(0)
        for k in range(5 * slots):
            at = base + k
            owner = owners[jnp.minimum(at, blocks - 1)]
            below += jnp.where((at < blocks) & (owner < me), 1, 0)
        table[0] = base + below

    block = table[0] + j
    safe = jnp.minimum(block, blocks - 1)
    live = (block < blocks) & (owners[safe] == me)
    place = jnp.int32(0)
    for delta in (-1, 0, 1, 2):
        place += jnp.where(start_of(me + delta) <= block, 1, 0)
    slot = block - starts[jnp.clip(me + place - 2, 0, devices - 1)]
    index = jnp.where(live, place * slots + slot, 0)

    gradient = gathered[index]
    l_two, r_two = split(left[0]), split(right[0])
    moment_new = BETA_ONE * moment[0] + (1.0 - BETA_ONE) * gradient.astype(F32)
    first_out[0] = jnp.where(live, moment_new, 0.0)
    half_turned = dot(l_two[0], gradient, TN) + dot(l_two[1], gradient, TN)
    turned = dot_three(split(half_turned), r_two, NN)
    turned_moment = dot_three(split(dot_three(l_two, split(moment_new), TN)), r_two, NN)
    second_next = BETA_TWO * second[0] + (1.0 - BETA_TWO) * turned * turned
    second_out[0] = jnp.where(live, second_next, 0.0)
    bias_one = 1.0 - BETA_ONE**STEP
    bias_two = 1.0 - BETA_TWO**STEP
    scaled = turned_moment / bias_one / (jnp.sqrt(second_next / bias_two) + EPSILON)
    l_half = split(left[0, pl.ds(pl.multiple_of(core * half, half), half)])
    update = dot_three(split(dot_three(l_half, split(scaled), NN)), r_two, NT)
    largest = jnp.maximum(jnp.max(jnp.abs(update), axis=0, keepdims=True), 1e-30)
    code = jnp.round(update * (TOP / largest)).astype(jnp.int32)

    @pl.when(live)
    def _():
        codes[index] = code.astype(I16)
        scales[index, 0:1] = largest * (1.0 / TOP)


def return_kernel(
    devices, codes, scales, out, out_scales, far_in, far_scales, merged, merged_scales, far_send, far_recv, ring_send, ring_recv, hand_send, hand_recv,
    sf_send, sf_recv, sr_send, sr_recv, sh_send, sh_recv
):
    core, right, left, twin = neighbours(devices)
    slots = codes.shape[1]
    half = codes.shape[2]
    rows = pl.ds(pl.multiple_of(core * half, half), half)
    greet((twin, right, left))
    copies = []
    far = []
    for k, side, peer in ((4, 0, right), (0, 1, left)):
        copy = push(scales.at[k], far_scales.at[side], sf_send.at[side], sf_recv.at[side], peer)
        copy.start()
        far.append(copy)
    far_copies = {}
    for s in range(slots):
        for k, side, peer in ((4, 0, right), (0, 1, left)):
            copy = push(codes.at[k, s], far_in.at[side, s], far_send.at[side, s], far_recv.at[side, s], peer)
            copy.start()
            far_copies[side, s] = copy

    def hand(k, s):
        return push(out.at[k, s, rows], out.at[k, s, rows], hand_send.at[k, s], hand_recv.at[k, s], twin)

    def hand_scales(k):
        return push(out_scales.at[k, core], out_scales.at[k, core], sh_send.at[k], sh_recv.at[k], twin)

    out_scales[2, core] = scales[2]
    for s in range(slots):
        out[2, s, rows] = codes[2, s]
    copy = hand_scales(2)
    copy.start()
    copies.append(copy)
    for s in range(slots):
        copy = hand(2, s)
        copy.start()
        copies.append(copy)

    near_scales = []
    for k, side, peer in ((3, 0, right), (1, 1, left)):
        far[side].wait_recv()
        merged_scales[side] = scales[k] + far_scales[side]
        copy = push(merged_scales.at[side], out_scales.at[side, core], sr_send.at[side], sr_recv.at[side], peer)
        copy.start()
        near_scales.append(copy)
    near = []
    for s in range(slots):
        for k, side, peer in ((3, 0, right), (1, 1, left)):
            far_copies[side, s].wait_recv()
            merged[side, s] = codes[k, s] + far_in[side, s]
            copy = push(merged.at[side, s], out.at[side, s, rows], ring_send.at[side, s], ring_recv.at[side, s], peer)
            copy.start()
            near.append((side, s, copy))
    for side in range(2):
        near_scales[side].wait_recv()
        copy = hand_scales(side)
        copy.start()
        copies.append(copy)
    for side, s, ring in near:
        ring.wait_recv()
        copy = hand(side, s)
        copy.start()
        copies.append(copy)
    for copy in copies + far + near_scales + list(far_copies.values()) + [ring for _, _, ring in near]:
        copy.wait_send()
    for k in range(3):
        hand_scales(k).wait_recv()
        for s in range(slots):
            hand(k, s).wait_recv()


def decode_kernel(codes, scales, out):
    s = pl.program_id(0)
    half = out.shape[1] // 2
    for core in range(2):
        rows = pl.ds(core * half, half)
        total = 0.0
        for k in range(3):
            total += codes[k, s, rows].astype(jnp.int32).astype(F32) * scales[k, core, pl.ds(s, 1)]
        out[0, rows] = total


def body(gradients, first_moment, second_moment, left_basis, right_basis, shard_starts, block_owners):
    devices = lax.axis_size("fsdp")
    slots = gradients.shape[1]
    owned, width = first_moment.shape[0], first_moment.shape[1]
    half = width // 2
    any_space = pl.BlockSpec(memory_space=pl.ANY)
    in_vmem = pl.BlockSpec(memory_space=pltpu.VMEM)
    dma = pltpu.SemaphoreType.DMA
    gathered = pl.pallas_call(
        functools.partial(gather_kernel, devices),
        out_shape=pltpu.VMEM((5, slots, width, width), BF16),
        in_specs=[any_space],
        out_specs=in_vmem,
        scratch_shapes=[pltpu.VMEM((slots, half, width), BF16)] * 3
        + [dma((2,)), dma((2,)), dma((5, slots)), dma((5, slots)), dma((5, slots)), dma((5, slots))],
        compiler_params=pltpu.CompilerParams(collective_id=0, has_side_effects=True),
        name="gather",
    )(gradients)

    block = pl.BlockSpec((1, width, width), lambda j, *_: (j, 0, 0))
    first_new, second_new, codes, scales = pl.pallas_call(
        functools.partial(step_kernel, devices),
        grid_spec=pltpu.PrefetchScalarGridSpec(
            num_scalar_prefetch=2,
            grid=(owned,),
            in_specs=[in_vmem, block, block, block, block],
            out_specs=[block, block, in_vmem, in_vmem],
            scratch_shapes=[pltpu.SMEM((1,), jnp.int32)],
        ),
        out_shape=[
            jax.ShapeDtypeStruct(first_moment.shape, F32),
            jax.ShapeDtypeStruct(first_moment.shape, F32),
            pltpu.VMEM((5 * slots, half, width), I16),
            pltpu.VMEM((5 * slots, 1, width), F32),
        ],
        name="step",
    )(shard_starts, block_owners, gathered.reshape(5 * slots, width, width), first_moment, second_moment, left_basis, right_basis)

    out, out_scales = pl.pallas_call(
        functools.partial(return_kernel, devices),
        out_shape=[
            pltpu.VMEM((3, slots, width, width), I16),
            pltpu.VMEM((3, 2, slots, width), F32),
        ],
        in_specs=[in_vmem, in_vmem],
        out_specs=[in_vmem, in_vmem],
        scratch_shapes=[
            pltpu.VMEM((2, slots, half, width), I16),
            pltpu.VMEM((2, slots, width), F32),
            pltpu.VMEM((2, slots, half, width), I16),
            pltpu.VMEM((2, slots, width), F32),
            dma((2, slots)), dma((2, slots)), dma((2, slots)), dma((2, slots)), dma((3, slots)), dma((3, slots)),
            dma((2,)), dma((2,)), dma((2,)), dma((2,)), dma((3,)), dma((3,)),
        ],
        compiler_params=pltpu.CompilerParams(collective_id=1, has_side_effects=True),
        name="bring",
    )(codes.reshape(5, slots, half, width), scales.reshape(5, slots, width))

    direction = pl.pallas_call(
        decode_kernel,
        grid=(slots,),
        out_shape=jax.ShapeDtypeStruct((slots, width, width), F32),
        in_specs=[in_vmem, in_vmem],
        out_specs=pl.BlockSpec((1, width, width), lambda s: (s, 0, 0)),
        name="decode",
    )(out, out_scales)
    return direction, first_new, second_new


def solution(mesh):
    in_specs = (
        P("dp", "fsdp", None, None),
        P("fsdp", None, None),
        P("fsdp", None, None),
        P("fsdp", None, None),
        P("fsdp", None, None),
        P(),
        P(),
    )
    out_specs = (P("fsdp", None, None), P("fsdp", None, None), P("fsdp", None, None))
    return jax.shard_map(body, mesh=mesh, in_specs=in_specs, out_specs=out_specs, check_vma=False)
```

```python
import functools

import jax
import jax.numpy as jnp
from jax import lax
from jax.experimental import pallas as pl
from jax.experimental.pallas import tpu as pltpu
from jax.sharding import PartitionSpec as P

STEP = 10
BETA_ONE = 0.9
BETA_TWO = 0.95
EPSILON = 1e-08
TOP = 32766.0
ROOM = 24 * 2**20
MESH = pl.DeviceIdType.MESH
F32 = jnp.float32
BF16 = jnp.bfloat16
I16 = jnp.int16


def neighbours(devices):
    me = lax.axis_index("fsdp")
    core = lax.axis_index("dp")
    right = {"fsdp": jnp.minimum(me + 1, devices - 1)}
    left = {"fsdp": jnp.maximum(me - 1, 0)}
    twin = {"dp": 1 - core}
    return me, core, right, left, twin


def greet(me, devices, right, left, twin):
    barrier = pltpu.get_barrier_semaphore()

    def signal(peer):
        pl.semaphore_signal(barrier, inc=1, device_id=peer, device_id_type=MESH)

    signal(twin)
    pl.when(me < devices - 1)(lambda: signal(right))
    pl.when(me > 0)(lambda: signal(left))
    at_end = (me == 0) | (me == devices - 1)
    pl.when(at_end)(lambda: pl.semaphore_wait(barrier, 2))
    pl.when(~at_end)(lambda: pl.semaphore_wait(barrier, 3))


def push(src, dst, send_sem, recv_sem, peer):
    return pltpu.make_async_remote_copy(
        src_ref=src,
        dst_ref=dst,
        send_sem=send_sem,
        recv_sem=recv_sem,
        device_id=peer,
        device_id_type=MESH,
    )


def gather_kernel(devices, grad, out, mine, theirs, other, load_sem, twin_sem, ring_send, ring_recv, hand_send, hand_recv):
    me, core, right, left, twin = neighbours(devices)
    slots = grad.shape[1]
    half = grad.shape[2] // 2
    rows = pl.ds(pl.multiple_of(core * half, half), half)
    other_rows = pl.ds(pl.multiple_of((1 - core) * half, half), half)
    load_other = pltpu.make_async_copy(grad.at[0, :, other_rows], other, load_sem.at[0])
    load_mine = pltpu.make_async_copy(grad.at[0, :, rows], mine, load_sem.at[1])
    load_other.start()
    load_mine.start()
    greet(me, devices, right, left, twin)
    load_other.wait()
    swap = push(other, theirs, twin_sem.at[0], twin_sem.at[1], twin)
    swap.start()
    load_mine.wait()
    swap.wait_recv()
    for s in range(slots):
        out[2, s, rows] = (mine[s].astype(F32) + theirs[s].astype(F32)).astype(BF16)

    def part(k, s):
        return out.at[k, s, rows]

    def ring(src_k, dst_k, s, peer):
        return push(part(src_k, s), part(dst_k, s), ring_send.at[dst_k, s], ring_recv.at[dst_k, s], peer)

    def hand(k, s):
        return push(part(k, s), part(k, s), hand_send.at[k, s], hand_recv.at[k, s], twin)

    sides = (
        dict(near=1, far=0, peer=right, has=me >= 1, gives=me >= 2, sends=me < devices - 1),
        dict(near=3, far=4, peer=left, has=me < devices - 1, gives=me < devices - 2, sends=me >= 1),
    )

    for side in sides:

        @pl.when(side["sends"])
        def _():
            for s in range(slots):
                ring(2, side["near"], s, side["peer"]).start()

    for s in range(slots):
        hand(2, s).start()
    for s in range(slots):
        for side in sides:

            @pl.when(side["has"])
            def _():
                ring(2, side["near"], s, side["peer"]).wait_recv()

            @pl.when(side["has"] & side["sends"])
            def _():
                ring(side["near"], side["far"], s, side["peer"]).start()

            @pl.when(side["has"])
            def _():
                hand(side["near"], s).start()

    for s in range(slots):
        for side in sides:

            @pl.when(side["gives"])
            def _():
                ring(side["near"], side["far"], s, side["peer"]).wait_recv()
                hand(side["far"], s).start()

    swap.wait_send()
    for s in range(slots):
        hand(2, s).wait_send()
        hand(2, s).wait_recv()
    for side in sides:

        @pl.when(side["sends"])
        def _():
            for s in range(slots):
                ring(2, side["near"], s, side["peer"]).wait_send()

        @pl.when(side["has"] & side["sends"])
        def _():
            for s in range(slots):
                ring(side["near"], side["far"], s, side["peer"]).wait_send()

        @pl.when(side["has"])
        def _():
            for s in range(slots):
                hand(side["near"], s).wait_send()
                hand(side["near"], s).wait_recv()

        @pl.when(side["gives"])
        def _():
            for s in range(slots):
                hand(side["far"], s).wait_send()
                hand(side["far"], s).wait_recv()


def split(x):
    high = x.astype(BF16)
    return high, (x - high.astype(F32)).astype(BF16)


def dot(a, b, dims):
    return lax.dot_general(a, b, (dims, ((), ())), preferred_element_type=F32)


def dot_three(a, b, dims):
    return dot(a[0], b[0], dims) + (dot(a[0], b[1], dims) + dot(a[1], b[0], dims))


NN = ((1,), (0,))
TN = ((0,), (0,))
NT = ((1,), (1,))


GROUP = 2


def step_kernel(devices, starts, owners, gathered, moment, second, left, right, first_out, second_out, codes, scales, table):
    step = pl.program_id(0)
    me = lax.axis_index("fsdp")
    core = lax.axis_index("dp")
    blocks = owners.shape[0]
    slots = gathered.shape[1]
    half = left.shape[1] // 2

    def start_of(device):
        value = starts[jnp.clip(device, 0, devices - 1)]
        return jnp.where(device < 0, -1, jnp.where(device >= devices, blocks, value))

    @pl.when(step == 0)
    def _():
        codes[...] = jnp.zeros(codes.shape, codes.dtype)
        scales[...] = jnp.zeros(scales.shape, scales.dtype)
        base = jnp.maximum(start_of(me - 2), 0)
        below = jnp.int32(0)
        for k in range(5 * slots):
            at = base + k
            owner = owners[jnp.minimum(at, blocks - 1)]
            below += jnp.where((at < blocks) & (owner < me), 1, 0)
        table[0] = base + below

    def solve(at):
        block = table[0] + step * GROUP + at
        safe = jnp.minimum(block, blocks - 1)
        live = (block < blocks) & (owners[safe] == me)
        place = jnp.int32(0)
        for delta in (-1, 0, 1, 2):
            place += jnp.where(start_of(me + delta) <= block, 1, 0)
        slot = block - starts[jnp.clip(me + place - 2, 0, devices - 1)]
        place = jnp.where(live, place, 0)
        slot = jnp.where(live, slot, 0)

        gradient = gathered[place, slot]
        l_two, r_two = split(left[at]), split(right[at])
        moment_new = BETA_ONE * moment[at] + (1.0 - BETA_ONE) * gradient.astype(F32)
        first_out[at] = jnp.where(live, moment_new, 0.0)
        half_turned = dot(l_two[0], gradient, TN) + dot(l_two[1], gradient, TN)
        turned = dot_three(split(half_turned), r_two, NN)
        turned_moment = dot_three(split(dot_three(l_two, split(moment_new), TN)), r_two, NN)
        second_next = BETA_TWO * second[at] + (1.0 - BETA_TWO) * turned * turned
        second_out[at] = jnp.where(live, second_next, 0.0)
        bias_one = 1.0 - BETA_ONE**STEP
        bias_two = 1.0 - BETA_TWO**STEP
        scaled = turned_moment * (1.0 / bias_one) / (jnp.sqrt(second_next * (1.0 / bias_two)) + EPSILON)
        l_half = split(left[at, pl.ds(pl.multiple_of(core * half, half), half)])
        update = dot_three(split(dot_three(l_half, split(scaled), NN)), r_two, NT)
        largest = jnp.maximum(jnp.max(jnp.abs(update), axis=0, keepdims=True), 1e-30)
        code = jnp.round(update * (TOP / largest)).astype(jnp.int32).astype(I16)
        return live, place, slot, code, largest * (1.0 / TOP)

    for live, place, slot, code, scale in [solve(at) for at in range(GROUP)]:

        @pl.when(live)
        def _():
            codes[place, slot] = code
            scales[place, pl.ds(slot, 1)] = scale


def return_kernel(
    devices, codes, scales, out, out_scales, far_in, far_scales, merged, merged_scales, far_send, far_recv, ring_send, ring_recv, hand_send, hand_recv,
    sf_send, sf_recv, sr_send, sr_recv, sh_send, sh_recv
):
    me, core, right, left, twin = neighbours(devices)
    slots = codes.shape[1]
    half = codes.shape[2]
    rows = pl.ds(pl.multiple_of(core * half, half), half)
    greet(me, devices, right, left, twin)

    def hand(k, s):
        return push(out.at[k, s, rows], out.at[k, s, rows], hand_send.at[k, s], hand_recv.at[k, s], twin)

    def hand_scales(k):
        return push(out_scales.at[k, core], out_scales.at[k, core], sh_send.at[k], sh_recv.at[k], twin)

    def far(side, s):
        return push(codes.at[side["far"], s], far_in.at[side["at"], s], far_send.at[side["at"], s], far_recv.at[side["at"], s], side["peer"])

    def far_scale(side):
        return push(scales.at[side["far"]], far_scales.at[side["at"]], sf_send.at[side["at"]], sf_recv.at[side["at"]], side["peer"])

    def ring(side, s):
        return push(
            merged.at[side["at"], s], out.at[side["at"], s, rows], ring_send.at[side["at"], s], ring_recv.at[side["at"], s], side["peer"]
        )

    def ring_scale(side):
        return push(merged_scales.at[side["at"]], out_scales.at[side["at"], core], sr_send.at[side["at"]], sr_recv.at[side["at"]], side["peer"])

    sides = (
        dict(at=0, far=4, near=3, peer=right, has=me >= 1, sends=me < devices - 1),
        dict(at=1, far=0, near=1, peer=left, has=me < devices - 1, sends=me >= 1),
    )
    for side in sides:

        @pl.when(side["sends"])
        def _():
            far_scale(side).start()
            for s in range(slots):
                far(side, s).start()

        @pl.when(~side["has"])
        def _():
            far_in[side["at"]] = jnp.zeros(far_in.shape[1:], I16)
            far_scales[side["at"]] = jnp.zeros(far_scales.shape[1:], F32)
            out[side["at"]] = jnp.zeros(out.shape[1:], I16)
            out_scales[side["at"]] = jnp.zeros(out_scales.shape[1:], F32)

    out_scales[2, core] = scales[2]
    for s in range(slots):
        out[2, s, rows] = codes[2, s]
    hand_scales(2).start()
    for s in range(slots):
        hand(2, s).start()

    for side in sides:

        @pl.when(side["has"])
        def _():
            far_scale(side).wait_recv()

        merged_scales[side["at"]] = scales[side["near"]] + far_scales[side["at"]]

        @pl.when(side["sends"])
        def _():
            ring_scale(side).start()

    for s in range(slots):
        for side in sides:

            @pl.when(side["has"])
            def _():
                far(side, s).wait_recv()

            merged[side["at"], s] = codes[side["near"], s] + far_in[side["at"], s]

            @pl.when(side["sends"])
            def _():
                ring(side, s).start()

    for side in sides:

        @pl.when(side["has"])
        def _():
            ring_scale(side).wait_recv()
            hand_scales(side["at"]).start()

    for s in range(slots):
        for side in sides:

            @pl.when(side["has"])
            def _():
                ring(side, s).wait_recv()
                hand(side["at"], s).start()

    hand_scales(2).wait_send()
    hand_scales(2).wait_recv()
    for s in range(slots):
        hand(2, s).wait_send()
        hand(2, s).wait_recv()
    for side in sides:

        @pl.when(side["sends"])
        def _():
            far_scale(side).wait_send()
            ring_scale(side).wait_send()
            for s in range(slots):
                far(side, s).wait_send()
                ring(side, s).wait_send()

        @pl.when(side["has"])
        def _():
            hand_scales(side["at"]).wait_send()
            hand_scales(side["at"]).wait_recv()
            for s in range(slots):
                hand(side["at"], s).wait_send()
                hand(side["at"], s).wait_recv()


def decode_kernel(codes, scales, out):
    s = pl.program_id(0)
    half = out.shape[1] // 2
    for core in range(2):
        rows = pl.ds(core * half, half)
        total = 0.0
        for k in range(3):
            total += codes[k, s, rows].astype(jnp.int32).astype(F32) * scales[k, core, pl.ds(s, 1)]
        out[0, rows] = total


def body(gradients, first_moment, second_moment, left_basis, right_basis, shard_starts, block_owners):
    devices = lax.axis_size("fsdp")
    slots = gradients.shape[1]
    owned, width = first_moment.shape[0], first_moment.shape[1]
    half = width // 2
    any_space = pl.BlockSpec(memory_space=pl.ANY)
    in_vmem = pl.BlockSpec(memory_space=pltpu.VMEM)
    dma = pltpu.SemaphoreType.DMA
    stay = functools.partial(pltpu.with_memory_space_constraint, memory_space=pltpu.HBM)
    gathered = pl.pallas_call(
        functools.partial(gather_kernel, devices),
        out_shape=pltpu.VMEM((5, slots, width, width), BF16),
        in_specs=[any_space],
        out_specs=in_vmem,
        scratch_shapes=[pltpu.VMEM((slots, half, width), BF16)] * 3
        + [dma((2,)), dma((2,)), dma((5, slots)), dma((5, slots)), dma((5, slots)), dma((5, slots))],
        compiler_params=pltpu.CompilerParams(collective_id=0, has_side_effects=True, vmem_limit_bytes=ROOM),
        name="gather",
    )(stay(gradients))

    keep = functools.partial(pltpu.with_memory_space_constraint, memory_space=pltpu.VMEM)
    block = pl.BlockSpec((GROUP, width, width), lambda j, *_: (j, 0, 0))
    first_new, second_new, codes, scales = pl.pallas_call(
        functools.partial(step_kernel, devices),
        grid_spec=pltpu.PrefetchScalarGridSpec(
            num_scalar_prefetch=2,
            grid=(owned // GROUP,),
            in_specs=[in_vmem, block, block, block, block],
            out_specs=[block, block, in_vmem, in_vmem],
            scratch_shapes=[pltpu.SMEM((1,), jnp.int32)],
        ),
        out_shape=[
            jax.ShapeDtypeStruct(first_moment.shape, F32),
            jax.ShapeDtypeStruct(first_moment.shape, F32),
            pltpu.VMEM((5, slots, half, width), I16),
            pltpu.VMEM((5, slots, width), F32),
        ],
        compiler_params=pltpu.CompilerParams(vmem_limit_bytes=ROOM),
        name="step",
    )(shard_starts, block_owners, keep(gathered), *map(stay, (first_moment, second_moment, left_basis, right_basis)))

    out, out_scales = pl.pallas_call(
        functools.partial(return_kernel, devices),
        out_shape=[
            pltpu.VMEM((3, slots, width, width), I16),
            pltpu.VMEM((3, 2, slots, width), F32),
        ],
        in_specs=[in_vmem, in_vmem],
        out_specs=[in_vmem, in_vmem],
        scratch_shapes=[
            pltpu.VMEM((2, slots, half, width), I16),
            pltpu.VMEM((2, slots, width), F32),
            pltpu.VMEM((2, slots, half, width), I16),
            pltpu.VMEM((2, slots, width), F32),
            dma((2, slots)), dma((2, slots)), dma((2, slots)), dma((2, slots)), dma((3, slots)), dma((3, slots)),
            dma((2,)), dma((2,)), dma((2,)), dma((2,)), dma((3,)), dma((3,)),
        ],
        compiler_params=pltpu.CompilerParams(collective_id=1, has_side_effects=True, vmem_limit_bytes=ROOM),
        name="bring",
    )(keep(codes), keep(scales))

    direction = pl.pallas_call(
        decode_kernel,
        grid=(slots,),
        out_shape=jax.ShapeDtypeStruct((slots, width, width), F32),
        in_specs=[in_vmem, in_vmem],
        out_specs=pl.BlockSpec((1, width, width), lambda s: (s, 0, 0)),
        compiler_params=pltpu.CompilerParams(vmem_limit_bytes=ROOM),
        name="decode",
    )(keep(out), keep(out_scales))
    return direction, first_new, second_new


def solution(mesh):
    in_specs = (
        P("dp", "fsdp", None, None),
        P("fsdp", None, None),
        P("fsdp", None, None),
        P("fsdp", None, None),
        P("fsdp", None, None),
        P(),
        P(),
    )
    out_specs = (P("fsdp", None, None), P("fsdp", None, None), P("fsdp", None, None))
    return jax.shard_map(body, mesh=mesh, in_specs=in_specs, out_specs=out_specs, check_vma=False)
```

```python
import functools

import jax
import jax.numpy as jnp
from jax import lax
from jax.experimental import pallas as pl
from jax.experimental.pallas import tpu as pltpu
from jax.sharding import PartitionSpec as P

STEP = 10
BETA_ONE = 0.9
BETA_TWO = 0.95
EPSILON = 1e-08
TOP = 32766.0
ROOM = 40 * 2**20
MESH = pl.DeviceIdType.MESH
F32 = jnp.float32
BF16 = jnp.bfloat16
I16 = jnp.int16


def neighbours(devices):
    me = lax.axis_index("fsdp")
    core = lax.axis_index("dp")
    right = {"fsdp": jnp.minimum(me + 1, devices - 1)}
    left = {"fsdp": jnp.maximum(me - 1, 0)}
    twin = {"dp": 1 - core}
    return me, core, right, left, twin


def greet(me, devices, right, left, twin):
    barrier = pltpu.get_barrier_semaphore()

    def signal(peer):
        pl.semaphore_signal(barrier, inc=1, device_id=peer, device_id_type=MESH)

    signal(twin)
    pl.when(me < devices - 1)(lambda: signal(right))
    pl.when(me > 0)(lambda: signal(left))
    at_end = (me == 0) | (me == devices - 1)
    pl.when(at_end)(lambda: pl.semaphore_wait(barrier, 2))
    pl.when(~at_end)(lambda: pl.semaphore_wait(barrier, 3))


def push(src, dst, send_sem, recv_sem, peer):
    return pltpu.make_async_remote_copy(
        src_ref=src,
        dst_ref=dst,
        send_sem=send_sem,
        recv_sem=recv_sem,
        device_id=peer,
        device_id_type=MESH,
    )


def split(x):
    high = x.astype(BF16)
    return high, (x - high.astype(F32)).astype(BF16)


def dot(a, b, dims):
    return lax.dot_general(a, b, (dims, ((), ())), preferred_element_type=F32)


def dot_three(a, b, dims):
    return dot(a[0], b[0], dims) + (dot(a[0], b[1], dims) + dot(a[1], b[0], dims))


NN = ((1,), (0,))
NT = ((1,), (1,))
GROUP = 2


def soap_kernel(
    devices, starts_in, owners_in, grad, moment_in, second_in, left_in, right_in, first_out, second_out, out, out_scales,
    starts, owners, table, mine, theirs, other, gathered, moment, second, left, right, lt_high, lt_low, lh_high, lh_low, r_high, r_low, base,
    update, update_scales, codes, scales, far_in, far_scales, merged, merged_scales,
    load_sem, twin_sem, ring_send, ring_recv, hand_send, hand_recv, back_send, back_recv, near_send, near_recv, give_send, give_recv,
    sf_send, sf_recv, sr_send, sr_recv, sh_send, sh_recv
):
    me, core, right_peer, left_peer, twin = neighbours(devices)
    slots = grad.shape[1]
    half = grad.shape[2] // 2
    owned = moment.shape[0]
    blocks = owners.shape[0]
    rows = pl.ds(pl.multiple_of(core * half, half), half)
    other_rows = pl.ds(pl.multiple_of((1 - core) * half, half), half)

    loads = [
        pltpu.make_async_copy(src, dst, load_sem.at[at])
        for at, (src, dst) in enumerate(
            (
                (grad.at[0, :, other_rows], other),
                (grad.at[0, :, rows], mine),
                (starts_in, starts),
                (owners_in, owners),
                (left_in, left),
                (moment_in, moment),
                (right_in, right),
                (second_in, second),
            )
        )
    ]
    for load in loads:
        load.start()
    greet(me, devices, right_peer, left_peer, twin)

    loads[0].wait()
    swap = push(other, theirs, twin_sem.at[0], twin_sem.at[1], twin)
    swap.start()
    loads[1].wait()
    swap.wait_recv()
    for s in range(slots):
        gathered[2, s, rows] = (mine[s].astype(F32) + theirs[s].astype(F32)).astype(BF16)

    def part(k, s):
        return gathered.at[k, s, rows]

    def ring(src_k, dst_k, s, peer):
        return push(part(src_k, s), part(dst_k, s), ring_send.at[dst_k, s], ring_recv.at[dst_k, s], peer)

    def hand(k, s):
        return push(part(k, s), part(k, s), hand_send.at[k, s], hand_recv.at[k, s], twin)

    sides = (
        dict(at=0, near=1, far=0, peer=right_peer, has=me >= 1, gives=me >= 2, sends=me < devices - 1, to_far=4, to_near=3),
        dict(at=1, near=3, far=4, peer=left_peer, has=me < devices - 1, gives=me < devices - 2, sends=me >= 1, to_far=0, to_near=1),
    )
    for side in sides:

        @pl.when(side["sends"])
        def _():
            for s in range(slots):
                ring(2, side["near"], s, side["peer"]).start()

        @pl.when(~side["has"])
        def _():
            gathered[side["near"]] = jnp.zeros(gathered.shape[1:], BF16)
            far_in[side["at"]] = jnp.zeros(far_in.shape[1:], I16)
            far_scales[side["at"]] = jnp.zeros(far_scales.shape[1:], F32)
            out[side["at"]] = jnp.zeros(out.shape[1:], I16)
            out_scales[side["at"]] = jnp.zeros(out_scales.shape[1:], F32)

        @pl.when(~side["gives"])
        def _():
            gathered[side["far"]] = jnp.zeros(gathered.shape[1:], BF16)

    for s in range(slots):
        hand(2, s).start()

    loads[2].wait()
    loads[3].wait()

    def start_of(device):
        value = starts[jnp.clip(device, 0, devices - 1)]
        return jnp.where(device < 0, -1, jnp.where(device >= devices, blocks, value))

    first = jnp.maximum(start_of(me - 2), 0)
    below = jnp.int32(0)
    for k in range(5 * slots):
        at = first + k
        owner = owners[jnp.minimum(at, blocks - 1)]
        below += jnp.where((at < blocks) & (owner < me), 1, 0)
    first = first + below
    for j in range(owned):
        block = first + j
        live = (block < blocks) & (owners[jnp.minimum(block, blocks - 1)] == me)
        place = jnp.int32(0)
        for delta in (-1, 0, 1, 2):
            place += jnp.where(start_of(me + delta) <= block, 1, 0)
        slot = block - starts[jnp.clip(me + place - 2, 0, devices - 1)]
        table[0, j] = jnp.where(live, 1, 0)
        table[1, j] = jnp.where(live, jnp.clip(place, 0, 4), 0)
        table[2, j] = jnp.where(live, jnp.clip(slot, 0, slots - 1), 0)
    for k in range(5):
        holder = me + k - 2
        begin, end = start_of(holder), start_of(holder + 1)
        for s in range(slots):
            block = begin + s
            valid = (holder >= 0) & (holder < devices) & (block < end) & (owners[jnp.clip(block, 0, blocks - 1)] == me)
            table[3 + 2 * k, s] = jnp.where(valid, 1, 0)
            table[4 + 2 * k, s] = jnp.where(valid, jnp.clip(block - first, 0, owned - 1), 0)

    loads[4].wait()
    loads[5].wait()
    loads[6].wait()

    def prepare(j):
        whole = left[j]
        l_two = split(whole.T)
        r_two = split(right[j])
        h_two = split(left[j, rows])
        lt_high[j], lt_low[j] = l_two
        r_high[j], r_low[j] = r_two
        lh_high[j], lh_low[j] = h_two
        turned = dot_three(split(dot_three(l_two, split(moment[j]), NN)), r_two, NN)
        base[j] = BETA_ONE * turned

    def relay(s):
        for side in sides:

            @pl.when(side["has"])
            def _():
                ring(2, side["near"], s, side["peer"]).wait_recv()

            @pl.when(side["has"] & side["sends"])
            def _():
                ring(side["near"], side["far"], s, side["peer"]).start()

            @pl.when(side["has"])
            def _():
                hand(side["near"], s).start()

    @pl.loop(0, owned)
    def _(j):
        prepare(j)

        @pl.when(j >= owned - slots)
        def _():
            relay(j - (owned - slots))

    loads[7].wait()
    for s in range(slots):
        for side in sides:

            @pl.when(side["gives"])
            def _():
                ring(side["near"], side["far"], s, side["peer"]).wait_recv()
                hand(side["far"], s).start()

    swap.wait_send()
    for s in range(slots):
        hand(2, s).wait_send()
        hand(2, s).wait_recv()
    for side in sides:

        @pl.when(side["sends"])
        def _():
            for s in range(slots):
                ring(2, side["near"], s, side["peer"]).wait_send()

        @pl.when(side["has"] & side["sends"])
        def _():
            for s in range(slots):
                ring(side["near"], side["far"], s, side["peer"]).wait_send()

        @pl.when(side["has"])
        def _():
            for s in range(slots):
                hand(side["near"], s).wait_send()
                hand(side["near"], s).wait_recv()

        @pl.when(side["gives"])
        def _():
            for s in range(slots):
                hand(side["far"], s).wait_send()
                hand(side["far"], s).wait_recv()

    def solve(j):
        live = table[0, j] == 1
        gradient = gathered[table[1, j], table[2, j]]
        r_two = (r_high[j], r_low[j])
        first_out[j] = jnp.where(live, BETA_ONE * moment[j] + (1.0 - BETA_ONE) * gradient.astype(F32), 0.0)
        half_turned = dot(lt_high[j], gradient, NN) + dot(lt_low[j], gradient, NN)
        turned = dot_three(split(half_turned), r_two, NN)
        second_next = BETA_TWO * second[j] + (1.0 - BETA_TWO) * turned * turned
        second_out[j] = jnp.where(live, second_next, 0.0)
        bias_one = 1.0 - BETA_ONE**STEP
        bias_two = 1.0 - BETA_TWO**STEP
        turned_moment = base[j] + (1.0 - BETA_ONE) * turned
        scaled = turned_moment * (1.0 / bias_one) / (jnp.sqrt(second_next * (1.0 / bias_two)) + EPSILON)
        new = dot_three(split(dot_three((lh_high[j], lh_low[j]), split(scaled), NN)), r_two, NT)
        largest = jnp.maximum(jnp.max(jnp.abs(new), axis=0, keepdims=True), 1e-30)
        update[j] = jnp.round(new * (TOP / largest)).astype(jnp.int32).astype(I16)
        update_scales[j] = largest * (1.0 / TOP)

    @pl.loop(0, owned // GROUP)
    def _(step):
        for at in range(GROUP):
            solve(step * GROUP + at)

    def chosen(k, s, absent):
        return jnp.where(table[3 + 2 * k, s] == 1, update[table[4 + 2 * k, s]], absent)

    def chosen_scale(k, s, absent):
        return jnp.where(table[3 + 2 * k, s] == 1, update_scales[table[4 + 2 * k, s]], absent)

    def far(side, s):
        at = side["at"]
        return push(codes.at[at, s], far_in.at[at, s], back_send.at[at, s], back_recv.at[at, s], side["peer"])

    def far_scale(side):
        at = side["at"]
        return push(scales.at[at], far_scales.at[at], sf_send.at[at], sf_recv.at[at], side["peer"])

    def near(side, s):
        at = side["at"]
        return push(merged.at[at, s], out.at[at, s, rows], near_send.at[at, s], near_recv.at[at, s], side["peer"])

    def near_scale(side):
        at = side["at"]
        return push(merged_scales.at[at], out_scales.at[at, core], sr_send.at[at], sr_recv.at[at], side["peer"])

    def give(k, s):
        return push(out.at[k, s, rows], out.at[k, s, rows], give_send.at[k, s], give_recv.at[k, s], twin)

    def give_scale(k):
        return push(out_scales.at[k, core], out_scales.at[k, core], sh_send.at[k], sh_recv.at[k], twin)

    for s in range(slots):
        for side in sides:
            codes[side["at"], s] = chosen(side["to_far"], s, jnp.zeros((), I16))
            pl.when(side["sends"])(far(side, s).start)
    for side in sides:
        for s in range(slots):
            scales[side["at"], pl.ds(s, 1)] = chosen_scale(side["to_far"], s, 0.0)
        pl.when(side["sends"])(far_scale(side).start)
    for s in range(slots):
        out[2, s, rows] = chosen(2, s, jnp.zeros((), I16))
        give(2, s).start()
        out_scales[2, core, pl.ds(s, 1)] = chosen_scale(2, s, 0.0)
    give_scale(2).start()
    for s in range(slots):
        for side in sides:
            pl.when(side["has"])(far(side, s).wait_recv)
            merged[side["at"], s] = chosen(side["to_near"], s, far_in[side["at"], s])
            pl.when(side["sends"])(near(side, s).start)
    for side in sides:
        pl.when(side["has"])(far_scale(side).wait_recv)
        for s in range(slots):
            merged_scales[side["at"], pl.ds(s, 1)] = chosen_scale(side["to_near"], s, far_scales[side["at"], pl.ds(s, 1)])
        pl.when(side["sends"])(near_scale(side).start)
    for s in range(slots):
        for side in sides:

            @pl.when(side["has"])
            def _():
                near(side, s).wait_recv()
                give(side["at"], s).start()

    for side in sides:

        @pl.when(side["has"])
        def _():
            near_scale(side).wait_recv()
            give_scale(side["at"]).start()

    give_scale(2).wait_send()
    give_scale(2).wait_recv()
    for s in range(slots):
        give(2, s).wait_send()
        give(2, s).wait_recv()
    for side in sides:

        @pl.when(side["sends"])
        def _():
            far_scale(side).wait_send()
            near_scale(side).wait_send()
            for s in range(slots):
                far(side, s).wait_send()
                near(side, s).wait_send()

        @pl.when(side["has"])
        def _():
            give_scale(side["at"]).wait_send()
            give_scale(side["at"]).wait_recv()
            for s in range(slots):
                give(side["at"], s).wait_send()
                give(side["at"], s).wait_recv()


def finish_kernel(codes, scales, first, second, direction, first_new, second_new, decoded, sem):
    slots = codes.shape[1]
    half = codes.shape[2] // 2
    copies = [pltpu.make_async_copy(first, first_new, sem.at[0]), pltpu.make_async_copy(second, second_new, sem.at[1])]
    for copy in copies:
        copy.start()
    for s in range(slots):
        for core in range(2):
            rows = pl.ds(core * half, half)
            total = 0.0
            for k in range(3):
                total += codes[k, s, rows].astype(jnp.int32).astype(F32) * scales[k, core, pl.ds(s, 1)]
            decoded[s, rows] = total
        copy = pltpu.make_async_copy(decoded.at[s], direction.at[s], sem.at[2 + s])
        copy.start()
        copies.append(copy)
    for copy in copies:
        copy.wait()


def body(gradients, first_moment, second_moment, left_basis, right_basis, shard_starts, block_owners):
    devices = lax.axis_size("fsdp")
    slots = gradients.shape[1]
    owned, width = first_moment.shape[0], first_moment.shape[1]
    half = width // 2
    any_space = pl.BlockSpec(memory_space=pl.ANY)
    in_vmem = pl.BlockSpec(memory_space=pltpu.VMEM)
    dma = pltpu.SemaphoreType.DMA
    keep = functools.partial(pltpu.with_memory_space_constraint, memory_space=pltpu.VMEM)
    stay = functools.partial(pltpu.with_memory_space_constraint, memory_space=pltpu.HBM)
    matrices = (owned, width, width)
    halves = (owned, half, width)
    first_new, second_new, out, out_scales = pl.pallas_call(
        functools.partial(soap_kernel, devices),
        out_shape=[
            pltpu.VMEM(matrices, F32),
            pltpu.VMEM(matrices, F32),
            pltpu.VMEM((3, slots, width, width), I16),
            pltpu.VMEM((3, 2, slots, width), F32),
        ],
        in_specs=[any_space] * 7,
        out_specs=[in_vmem] * 4,
        scratch_shapes=[
            pltpu.SMEM(shard_starts.shape, jnp.int32),
            pltpu.SMEM(block_owners.shape, jnp.int32),
            pltpu.SMEM((13, 8), jnp.int32),
            *[pltpu.VMEM((slots, half, width), BF16)] * 3,
            pltpu.VMEM((5, slots, width, width), BF16),
            *[pltpu.VMEM(matrices, F32)] * 4,
            *[pltpu.VMEM(matrices, BF16)] * 2,
            *[pltpu.VMEM(halves, BF16)] * 2,
            *[pltpu.VMEM(matrices, BF16)] * 2,
            pltpu.VMEM(matrices, F32),
            pltpu.VMEM(halves, I16),
            pltpu.VMEM((owned, 1, width), F32),
            *[pltpu.VMEM((2, slots, half, width), I16), pltpu.VMEM((2, slots, width), F32)] * 3,
            dma((8,)), dma((2,)), *[dma((5, slots))] * 4, *[dma((2, slots))] * 4, *[dma((3, slots))] * 2, *[dma((2,))] * 4, *[dma((3,))] * 2,
        ],
        compiler_params=pltpu.CompilerParams(collective_id=0, has_side_effects=True, vmem_limit_bytes=ROOM),
        name="soap",
    )(*map(stay, (shard_starts, block_owners, gradients, first_moment, second_moment, left_basis, right_basis)))

    return tuple(
        pl.pallas_call(
            finish_kernel,
            out_shape=[
                jax.ShapeDtypeStruct((slots, width, width), F32),
                jax.ShapeDtypeStruct(matrices, F32),
                jax.ShapeDtypeStruct(matrices, F32),
            ],
            in_specs=[in_vmem] * 4,
            out_specs=[any_space] * 3,
            scratch_shapes=[pltpu.VMEM((slots, width, width), F32), dma((2 + slots,))],
            compiler_params=pltpu.CompilerParams(vmem_limit_bytes=8 * 2**20),
            name="finish",
        )(*map(keep, (out, out_scales, first_new, second_new)))
    )


def solution(mesh):
    in_specs = (
        P("dp", "fsdp", None, None),
        P("fsdp", None, None),
        P("fsdp", None, None),
        P("fsdp", None, None),
        P("fsdp", None, None),
        P(),
        P(),
    )
    out_specs = (P("fsdp", None, None), P("fsdp", None, None), P("fsdp", None, None))
    return jax.shard_map(body, mesh=mesh, in_specs=in_specs, out_specs=out_specs, check_vma=False)
```

```python
import functools

import jax
import jax.numpy as jnp
from jax import lax
from jax.experimental import pallas as pl
from jax.experimental.pallas import tpu as pltpu
from jax.sharding import PartitionSpec as P

STEP = 10
BETA_ONE = 0.9
BETA_TWO = 0.95
EPSILON = 1e-08
TOP = 32766.0
ROOM = 40 * 2**20
MESH = pl.DeviceIdType.MESH
F32 = jnp.float32
BF16 = jnp.bfloat16
I16 = jnp.int16


def neighbours(devices):
    me = lax.axis_index("fsdp")
    core = lax.axis_index("dp")
    right = {"fsdp": jnp.minimum(me + 1, devices - 1)}
    left = {"fsdp": jnp.maximum(me - 1, 0)}
    twin = {"dp": 1 - core}
    return me, core, right, left, twin


def greet(me, devices, right, left, twin):
    barrier = pltpu.get_barrier_semaphore()

    def signal(peer):
        pl.semaphore_signal(barrier, inc=1, device_id=peer, device_id_type=MESH)

    signal(twin)
    pl.when(me < devices - 1)(lambda: signal(right))
    pl.when(me > 0)(lambda: signal(left))
    at_end = (me == 0) | (me == devices - 1)
    pl.when(at_end)(lambda: pl.semaphore_wait(barrier, 2))
    pl.when(~at_end)(lambda: pl.semaphore_wait(barrier, 3))


def push(src, dst, send_sem, recv_sem, peer):
    return pltpu.make_async_remote_copy(
        src_ref=src,
        dst_ref=dst,
        send_sem=send_sem,
        recv_sem=recv_sem,
        device_id=peer,
        device_id_type=MESH,
    )


def split(x):
    high = x.astype(BF16)
    return high, (x - high.astype(F32)).astype(BF16)


def dot(a, b, dims):
    return lax.dot_general(a, b, (dims, ((), ())), preferred_element_type=F32)


def dot_three(a, b, dims):
    return dot(a[0], b[0], dims) + (dot(a[0], b[1], dims) + dot(a[1], b[0], dims))


NN = ((1,), (0,))
NT = ((1,), (1,))
GROUP = 2
WAVE = 2
LATE = 4


def soap_kernel(
    devices, starts_in, owners_in, grad, moment_in, second_in, left_in, right_in, first_out, second_out, out, out_scales,
    starts, owners, table, mine, theirs, other, gathered_a, gathered_b, moment, second, left, right, lt_high, lt_low, lh_high, lh_low, r_high, r_low,
    base, update_a, update_b, scales_a, scales_b, second_late, codes, scales, far_in, far_scales, merged, merged_scales,
    load_sem, swap_send, swap_recv, own_send, relay_send, ring_recv, hand_send, hand_recv, far_send, far_recv, near_send, near_recv, give_send, give_recv,
    sf_send, sf_recv, sr_send, sr_recv, sh_send, sh_recv
):
    me, core, right_peer, left_peer, twin = neighbours(devices)
    slots = grad.shape[1]
    half = grad.shape[2] // 2
    owned = moment.shape[0]
    blocks = owners.shape[0]
    rows = pl.ds(pl.multiple_of(core * half, half), half)
    other_rows = pl.ds(pl.multiple_of((1 - core) * half, half), half)
    gathered = (gathered_a, gathered_b)

    loads = [
        pltpu.make_async_copy(src, dst, load_sem.at[at])
        for at, (src, dst) in enumerate(
            (
                (grad.at[0, :, other_rows], other),
                (grad.at[0, :, rows], mine),
                (starts_in, starts),
                (owners_in, owners),
                (left_in, left),
                (moment_in, moment),
                (right_in, right),
                (second_in, second),
            )
        )
    ]
    for load in loads:
        load.start()
    greet(me, devices, right_peer, left_peer, twin)

    def swap(w):
        part = pl.ds(WAVE * w, WAVE)
        return push(other.at[part], theirs.at[part], swap_send.at[w], swap_recv.at[w], twin)

    def own(w, side, t):
        source = gathered[w].at[2, t, rows] if t is not None else gathered[w].at[2, :, rows]
        target = gathered[w].at[side["near"], t, rows] if t is not None else gathered[w].at[side["near"], :, rows]
        arrived = ring_recv.at[side["near"], WAVE * w + (t or 0)]
        return push(source, target, own_send.at[side["at"], w], arrived, side["peer"])

    def relay(w, side, t):
        source = gathered[w].at[side["near"], t, rows] if t is not None else gathered[w].at[side["near"], :, rows]
        target = gathered[w].at[side["far"], t, rows] if t is not None else gathered[w].at[side["far"], :, rows]
        arrived = ring_recv.at[side["far"], WAVE * w + (t or 0)]
        return push(source, target, relay_send.at[side["at"], w], arrived, side["peer"])

    def hand(w, k, t):
        part = gathered[w].at[k, t, rows] if t is not None else gathered[w].at[k, :, rows]
        return push(part, part, hand_send.at[w, k], hand_recv.at[w, k], twin)

    to_right = dict(at=0, near=1, far=0, peer=right_peer, has=me >= 1, gives=me >= 2, sends=me < devices - 1, to_far=4, to_near=3)
    to_left = dict(at=1, near=3, far=4, peer=left_peer, has=me < devices - 1, gives=me < devices - 2, sends=me >= 1, to_far=0, to_near=1)
    sides = (to_right, to_left)

    def send_own(w, side):
        @pl.when(side["sends"])
        def _():
            for t in range(WAVE):
                own(w, side, t).start()

    def send_on(w, side):
        for t in range(WAVE):

            @pl.when(side["has"])
            def _():
                own(w, side, t).wait_recv()

            @pl.when(side["has"] & side["sends"])
            def _():
                relay(w, side, t).start()

            @pl.when(side["has"])
            def _():
                hand(w, side["near"], t).start()

    def add_up(w):
        swap(w).wait_recv()
        for t in range(WAVE):
            s = WAVE * w + t
            gathered[w][2, t, rows] = (mine[s].astype(F32) + theirs[s].astype(F32)).astype(BF16)

    loads[0].wait()
    swap(0).start()
    swap(1).start()
    loads[1].wait()
    add_up(0)
    for side in sides:
        send_own(0, side)
    for t in range(WAVE):
        hand(0, 2, t).start()
    add_up(1)
    for t in range(WAVE):
        hand(1, 2, t).start()

    for side in sides:

        @pl.when(~side["has"])
        def _():
            far_in[side["at"]] = jnp.zeros(far_in.shape[1:], I16)
            far_scales[side["at"]] = jnp.zeros(far_scales.shape[1:], F32)
            out[side["at"]] = jnp.zeros(out.shape[1:], I16)
            out_scales[side["at"]] = jnp.zeros(out_scales.shape[1:], F32)
            for w in range(2):
                gathered[w][side["near"]] = jnp.zeros(gathered[w].shape[1:], BF16)

        @pl.when(~side["gives"])
        def _():
            for w in range(2):
                gathered[w][side["far"]] = jnp.zeros(gathered[w].shape[1:], BF16)

    loads[2].wait()
    loads[3].wait()

    def start_of(device):
        value = starts[jnp.clip(device, 0, devices - 1)]
        return jnp.where(device < 0, -1, jnp.where(device >= devices, blocks, value))

    first = jnp.maximum(start_of(me - 2), 0)
    below = jnp.int32(0)
    for k in range(5 * slots):
        at = first + k
        owner = owners[jnp.minimum(at, blocks - 1)]
        below += jnp.where((at < blocks) & (owner < me), 1, 0)
    first = first + below
    rank = jnp.int32(0)
    chosen_late = [jnp.int32(0)] * LATE
    for j in range(owned):
        block = first + j
        live = (block < blocks) & (owners[jnp.minimum(block, blocks - 1)] == me)
        place = jnp.int32(0)
        for delta in (-1, 0, 1, 2):
            place += jnp.where(start_of(me + delta) <= block, 1, 0)
        slot = block - starts[jnp.clip(me + place - 2, 0, devices - 1)]
        late = live & (slot >= WAVE)
        table[0, j] = jnp.where(live & ~late, 1, 0)
        table[1, j] = jnp.where(late, 1, 0)
        table[2, j] = jnp.where(live, jnp.clip(place, 0, 4), 0)
        table[3, j] = jnp.where(live, jnp.clip(lax.rem(slot, WAVE), 0, WAVE - 1), 0)
        table[4, j] = rank
        for b in range(LATE):
            chosen_late[b] = jnp.where(late & (rank == b), j, chosen_late[b])
        rank = jnp.minimum(rank + jnp.where(late, 1, 0), LATE - 1)
    for b in range(LATE):
        table[5, b] = chosen_late[b]
    for k in range(5):
        holder = me + k - 2
        begin, end = start_of(holder), start_of(holder + 1)
        for s in range(slots):
            block = begin + s
            valid = (holder >= 0) & (holder < devices) & (block < end) & (owners[jnp.clip(block, 0, blocks - 1)] == me)
            table[6 + 2 * k, s] = jnp.where(valid, 1, 0)
            table[7 + 2 * k, s] = jnp.where(valid, jnp.clip(block - first, 0, owned - 1), 0)

    loads[4].wait()
    loads[5].wait()
    loads[6].wait()

    def prepare(j):
        whole = left[j]
        l_two = split(whole.T)
        r_two = split(right[j])
        h_two = split(left[j, rows])
        lt_high[j], lt_low[j] = l_two
        r_high[j], r_low[j] = r_two
        lh_high[j], lh_low[j] = h_two
        turned = dot_three(split(dot_three(l_two, split(moment[j]), NN)), r_two, NN)
        base[j] = BETA_ONE * turned

    place_in_plane = lax.rem(me, 16)
    z_left, z_right = place_in_plane == 0, place_in_plane == 15
    z_edge = z_left | z_right
    x_left = (lax.rem(me, 4) == 0) & ~z_left

    def middle(first_side, second_side):
        for side in (first_side, second_side):
            send_on(0, side)
            send_own(1, side)

    def middle_at_edge(early, late):
        send_own(1, late)
        send_on(0, early)
        send_own(1, early)
        send_on(1, early)
        send_on(0, late)

    @pl.loop(0, owned // 2)
    def _(j):
        prepare(j)

    pl.when(z_left)(lambda: middle_at_edge(to_left, to_right))
    pl.when(z_right)(lambda: middle_at_edge(to_right, to_left))
    pl.when(x_left)(lambda: middle(to_left, to_right))
    pl.when(~z_edge & ~x_left)(lambda: middle(to_right, to_left))

    @pl.loop(owned // 2, owned)
    def _(j):
        prepare(j)

    loads[7].wait()

    def arrive(w):
        for t in range(WAVE):
            for side in sides:

                @pl.when(side["gives"])
                def _():
                    relay(w, side, t).wait_recv()
                    hand(w, side["far"], t).start()

        hand(w, 2, None).wait_recv()
        for side in sides:

            @pl.when(side["has"])
            def _():
                hand(w, side["near"], None).wait_recv()

            @pl.when(side["gives"])
            def _():
                hand(w, side["far"], None).wait_recv()

    def solve(j, gradient):
        r_two = (r_high[j], r_low[j])
        half_turned = dot(lt_high[j], gradient, NN) + dot(lt_low[j], gradient, NN)
        turned = dot_three(split(half_turned), r_two, NN)
        second_next = BETA_TWO * second[j] + (1.0 - BETA_TWO) * turned * turned
        bias_one = 1.0 - BETA_ONE**STEP
        bias_two = 1.0 - BETA_TWO**STEP
        turned_moment = base[j] + (1.0 - BETA_ONE) * turned
        scaled = turned_moment * (1.0 / bias_one) / (jnp.sqrt(second_next * (1.0 / bias_two)) + EPSILON)
        new = dot_three(split(dot_three((lh_high[j], lh_low[j]), split(scaled), NN)), r_two, NT)
        largest = jnp.maximum(jnp.max(jnp.abs(new), axis=0, keepdims=True), 1e-30)
        return second_next, jnp.round(new * (TOP / largest)).astype(jnp.int32).astype(I16), largest * (1.0 / TOP)

    arrive(0)

    @pl.loop(0, owned // GROUP)
    def _(step):
        @pl.when((step == 1) & ~z_left)
        def _():
            pl.when(~z_right)(lambda: send_on(1, to_right))
            send_on(1, to_left)

        @pl.when((step == 1) & z_left)
        def _():
            send_on(1, to_right)

        for at in range(GROUP):
            j = step * GROUP + at
            second_out[j], update_a[j], scales_a[j] = solve(j, gathered_a[table[2, j], table[3, j]])

    def chosen(k, s, absent):
        at = table[7 + 2 * k, s]
        value = update_a[at] if s < WAVE else update_b[table[4, at]]
        return jnp.where(table[6 + 2 * k, s] == 1, value, absent)

    def chosen_scale(k, s, absent):
        at = table[7 + 2 * k, s]
        value = scales_a[at] if s < WAVE else scales_b[table[4, at]]
        return jnp.where(table[6 + 2 * k, s] == 1, value, absent)

    def far(w, side, t):
        at = side["at"]
        part = (at, w, t) if t is not None else (at, w)
        return push(codes.at[part], far_in.at[part], far_send.at[at, w], far_recv.at[at, WAVE * w + (t or 0)], side["peer"])

    def far_scale(w, side):
        at = side["at"]
        return push(scales.at[at, w], far_scales.at[at, w], sf_send.at[at, w], sf_recv.at[at, w], side["peer"])

    def near(w, side, t):
        at = side["at"]
        part = (at, w, t) if t is not None else (at, w)
        held = (at, WAVE * w + t, rows) if t is not None else (at, pl.ds(WAVE * w, WAVE), rows)
        return push(merged.at[part], out.at[held], near_send.at[at, w], near_recv.at[at, WAVE * w + (t or 0)], side["peer"])

    def near_scale(w, side):
        at = side["at"]
        return push(merged_scales.at[at, w], out_scales.at[at, core, w], sr_send.at[at, w], sr_recv.at[at, w], side["peer"])

    def give(k, s):
        part = out.at[k, s, rows] if s is not None else out.at[k, :, rows]
        return push(part, part, give_send.at[k], give_recv.at[k], twin)

    def give_scale(k):
        return push(out_scales.at[k, core], out_scales.at[k, core], sh_send.at[k], sh_recv.at[k], twin)

    def send_far(w):
        for t in range(WAVE):
            for side in sides:
                codes[side["at"], w, t] = chosen(side["to_far"], WAVE * w + t, jnp.zeros((), I16))
                pl.when(side["sends"])(far(w, side, t).start)
        for side in sides:
            for t in range(WAVE):
                scales[side["at"], w, pl.ds(t, 1)] = chosen_scale(side["to_far"], WAVE * w + t, 0.0)
            pl.when(side["sends"])(far_scale(w, side).start)
        for t in range(WAVE):
            s = WAVE * w + t
            out[2, s, rows] = chosen(2, s, jnp.zeros((), I16))
            give(2, s).start()
            out_scales[2, core, w, pl.ds(t, 1)] = chosen_scale(2, s, 0.0)

    def send_near(w, side):
        for t in range(WAVE):
            pl.when(side["has"])(far(w, side, t).wait_recv)
            merged[side["at"], w, t] = chosen(side["to_near"], WAVE * w + t, far_in[side["at"], w, t])
            pl.when(side["sends"])(near(w, side, t).start)
        pl.when(side["has"])(far_scale(w, side).wait_recv)
        for t in range(WAVE):
            merged_scales[side["at"], w, pl.ds(t, 1)] = chosen_scale(
                side["to_near"], WAVE * w + t, far_scales[side["at"], w, pl.ds(t, 1)]
            )
        pl.when(side["sends"])(near_scale(w, side).start)

    send_far(0)
    arrive(1)

    @pl.loop(0, LATE // GROUP)
    def _(step):
        for at in range(GROUP):
            b = step * GROUP + at
            j = table[5, b]
            second_late[b], update_b[b], scales_b[b] = solve(j, gathered_b[table[2, j], table[3, j]])

    send_far(1)
    give_scale(2).start()

    def send_all_near(order):
        for w, side in order:
            send_near(w, side)

    pl.when(z_left)(lambda: send_all_near(((0, to_left), (1, to_left), (0, to_right), (1, to_right))))
    pl.when(z_right)(lambda: send_all_near(((0, to_right), (1, to_right), (0, to_left), (1, to_left))))
    pl.when(x_left)(lambda: send_all_near(((0, to_left), (0, to_right), (1, to_left), (1, to_right))))
    pl.when(~z_edge & ~x_left)(lambda: send_all_near(((0, to_right), (0, to_left), (1, to_right), (1, to_left))))

    @pl.loop(0, owned)
    def _(j):
        early, late = table[0, j] == 1, table[1, j] == 1
        gradient = jnp.where(late, gathered_b[table[2, j], table[3, j]].astype(F32), gathered_a[table[2, j], table[3, j]].astype(F32))
        first_out[j] = jnp.where(early | late, BETA_ONE * moment[j] + (1.0 - BETA_ONE) * gradient, 0.0)
        second_out[j] = jnp.where(late, second_late[table[4, j]], jnp.where(early, second_out[j], 0.0))

    for s in range(slots):
        for side in sides:

            @pl.when(side["has"])
            def _():
                near(s // WAVE, side, s % WAVE).wait_recv()
                give(side["at"], s).start()

    for side in sides:

        @pl.when(side["has"])
        def _():
            for w in range(2):
                near_scale(w, side).wait_recv()
            give_scale(side["at"]).start()

    for w in range(2):
        swap(w).wait_send()
        hand(w, 2, None).wait_send()
    give(2, None).wait_send()
    give_scale(2).wait_send()
    for side in sides:

        @pl.when(side["sends"])
        def _():
            for w in range(2):
                own(w, side, None).wait_send()
                far(w, side, None).wait_send()
                far_scale(w, side).wait_send()
                near(w, side, None).wait_send()
                near_scale(w, side).wait_send()

        @pl.when(side["has"] & side["sends"])
        def _():
            for w in range(2):
                relay(w, side, None).wait_send()

        @pl.when(side["has"])
        def _():
            for w in range(2):
                hand(w, side["near"], None).wait_send()
            give(side["at"], None).wait_send()
            give_scale(side["at"]).wait_send()

        @pl.when(side["gives"])
        def _():
            for w in range(2):
                hand(w, side["far"], None).wait_send()

    give(2, None).wait_recv()
    give_scale(2).wait_recv()
    for side in sides:

        @pl.when(side["has"])
        def _():
            give(side["at"], None).wait_recv()
            give_scale(side["at"]).wait_recv()


def finish_kernel(codes, scales, first, second, direction, first_new, second_new, decoded, sem):
    slots = codes.shape[1]
    half = codes.shape[2] // 2
    copies = [pltpu.make_async_copy(first, first_new, sem.at[0]), pltpu.make_async_copy(second, second_new, sem.at[1])]
    for copy in copies:
        copy.start()
    for s in range(slots):
        for core in range(2):
            rows = pl.ds(core * half, half)
            total = 0.0
            for k in range(3):
                total += codes[k, s, rows].astype(jnp.int32).astype(F32) * scales[k, core, s // WAVE, pl.ds(s % WAVE, 1)]
            decoded[s, rows] = total
        copy = pltpu.make_async_copy(decoded.at[s], direction.at[s], sem.at[2 + s])
        copy.start()
        copies.append(copy)
    for copy in copies:
        copy.wait()


def body(gradients, first_moment, second_moment, left_basis, right_basis, shard_starts, block_owners):
    devices = lax.axis_size("fsdp")
    slots = gradients.shape[1]
    owned, width = first_moment.shape[0], first_moment.shape[1]
    half = width // 2
    any_space = pl.BlockSpec(memory_space=pl.ANY)
    in_vmem = pl.BlockSpec(memory_space=pltpu.VMEM)
    dma = pltpu.SemaphoreType.DMA
    keep = functools.partial(pltpu.with_memory_space_constraint, memory_space=pltpu.VMEM)
    stay = functools.partial(pltpu.with_memory_space_constraint, memory_space=pltpu.HBM)
    matrices = (owned, width, width)
    halves = (owned, half, width)
    first_new, second_new, out, out_scales = pl.pallas_call(
        functools.partial(soap_kernel, devices),
        out_shape=[
            pltpu.VMEM(matrices, F32),
            pltpu.VMEM(matrices, F32),
            pltpu.VMEM((3, slots, width, width), I16),
            pltpu.VMEM((3, 2, 2, WAVE, width), F32),
        ],
        in_specs=[any_space] * 7,
        out_specs=[in_vmem] * 4,
        scratch_shapes=[
            pltpu.SMEM(shard_starts.shape, jnp.int32),
            pltpu.SMEM(block_owners.shape, jnp.int32),
            pltpu.SMEM((16, 8), jnp.int32),
            *[pltpu.VMEM((slots, half, width), BF16)] * 3,
            *[pltpu.VMEM((5, WAVE, width, width), BF16)] * 2,
            *[pltpu.VMEM(matrices, F32)] * 4,
            *[pltpu.VMEM(matrices, BF16)] * 2,
            *[pltpu.VMEM(halves, BF16)] * 2,
            *[pltpu.VMEM(matrices, BF16)] * 2,
            pltpu.VMEM(matrices, F32),
            pltpu.VMEM(halves, I16),
            pltpu.VMEM((LATE, half, width), I16),
            pltpu.VMEM((owned, 1, width), F32),
            pltpu.VMEM((LATE, 1, width), F32),
            pltpu.VMEM((LATE, width, width), F32),
            *[pltpu.VMEM((2, 2, WAVE, half, width), I16), pltpu.VMEM((2, 2, WAVE, width), F32)] * 3,
            dma((8,)), *[dma((2,))] * 2, *[dma((2, 2))] * 2, dma((5, slots)), *[dma((2, 5))] * 2,
            *[dma((2, 2)), dma((2, slots))] * 2, *[dma((3,))] * 2, *[dma((2, 2))] * 4, *[dma((3,))] * 2,
        ],
        compiler_params=pltpu.CompilerParams(collective_id=0, has_side_effects=True, vmem_limit_bytes=ROOM),
        name="soap",
    )(*map(stay, (shard_starts, block_owners, gradients, first_moment, second_moment, left_basis, right_basis)))

    return tuple(
        pl.pallas_call(
            finish_kernel,
            out_shape=[
                jax.ShapeDtypeStruct((slots, width, width), F32),
                jax.ShapeDtypeStruct(matrices, F32),
                jax.ShapeDtypeStruct(matrices, F32),
            ],
            in_specs=[in_vmem] * 4,
            out_specs=[any_space] * 3,
            scratch_shapes=[pltpu.VMEM((slots, width, width), F32), dma((2 + slots,))],
            compiler_params=pltpu.CompilerParams(vmem_limit_bytes=8 * 2**20),
            name="finish",
        )(*map(keep, (out, out_scales, first_new, second_new)))
    )


def solution(mesh):
    in_specs = (
        P("dp", "fsdp", None, None),
        P("fsdp", None, None),
        P("fsdp", None, None),
        P("fsdp", None, None),
        P("fsdp", None, None),
        P(),
        P(),
    )
    out_specs = (P("fsdp", None, None), P("fsdp", None, None), P("fsdp", None, None))
    return jax.shard_map(body, mesh=mesh, in_specs=in_specs, out_specs=out_specs, check_vma=False)
```

```python
import functools

import jax
import jax.numpy as jnp
from jax import lax
from jax.experimental import pallas as pl
from jax.experimental.pallas import tpu as pltpu
from jax.sharding import PartitionSpec as P

STEP = 10
BETA_ONE = 0.9
BETA_TWO = 0.95
EPSILON = 1e-08
TOP = 32766.0
ROOM = 40 * 2**20
MESH = pl.DeviceIdType.MESH
F32 = jnp.float32
BF16 = jnp.bfloat16
I16 = jnp.int16


def neighbours(devices):
    me = lax.axis_index("fsdp")
    core = lax.axis_index("dp")
    right = {"fsdp": jnp.minimum(me + 1, devices - 1)}
    left = {"fsdp": jnp.maximum(me - 1, 0)}
    twin = {"dp": 1 - core}
    return me, core, right, left, twin


def greet(me, devices, right, left, twin):
    barrier = pltpu.get_barrier_semaphore()

    def signal(peer):
        pl.semaphore_signal(barrier, inc=1, device_id=peer, device_id_type=MESH)

    signal(twin)
    pl.when(me < devices - 1)(lambda: signal(right))
    pl.when(me > 0)(lambda: signal(left))
    at_end = (me == 0) | (me == devices - 1)
    pl.when(at_end)(lambda: pl.semaphore_wait(barrier, 2))
    pl.when(~at_end)(lambda: pl.semaphore_wait(barrier, 3))


def push(src, dst, send_sem, recv_sem, peer):
    return pltpu.make_async_remote_copy(
        src_ref=src,
        dst_ref=dst,
        send_sem=send_sem,
        recv_sem=recv_sem,
        device_id=peer,
        device_id_type=MESH,
    )


def split(x):
    high = x.astype(BF16)
    return high, (x - high.astype(F32)).astype(BF16)


def dot(a, b, dims):
    return lax.dot_general(a, b, (dims, ((), ())), preferred_element_type=F32)


def dot_three(a, b, dims):
    return dot(a[0], b[0], dims) + (dot(a[0], b[1], dims) + dot(a[1], b[0], dims))


NN = ((1,), (0,))
NT = ((1,), (1,))
GROUP = 2
WAVE = 2
LATE = 4


def soap_kernel(
    devices, starts_in, owners_in, grad, moment_in, second_in, left_in, right_in, first_out, second_out, out, out_scales,
    starts, owners, table, mine, theirs, other, gathered_a, gathered_b, moment, second, left, right, lt_two, lh_two, r_high, r_low, rt_high, rt_low,
    base, update_a, update_b, scales_a, scales_b, second_late, codes, scales, far_in, far_scales, merged, merged_scales,
    load_sem, swap_sem, own_send, relay_send, ring_recv, hand_send, hand_recv, far_send, far_recv, near_send, near_recv, give_sem, scale_send, scale_recv
):
    me, core, right_peer, left_peer, twin = neighbours(devices)
    slots = grad.shape[1]
    half = grad.shape[2] // 2
    owned = moment.shape[0]
    blocks = owners.shape[0]
    rows = pl.ds(pl.multiple_of(core * half, half), half)
    other_rows = pl.ds(pl.multiple_of((1 - core) * half, half), half)
    gathered = (gathered_a, gathered_b)

    loads = [
        pltpu.make_async_copy(src, dst, load_sem.at[at])
        for at, (src, dst) in enumerate(
            (
                (grad.at[0, :, other_rows], other),
                (grad.at[0, :, rows], mine),
                (starts_in, starts),
                (owners_in, owners),
                (left_in, left),
                (moment_in, moment),
                (right_in, right),
                (second_in, second),
            )
        )
    ]
    for load in loads:
        load.start()
    greet(me, devices, right_peer, left_peer, twin)

    swap = push(other, theirs, swap_sem.at[0], swap_sem.at[1], twin)

    def own(w, side, t):
        source = gathered[w].at[2, t, rows] if t is not None else gathered[w].at[2, :, rows]
        target = gathered[w].at[side["near"], t, rows] if t is not None else gathered[w].at[side["near"], :, rows]
        arrived = ring_recv.at[side["at"], WAVE * w + (t or 0)]
        return push(source, target, own_send.at[side["at"], w], arrived, side["peer"])

    def relay(w, side, t):
        source = gathered[w].at[side["near"], t, rows] if t is not None else gathered[w].at[side["near"], :, rows]
        target = gathered[w].at[side["far"], t, rows] if t is not None else gathered[w].at[side["far"], :, rows]
        arrived = ring_recv.at[2 + side["at"], WAVE * w + (t or 0)]
        return push(source, target, relay_send.at[side["at"], w], arrived, side["peer"])

    def hand(w, k=None, t=None):
        part = gathered[w].at[:, :, rows] if k is None else gathered[w].at[k, t, rows]
        return push(part, part, hand_send.at[w], hand_recv.at[w], twin)

    to_right = dict(at=0, near=1, far=0, peer=right_peer, has=me >= 1, gives=me >= 2, sends=me < devices - 1, to_far=4, to_near=3)
    to_left = dict(at=1, near=3, far=4, peer=left_peer, has=me < devices - 1, gives=me < devices - 2, sends=me >= 1, to_far=0, to_near=1)
    sides = (to_right, to_left)

    def send_own(w, side):
        @pl.when(side["sends"])
        def _():
            for t in range(WAVE):
                own(w, side, t).start()

    def send_on(w, side):
        for t in range(WAVE):

            @pl.when(side["has"])
            def _():
                own(w, side, t).wait_recv()

            @pl.when(side["has"] & side["sends"])
            def _():
                relay(w, side, t).start()

            hand(w, side["near"], t).start()

    loads[0].wait()
    swap.start()
    loads[1].wait()
    swap.wait_recv()
    for w in range(2):
        for t in range(WAVE):
            s = WAVE * w + t
            gathered[w][2, t, rows] = (mine[s].astype(F32) + theirs[s].astype(F32)).astype(BF16)
        for side in sides:
            send_own(w, side)
    for w in range(2):
        for t in range(WAVE):
            hand(w, 2, t).start()

    for side in sides:

        @pl.when(~side["has"])
        def _():
            far_in[side["at"]] = jnp.zeros(far_in.shape[1:], I16)
            far_scales[side["at"]] = jnp.zeros(far_scales.shape[1:], F32)
            out_scales[side["at"], core] = jnp.zeros(out_scales.shape[2:], F32)
            for s in range(slots):
                out[side["at"], s, rows] = jnp.zeros((half, out.shape[3]), I16)
                gathered[s // WAVE][side["near"], s % WAVE, rows] = jnp.zeros((half, out.shape[3]), BF16)

        @pl.when(~side["gives"])
        def _():
            for s in range(slots):
                gathered[s // WAVE][side["far"], s % WAVE, rows] = jnp.zeros((half, out.shape[3]), BF16)

    loads[2].wait()
    loads[3].wait()

    def start_of(device):
        value = starts[jnp.clip(device, 0, devices - 1)]
        return jnp.where(device < 0, -1, jnp.where(device >= devices, blocks, value))

    first = jnp.maximum(start_of(me - 2), 0)
    below = jnp.int32(0)
    for k in range(5 * slots):
        at = first + k
        owner = owners[jnp.minimum(at, blocks - 1)]
        below += jnp.where((at < blocks) & (owner < me), 1, 0)
    first = first + below
    rank = jnp.int32(0)
    chosen_late = [jnp.int32(0)] * LATE
    for j in range(owned):
        block = first + j
        live = (block < blocks) & (owners[jnp.minimum(block, blocks - 1)] == me)
        place = jnp.int32(0)
        for delta in (-1, 0, 1, 2):
            place += jnp.where(start_of(me + delta) <= block, 1, 0)
        slot = block - starts[jnp.clip(me + place - 2, 0, devices - 1)]
        late = live & (slot >= WAVE)
        table[0, j] = jnp.where(live & ~late, 1, 0)
        table[1, j] = jnp.where(late, 1, 0)
        table[2, j] = jnp.where(live, jnp.clip(place, 0, 4), 0)
        table[3, j] = jnp.where(live, jnp.clip(lax.rem(slot, WAVE), 0, WAVE - 1), 0)
        table[4, j] = rank
        for b in range(LATE):
            chosen_late[b] = jnp.where(late & (rank == b), j, chosen_late[b])
        rank = jnp.minimum(rank + jnp.where(late, 1, 0), LATE - 1)
    for b in range(LATE):
        table[5, b] = chosen_late[b]
    for k in range(5):
        holder = me + k - 2
        begin, end = start_of(holder), start_of(holder + 1)
        for s in range(slots):
            block = begin + s
            valid = (holder >= 0) & (holder < devices) & (block < end) & (owners[jnp.clip(block, 0, blocks - 1)] == me)
            table[6 + 2 * k, s] = jnp.where(valid, 1, 0)
            table[7 + 2 * k, s] = jnp.where(valid, jnp.clip(block - first, 0, owned - 1), 0)

    loads[4].wait()
    loads[5].wait()
    loads[6].wait()

    bias_one = 1.0 - BETA_ONE**STEP
    bias_two = 1.0 - BETA_TWO**STEP
    gain = bias_two**0.5 / bias_one

    def prepare(j):
        whole = left[j]
        l_two = split(whole.T)
        h_two = split(left[j, rows])
        r_two = split(right[j])
        for at in range(2):
            lt_two[j, at * whole.shape[0] : (at + 1) * whole.shape[0]] = l_two[at]
            lh_two[j, at * half : (at + 1) * half] = h_two[at]
        r_high[j], r_low[j] = r_two
        rt_high[j], rt_low[j] = split(right[j].T)
        turned = dot_three(split(dot_three(l_two, split(moment[j]), NN)), r_two, NN)
        base[j] = (BETA_ONE * gain) * turned

    @pl.loop(0, owned)
    def _(j):
        prepare(j)

    left_edge, right_edge = lax.rem(me, 4) == 0, lax.rem(me, 4) == 3

    def in_order(step):
        def each(order):
            for w, side in order:
                step(w, side)

        pl.when(left_edge)(lambda: each(((0, to_left), (1, to_left), (0, to_right), (1, to_right))))
        pl.when(right_edge)(lambda: each(((0, to_right), (1, to_right), (0, to_left), (1, to_left))))
        pl.when(~(left_edge | right_edge))(lambda: each(((0, to_right), (0, to_left), (1, to_right), (1, to_left))))

    in_order(send_on)
    loads[7].wait()

    def pass_far(w):
        for t in range(WAVE):
            for side in sides:
                pl.when(side["gives"])(relay(w, side, t).wait_recv)
                hand(w, side["far"], t).start()

    def stacked(two, b_high, b_low, size):
        full = dot(two, b_high, NN)
        return full[:size] + (full[size:] + dot(two[:size], b_low, NN))

    def solve(j, gradient):
        size = gradient.shape[0]
        both = dot(lt_two[j], gradient, NN)
        turned = stacked(jnp.concatenate(split(both[:size] + both[size:]), axis=0), r_high[j], r_low[j], size)
        second_next = BETA_TWO * second[j] + ((1.0 - BETA_TWO) * turned) * turned
        scaled = (base[j] + ((1.0 - BETA_ONE) * gain) * turned) / (second_next * lax.rsqrt(second_next) + EPSILON * bias_two**0.5)
        s_high, s_low = split(scaled)
        new = stacked(jnp.concatenate(split(stacked(lh_two[j], s_high, s_low, half)), axis=0), rt_high[j], rt_low[j], half)
        largest = jnp.maximum(jnp.max(jnp.abs(new), axis=0, keepdims=True), 1e-30)
        return second_next, jnp.round(new * (TOP / largest)).astype(jnp.int32).astype(I16), largest * (1.0 / TOP)

    pass_far(0)
    hand(0).wait_recv()

    @pl.loop(0, owned // GROUP)
    def _(step):
        @pl.when(step == owned // GROUP - 1)
        def _():
            pass_far(1)

        for at in range(GROUP):
            j = step * GROUP + at
            second_out[j], update_a[j], scales_a[j] = solve(j, gathered_a[table[2, j], table[3, j]])

    def chosen(k, s, absent):
        at = table[7 + 2 * k, s]
        value = update_a[at] if s < WAVE else update_b[table[4, at]]
        return jnp.where(table[6 + 2 * k, s] == 1, value, absent)

    def chosen_scale(k, s, absent):
        at = table[7 + 2 * k, s]
        value = scales_a[at] if s < WAVE else scales_b[table[4, at]]
        return jnp.where(table[6 + 2 * k, s] == 1, value, absent)

    def far(w, side, t):
        at = side["at"]
        part = (at, w, t) if t is not None else (at,)
        return push(codes.at[part], far_in.at[part], far_send.at[at], far_recv.at[at, WAVE * (w or 0) + (t or 0)], side["peer"])

    def far_scale(side):
        at = side["at"]
        return push(scales.at[at], far_scales.at[at], scale_send.at[at], scale_recv.at[at], side["peer"])

    def near(w, side, t):
        at = side["at"]
        part = (at, WAVE * w + t) if t is not None else (at,)
        held = (at, WAVE * w + t, rows) if t is not None else (at, slice(None), rows)
        return push(merged.at[part], out.at[held], near_send.at[at], near_recv.at[at, WAVE * (w or 0) + (t or 0)], side["peer"])

    def near_scale(side):
        at = side["at"]
        return push(merged_scales.at[at], out_scales.at[at, core], scale_send.at[2 + at], scale_recv.at[2 + at], side["peer"])

    def give(k=None, s=None):
        part = out.at[:, :, rows] if k is None else out.at[k, s, rows]
        return push(part, part, give_sem.at[0], give_sem.at[1], twin)

    def give_scale():
        part = out_scales.at[:, core]
        return push(part, part, scale_send.at[4], scale_recv.at[4], twin)

    def send_far(w):
        for t in range(WAVE):
            for side in sides:
                codes[side["at"], w, t] = chosen(side["to_far"], WAVE * w + t, jnp.zeros((), I16))
                pl.when(side["sends"])(far(w, side, t).start)
                scales[side["at"], w, pl.ds(t, 1)] = chosen_scale(side["to_far"], WAVE * w + t, 0.0)
        if w == 1:
            for side in sides:
                pl.when(side["sends"])(far_scale(side).start)
        for t in range(WAVE):
            s = WAVE * w + t
            out[2, s, rows] = chosen(2, s, jnp.zeros((), I16))
            give(2, s).start()
            out_scales[2, core, w, pl.ds(t, 1)] = chosen_scale(2, s, 0.0)

    def send_near(w, side):
        for t in range(WAVE):
            pl.when(side["has"])(far(w, side, t).wait_recv)
            merged[side["at"], WAVE * w + t] = chosen(side["to_near"], WAVE * w + t, far_in[side["at"], w, t])
            pl.when(side["sends"])(near(w, side, t).start)
        if w == 1:
            pl.when(side["has"])(far_scale(side).wait_recv)
            for s in range(slots):
                place = (side["at"], s // WAVE, pl.ds(s % WAVE, 1))
                merged_scales[place] = chosen_scale(side["to_near"], s, far_scales[place])
            pl.when(side["sends"])(near_scale(side).start)

    send_far(0)
    hand(1).wait_recv()

    @pl.loop(0, LATE // GROUP)
    def _(step):
        for at in range(GROUP):
            b = step * GROUP + at
            j = table[5, b]
            second_late[b], update_b[b], scales_b[b] = solve(j, gathered_b[table[2, j], table[3, j]])

    send_far(1)
    in_order(send_near)

    @pl.loop(0, owned)
    def _(j):
        early, late = table[0, j] == 1, table[1, j] == 1
        gradient = jnp.where(late, gathered_b[table[2, j], table[3, j]].astype(F32), gathered_a[table[2, j], table[3, j]].astype(F32))
        first_out[j] = jnp.where(early | late, BETA_ONE * moment[j] + (1.0 - BETA_ONE) * gradient, 0.0)
        second_out[j] = jnp.where(late, second_late[table[4, j]], jnp.where(early, second_out[j], 0.0))

    for s in range(slots):
        for side in sides:
            pl.when(side["has"])(near(s // WAVE, side, s % WAVE).wait_recv)
            give(side["at"], s).start()
    for side in sides:
        pl.when(side["has"])(near_scale(side).wait_recv)
    give_scale().start()

    swap.wait_send()
    for w in range(2):
        hand(w).wait_send()
    for side in sides:

        @pl.when(side["sends"])
        def _():
            for w in range(2):
                own(w, side, None).wait_send()
            far(None, side, None).wait_send()
            far_scale(side).wait_send()
            near(None, side, None).wait_send()
            near_scale(side).wait_send()

        @pl.when(side["has"] & side["sends"])
        def _():
            for w in range(2):
                relay(w, side, None).wait_send()

    give().wait_send()
    give_scale().wait_send()
    give().wait_recv()
    give_scale().wait_recv()


def finish_kernel(codes, scales, first, second, direction, first_new, second_new, decoded, sem):
    slots = codes.shape[1]
    half = codes.shape[2] // 2
    copies = [pltpu.make_async_copy(first, first_new, sem.at[0]), pltpu.make_async_copy(second, second_new, sem.at[1])]
    for j in range(first.shape[0]):
        pltpu.make_async_copy(first.at[j], first_new.at[j], sem.at[0]).start()
        pltpu.make_async_copy(second.at[j], second_new.at[j], sem.at[1]).start()
    for s in range(slots):
        for core in range(2):
            rows = pl.ds(core * half, half)
            total = 0.0
            for k in range(3):
                total += codes[k, s, rows].astype(jnp.int32).astype(F32) * scales[k, core, s // WAVE, pl.ds(s % WAVE, 1)]
            decoded[s, rows] = total
        copy = pltpu.make_async_copy(decoded.at[s], direction.at[s], sem.at[2 + s])
        copy.start()
        copies.append(copy)
    for copy in copies:
        copy.wait()


def body(gradients, first_moment, second_moment, left_basis, right_basis, shard_starts, block_owners):
    devices = lax.axis_size("fsdp")
    slots = gradients.shape[1]
    owned, width = first_moment.shape[0], first_moment.shape[1]
    half = width // 2
    any_space = pl.BlockSpec(memory_space=pl.ANY)
    in_vmem = pl.BlockSpec(memory_space=pltpu.VMEM)
    dma = pltpu.SemaphoreType.DMA
    keep = functools.partial(pltpu.with_memory_space_constraint, memory_space=pltpu.VMEM)
    stay = functools.partial(pltpu.with_memory_space_constraint, memory_space=pltpu.HBM)
    matrices = (owned, width, width)
    halves = (owned, half, width)
    first_new, second_new, out, out_scales = pl.pallas_call(
        functools.partial(soap_kernel, devices),
        out_shape=[
            pltpu.VMEM(matrices, F32),
            pltpu.VMEM(matrices, F32),
            pltpu.VMEM((3, slots, width, width), I16),
            pltpu.VMEM((3, 2, 2, WAVE, width), F32),
        ],
        in_specs=[any_space] * 7,
        out_specs=[in_vmem] * 4,
        scratch_shapes=[
            pltpu.SMEM(shard_starts.shape, jnp.int32),
            pltpu.SMEM(block_owners.shape, jnp.int32),
            pltpu.SMEM((16, 8), jnp.int32),
            *[pltpu.VMEM((slots, half, width), BF16)] * 3,
            *[pltpu.VMEM((5, WAVE, width, width), BF16)] * 2,
            *[pltpu.VMEM(matrices, F32)] * 4,
            pltpu.VMEM((owned, 2 * width, width), BF16),
            pltpu.VMEM((owned, width, width), BF16),
            *[pltpu.VMEM(matrices, BF16)] * 4,
            pltpu.VMEM(matrices, F32),
            pltpu.VMEM(halves, I16),
            pltpu.VMEM((LATE, half, width), I16),
            pltpu.VMEM((owned, 1, width), F32),
            pltpu.VMEM((LATE, 1, width), F32),
            pltpu.VMEM((LATE, width, width), F32),
            *[pltpu.VMEM((2, 2, WAVE, half, width), I16), pltpu.VMEM((2, 2, WAVE, width), F32)] * 2,
            pltpu.VMEM((2, slots, half, width), I16),
            pltpu.VMEM((2, 2, WAVE, width), F32),
            dma((8,)), dma((2,)), *[dma((2, 2))] * 2, dma((4, slots)), *[dma((2,))] * 2,
            *[dma((2,)), dma((2, slots))] * 2, dma((2,)), *[dma((5,))] * 2,
        ],
        compiler_params=pltpu.CompilerParams(collective_id=0, has_side_effects=True, vmem_limit_bytes=ROOM),
        name="soap",
    )(*map(stay, (shard_starts, block_owners, gradients, first_moment, second_moment, left_basis, right_basis)))

    return tuple(
        pl.pallas_call(
            finish_kernel,
            out_shape=[
                jax.ShapeDtypeStruct((slots, width, width), F32),
                jax.ShapeDtypeStruct(matrices, F32),
                jax.ShapeDtypeStruct(matrices, F32),
            ],
            in_specs=[in_vmem] * 4,
            out_specs=[any_space] * 3,
            scratch_shapes=[pltpu.VMEM((slots, width, width), F32), dma((2 + slots,))],
            compiler_params=pltpu.CompilerParams(vmem_limit_bytes=8 * 2**20),
            name="finish",
        )(*map(keep, (out, out_scales, first_new, second_new)))
    )


def solution(mesh):
    in_specs = (
        P("dp", "fsdp", None, None),
        P("fsdp", None, None),
        P("fsdp", None, None),
        P("fsdp", None, None),
        P("fsdp", None, None),
        P(),
        P(),
    )
    out_specs = (P("fsdp", None, None), P("fsdp", None, None), P("fsdp", None, None))
    return jax.shard_map(body, mesh=mesh, in_specs=in_specs, out_specs=out_specs, check_vma=False)
```

```python
import functools

import jax
import jax.numpy as jnp
from jax import lax
from jax.experimental import pallas as pl
from jax.experimental.pallas import tpu as pltpu
from jax.sharding import PartitionSpec as P

STEP = 10
BETA_ONE = 0.9
BETA_TWO = 0.95
EPSILON = 1e-08
TOP = 32766.0
ROOM = 40 * 2**20
MESH = pl.DeviceIdType.MESH
F32 = jnp.float32
BF16 = jnp.bfloat16
I16 = jnp.int16


def neighbours(devices):
    me = lax.axis_index("fsdp")
    core = lax.axis_index("dp")
    right = {"fsdp": jnp.minimum(me + 1, devices - 1)}
    left = {"fsdp": jnp.maximum(me - 1, 0)}
    twin = {"dp": 1 - core}
    return me, core, right, left, twin


def greet(me, devices, right, left, twin):
    barrier = pltpu.get_barrier_semaphore()

    def signal(peer):
        pl.semaphore_signal(barrier, inc=1, device_id=peer, device_id_type=MESH)

    signal(twin)
    pl.when(me < devices - 1)(lambda: signal(right))
    pl.when(me > 0)(lambda: signal(left))
    at_end = (me == 0) | (me == devices - 1)
    pl.when(at_end)(lambda: pl.semaphore_wait(barrier, 2))
    pl.when(~at_end)(lambda: pl.semaphore_wait(barrier, 3))


def push(src, dst, send_sem, recv_sem, peer):
    return pltpu.make_async_remote_copy(
        src_ref=src,
        dst_ref=dst,
        send_sem=send_sem,
        recv_sem=recv_sem,
        device_id=peer,
        device_id_type=MESH,
    )


def split(x):
    high = x.astype(BF16)
    return high, (x - high.astype(F32)).astype(BF16)


def dot(a, b, dims):
    return lax.dot_general(a, b, (dims, ((), ())), preferred_element_type=F32)


def dot_three(a, b, dims):
    return dot(a[0], b[0], dims) + (dot(a[0], b[1], dims) + dot(a[1], b[0], dims))


NN = ((1,), (0,))
NT = ((1,), (1,))
WAVE = 2
LATE = 4


def soap_kernel(
    devices, starts_in, owners_in, grad, moment_in, second_in, left_in, right_in, first_out, second_out, out, out_scales,
    starts, owners, table, mine, theirs, other, gathered_a, gathered_b, moment, second, left, right, lt_two, lh_two, r_high, r_low, rt_high, rt_low,
    base, update_a, update_b, scales_a, scales_b, second_late, codes, scales, far_in, far_scales, merged, merged_scales, h_two, s_high, s_low, z_two,
    load_sem, swap_sem, own_send, relay_send, ring_recv, hand_send, hand_recv, far_send, far_recv, near_send, near_recv, give_sem, scale_send, scale_recv
):
    me, core, right_peer, left_peer, twin = neighbours(devices)
    slots = grad.shape[1]
    half = grad.shape[2] // 2
    owned = moment.shape[0]
    blocks = owners.shape[0]
    rows = pl.ds(pl.multiple_of(core * half, half), half)
    other_rows = pl.ds(pl.multiple_of((1 - core) * half, half), half)
    gathered = (gathered_a, gathered_b)

    loads = [
        pltpu.make_async_copy(src, dst, load_sem.at[at])
        for at, (src, dst) in enumerate(
            (
                (grad.at[0, :, other_rows], other),
                (grad.at[0, :, rows], mine),
                (starts_in, starts),
                (owners_in, owners),
                (left_in, left),
                (moment_in, moment),
                (right_in, right),
                (second_in, second),
            )
        )
    ]
    for load in loads:
        load.start()
    greet(me, devices, right_peer, left_peer, twin)

    def swap(s):
        return push(other.at[s], theirs.at[s], swap_sem.at[0, s], swap_sem.at[1, s], twin)

    def own(w, side, t):
        source = gathered[w].at[2, t, rows] if t is not None else gathered[w].at[2, :, rows]
        target = gathered[w].at[side["near"], t, rows] if t is not None else gathered[w].at[side["near"], :, rows]
        arrived = ring_recv.at[side["at"], WAVE * w + (t or 0)]
        return push(source, target, own_send.at[side["at"], w], arrived, side["peer"])

    def relay(w, side, t):
        source = gathered[w].at[side["near"], t, rows] if t is not None else gathered[w].at[side["near"], :, rows]
        target = gathered[w].at[side["far"], t, rows] if t is not None else gathered[w].at[side["far"], :, rows]
        arrived = ring_recv.at[2 + side["at"], WAVE * w + (t or 0)]
        return push(source, target, relay_send.at[side["at"], w], arrived, side["peer"])

    def hand(w, k=None, t=None):
        part = gathered[w].at[:, :, rows] if k is None else gathered[w].at[k, t, rows]
        return push(part, part, hand_send.at[w], hand_recv.at[w], twin)

    to_right = dict(at=0, near=1, far=0, peer=right_peer, has=me >= 1, gives=me >= 2, sends=me < devices - 1, to_far=4, to_near=3)
    to_left = dict(at=1, near=3, far=4, peer=left_peer, has=me < devices - 1, gives=me < devices - 2, sends=me >= 1, to_far=0, to_near=1)
    sides = (to_right, to_left)

    def send_own(w, side, t):
        pl.when(side["sends"])(own(w, side, t).start)

    def send_on(w, side):
        for t in range(WAVE):

            @pl.when(side["has"])
            def _():
                own(w, side, t).wait_recv()

            @pl.when(side["has"] & side["sends"])
            def _():
                relay(w, side, t).start()

            hand(w, side["near"], t).start()

    loads[0].wait()
    for s in range(slots):
        swap(s).start()
    loads[1].wait()
    for w in range(2):
        for t in range(WAVE):
            s = WAVE * w + t
            swap(s).wait_recv()
            gathered[w][2, t, rows] = (mine[s].astype(F32) + theirs[s].astype(F32)).astype(BF16)
            for side in sides:
                send_own(w, side, t)
    for w in range(2):
        for t in range(WAVE):
            hand(w, 2, t).start()

    for side in sides:

        @pl.when(~side["has"])
        def _():
            far_in[side["at"]] = jnp.zeros(far_in.shape[1:], I16)
            far_scales[side["at"]] = jnp.zeros(far_scales.shape[1:], F32)
            out_scales[side["at"], core] = jnp.zeros(out_scales.shape[2:], F32)
            for s in range(slots):
                out[side["at"], s, rows] = jnp.zeros((half, out.shape[3]), I16)
                gathered[s // WAVE][side["near"], s % WAVE, rows] = jnp.zeros((half, out.shape[3]), BF16)

        @pl.when(~side["gives"])
        def _():
            for s in range(slots):
                gathered[s // WAVE][side["far"], s % WAVE, rows] = jnp.zeros((half, out.shape[3]), BF16)

    loads[2].wait()
    loads[3].wait()

    def start_of(device):
        value = starts[jnp.clip(device, 0, devices - 1)]
        return jnp.where(device < 0, -1, jnp.where(device >= devices, blocks, value))

    first = jnp.maximum(start_of(me - 2), 0)
    below = jnp.int32(0)
    for k in range(5 * slots):
        at = first + k
        owner = owners[jnp.minimum(at, blocks - 1)]
        below += jnp.where((at < blocks) & (owner < me), 1, 0)
    first = first + below
    rank = jnp.int32(0)
    chosen_late = [jnp.int32(0)] * LATE
    for j in range(owned):
        block = first + j
        live = (block < blocks) & (owners[jnp.minimum(block, blocks - 1)] == me)
        place = jnp.int32(0)
        for delta in (-1, 0, 1, 2):
            place += jnp.where(start_of(me + delta) <= block, 1, 0)
        slot = block - starts[jnp.clip(me + place - 2, 0, devices - 1)]
        late = live & (slot >= WAVE)
        table[0, j] = jnp.where(live & ~late, 1, 0)
        table[1, j] = jnp.where(late, 1, 0)
        table[2, j] = jnp.where(live, jnp.clip(place, 0, 4), 0)
        table[3, j] = jnp.where(live, jnp.clip(lax.rem(slot, WAVE), 0, WAVE - 1), 0)
        table[4, j] = rank
        for b in range(LATE):
            chosen_late[b] = jnp.where(late & (rank == b), j, chosen_late[b])
        rank = jnp.minimum(rank + jnp.where(late, 1, 0), LATE - 1)
    for b in range(LATE):
        table[5, b] = chosen_late[b]
    for k in range(5):
        holder = me + k - 2
        begin, end = start_of(holder), start_of(holder + 1)
        for s in range(slots):
            block = begin + s
            valid = (holder >= 0) & (holder < devices) & (block < end) & (owners[jnp.clip(block, 0, blocks - 1)] == me)
            table[6 + 2 * k, s] = jnp.where(valid, 1, 0)
            table[7 + 2 * k, s] = jnp.where(valid, jnp.clip(block - first, 0, owned - 1), 0)

    loads[4].wait()
    loads[5].wait()
    loads[6].wait()

    bias_one = 1.0 - BETA_ONE**STEP
    bias_two = 1.0 - BETA_TWO**STEP
    gain = bias_two**0.5 / bias_one

    def prepare(j):
        whole = left[j]
        l_two = split(whole.T)
        half_l = split(left[j, rows])
        r_two = split(right[j])
        for at in range(2):
            lt_two[j, at * whole.shape[0] : (at + 1) * whole.shape[0]] = l_two[at]
            lh_two[j, at * half : (at + 1) * half] = half_l[at]
        r_high[j], r_low[j] = r_two
        rt_high[j], rt_low[j] = split(right[j].T)
        turned = dot_three(split(dot_three(l_two, split(moment[j]), NN)), r_two, NN)
        base[j] = (BETA_ONE * gain) * turned

    @pl.loop(0, owned)
    def _(j):
        prepare(j)

    left_edge, right_edge = lax.rem(me, 4) == 0, lax.rem(me, 4) == 3

    def in_order(step):
        def each(order):
            for w, side in order:
                step(w, side)

        pl.when(left_edge)(lambda: each(((0, to_left), (1, to_left), (0, to_right), (1, to_right))))
        pl.when(right_edge)(lambda: each(((0, to_right), (1, to_right), (0, to_left), (1, to_left))))
        pl.when(~(left_edge | right_edge))(lambda: each(((0, to_right), (0, to_left), (1, to_right), (1, to_left))))

    in_order(send_on)
    loads[7].wait()

    def pass_far(w):
        for t in range(WAVE):
            for side in sides:
                pl.when(side["gives"])(relay(w, side, t).wait_recv)
                hand(w, side["far"], t).start()

    def stacked(two, b_high, b_low):
        size = two.shape[0] // 2
        full = dot(two, b_high, NN)
        return full[:size] + (full[size:] + dot(two[:size], b_low, NN))

    def stack(two, at, value):
        size = value.shape[0]
        two[at, :size], two[at, size:] = split(value)

    def solve(indices, source, second_to, update_to, scales_to, between):
        size = source.shape[2]
        for at, j in enumerate(indices):
            both = dot(lt_two[j], source[table[2, j], table[3, j]], NN)
            stack(h_two, at, both[:size] + both[size:])
        for at, j in enumerate(indices):
            turned = stacked(h_two[at], r_high[j], r_low[j])
            second_next = BETA_TWO * second[j] + ((1.0 - BETA_TWO) * turned) * turned
            second_to[at] = second_next
            scaled = (base[j] + ((1.0 - BETA_ONE) * gain) * turned) / (second_next * lax.rsqrt(second_next) + EPSILON * bias_two**0.5)
            s_high[at], s_low[at] = split(scaled)
        between()
        for at, j in enumerate(indices):
            stack(z_two, at, stacked(lh_two[j], s_high[at], s_low[at]))
        for at, j in enumerate(indices):
            new = stacked(z_two[at], rt_high[j], rt_low[j])
            largest = jnp.maximum(jnp.max(jnp.abs(new), axis=0, keepdims=True), 1e-30)
            update_to[at] = jnp.round(new * (TOP / largest)).astype(jnp.int32).astype(I16)
            scales_to[at] = largest * (1.0 / TOP)

    pass_far(0)
    hand(0).wait_recv()
    solve(range(owned), gathered_a, second_out, update_a, scales_a, lambda: pass_far(1))

    def chosen(k, s, absent):
        at = table[7 + 2 * k, s]
        value = update_a[at] if s < WAVE else update_b[table[4, at]]
        return jnp.where(table[6 + 2 * k, s] == 1, value, absent)

    def chosen_scale(k, s, absent):
        at = table[7 + 2 * k, s]
        value = scales_a[at] if s < WAVE else scales_b[table[4, at]]
        return jnp.where(table[6 + 2 * k, s] == 1, value, absent)

    def far(w, side, t):
        at = side["at"]
        part = (at, w, t) if t is not None else (at,)
        return push(codes.at[part], far_in.at[part], far_send.at[at], far_recv.at[at, WAVE * (w or 0) + (t or 0)], side["peer"])

    def far_scale(side):
        at = side["at"]
        return push(scales.at[at], far_scales.at[at], scale_send.at[at], scale_recv.at[at], side["peer"])

    def near(w, side, t):
        at = side["at"]
        part = (at, WAVE * w + t) if t is not None else (at,)
        held = (at, WAVE * w + t, rows) if t is not None else (at, slice(None), rows)
        return push(merged.at[part], out.at[held], near_send.at[at], near_recv.at[at, WAVE * (w or 0) + (t or 0)], side["peer"])

    def near_scale(side):
        at = side["at"]
        return push(merged_scales.at[at], out_scales.at[at, core], scale_send.at[2 + at], scale_recv.at[2 + at], side["peer"])

    def give(k=None, s=None):
        part = out.at[:, :, rows] if k is None else out.at[k, s, rows]
        return push(part, part, give_sem.at[0], give_sem.at[1], twin)

    def give_scale():
        part = out_scales.at[:, core]
        return push(part, part, scale_send.at[4], scale_recv.at[4], twin)

    def send_far(w):
        for t in range(WAVE):
            for side in sides:
                codes[side["at"], w, t] = chosen(side["to_far"], WAVE * w + t, jnp.zeros((), I16))
                pl.when(side["sends"])(far(w, side, t).start)
                scales[side["at"], w, pl.ds(t, 1)] = chosen_scale(side["to_far"], WAVE * w + t, 0.0)
        if w == 1:
            for side in sides:
                pl.when(side["sends"])(far_scale(side).start)
        for t in range(WAVE):
            s = WAVE * w + t
            out[2, s, rows] = chosen(2, s, jnp.zeros((), I16))
            give(2, s).start()
            out_scales[2, core, w, pl.ds(t, 1)] = chosen_scale(2, s, 0.0)

    def send_near(w, side):
        for t in range(WAVE):
            pl.when(side["has"])(far(w, side, t).wait_recv)
            merged[side["at"], WAVE * w + t] = chosen(side["to_near"], WAVE * w + t, far_in[side["at"], w, t])
            pl.when(side["sends"])(near(w, side, t).start)
        if w == 1:
            pl.when(side["has"])(far_scale(side).wait_recv)
            for s in range(slots):
                place = (side["at"], s // WAVE, pl.ds(s % WAVE, 1))
                merged_scales[place] = chosen_scale(side["to_near"], s, far_scales[place])
            pl.when(side["sends"])(near_scale(side).start)

    send_far(0)
    hand(1).wait_recv()

    solve([table[5, b] for b in range(LATE)], gathered_b, second_late, update_b, scales_b, lambda: None)

    send_far(1)
    in_order(send_near)

    @pl.loop(0, owned)
    def _(j):
        early, late = table[0, j] == 1, table[1, j] == 1
        gradient = jnp.where(late, gathered_b[table[2, j], table[3, j]].astype(F32), gathered_a[table[2, j], table[3, j]].astype(F32))
        first_out[j] = jnp.where(early | late, BETA_ONE * moment[j] + (1.0 - BETA_ONE) * gradient, 0.0)
        second_out[j] = jnp.where(late, second_late[table[4, j]], jnp.where(early, second_out[j], 0.0))

    for s in range(slots):
        for side in sides:
            pl.when(side["has"])(near(s // WAVE, side, s % WAVE).wait_recv)
            give(side["at"], s).start()
    for side in sides:
        pl.when(side["has"])(near_scale(side).wait_recv)
    give_scale().start()

    for s in range(slots):
        swap(s).wait_send()
    for w in range(2):
        hand(w).wait_send()
    for side in sides:

        @pl.when(side["sends"])
        def _():
            for w in range(2):
                own(w, side, None).wait_send()
            far(None, side, None).wait_send()
            far_scale(side).wait_send()
            near(None, side, None).wait_send()
            near_scale(side).wait_send()

        @pl.when(side["has"] & side["sends"])
        def _():
            for w in range(2):
                relay(w, side, None).wait_send()

    give().wait_send()
    give_scale().wait_send()
    give().wait_recv()
    give_scale().wait_recv()


def finish_kernel(codes, scales, first, second, direction, first_new, second_new, decoded, sem):
    slots = codes.shape[1]
    half = codes.shape[2] // 2
    copies = [pltpu.make_async_copy(first, first_new, sem.at[0]), pltpu.make_async_copy(second, second_new, sem.at[1])]
    for j in range(first.shape[0]):
        pltpu.make_async_copy(first.at[j], first_new.at[j], sem.at[0]).start()
        pltpu.make_async_copy(second.at[j], second_new.at[j], sem.at[1]).start()
    for s in range(slots):
        for core in range(2):
            rows = pl.ds(core * half, half)
            total = 0.0
            for k in range(3):
                total += codes[k, s, rows].astype(jnp.int32).astype(F32) * scales[k, core, s // WAVE, pl.ds(s % WAVE, 1)]
            decoded[s, rows] = total
        copy = pltpu.make_async_copy(decoded.at[s], direction.at[s], sem.at[2 + s])
        copy.start()
        copies.append(copy)
    for copy in copies:
        copy.wait()


def body(gradients, first_moment, second_moment, left_basis, right_basis, shard_starts, block_owners):
    devices = lax.axis_size("fsdp")
    slots = gradients.shape[1]
    owned, width = first_moment.shape[0], first_moment.shape[1]
    half = width // 2
    any_space = pl.BlockSpec(memory_space=pl.ANY)
    in_vmem = pl.BlockSpec(memory_space=pltpu.VMEM)
    dma = pltpu.SemaphoreType.DMA
    keep = functools.partial(pltpu.with_memory_space_constraint, memory_space=pltpu.VMEM)
    stay = functools.partial(pltpu.with_memory_space_constraint, memory_space=pltpu.HBM)
    matrices = (owned, width, width)
    halves = (owned, half, width)
    first_new, second_new, out, out_scales = pl.pallas_call(
        functools.partial(soap_kernel, devices),
        out_shape=[
            pltpu.VMEM(matrices, F32),
            pltpu.VMEM(matrices, F32),
            pltpu.VMEM((3, slots, width, width), I16),
            pltpu.VMEM((3, 2, 2, WAVE, width), F32),
        ],
        in_specs=[any_space] * 7,
        out_specs=[in_vmem] * 4,
        scratch_shapes=[
            pltpu.SMEM(shard_starts.shape, jnp.int32),
            pltpu.SMEM(block_owners.shape, jnp.int32),
            pltpu.SMEM((16, 8), jnp.int32),
            *[pltpu.VMEM((slots, half, width), BF16)] * 3,
            *[pltpu.VMEM((5, WAVE, width, width), BF16)] * 2,
            *[pltpu.VMEM(matrices, F32)] * 4,
            pltpu.VMEM((owned, 2 * width, width), BF16),
            pltpu.VMEM((owned, width, width), BF16),
            *[pltpu.VMEM(matrices, BF16)] * 4,
            pltpu.VMEM(matrices, F32),
            pltpu.VMEM(halves, I16),
            pltpu.VMEM((LATE, half, width), I16),
            pltpu.VMEM((owned, 1, width), F32),
            pltpu.VMEM((LATE, 1, width), F32),
            pltpu.VMEM((LATE, width, width), F32),
            *[pltpu.VMEM((2, 2, WAVE, half, width), I16), pltpu.VMEM((2, 2, WAVE, width), F32)] * 2,
            pltpu.VMEM((2, slots, half, width), I16),
            pltpu.VMEM((2, 2, WAVE, width), F32),
            pltpu.VMEM((owned, 2 * width, width), BF16),
            *[pltpu.VMEM(matrices, BF16)] * 2,
            pltpu.VMEM((owned, width, width), BF16),
            dma((8,)), dma((2, slots)), *[dma((2, 2))] * 2, dma((4, slots)), *[dma((2,))] * 2,
            *[dma((2,)), dma((2, slots))] * 2, dma((2,)), *[dma((5,))] * 2,
        ],
        compiler_params=pltpu.CompilerParams(collective_id=0, has_side_effects=True, vmem_limit_bytes=ROOM),
        name="soap",
    )(*map(stay, (shard_starts, block_owners, gradients, first_moment, second_moment, left_basis, right_basis)))

    return tuple(
        pl.pallas_call(
            finish_kernel,
            out_shape=[
                jax.ShapeDtypeStruct((slots, width, width), F32),
                jax.ShapeDtypeStruct(matrices, F32),
                jax.ShapeDtypeStruct(matrices, F32),
            ],
            in_specs=[in_vmem] * 4,
            out_specs=[any_space] * 3,
            scratch_shapes=[pltpu.VMEM((slots, width, width), F32), dma((2 + slots,))],
            compiler_params=pltpu.CompilerParams(vmem_limit_bytes=8 * 2**20),
            name="finish",
        )(*map(keep, (out, out_scales, first_new, second_new)))
    )


def solution(mesh):
    in_specs = (
        P("dp", "fsdp", None, None),
        P("fsdp", None, None),
        P("fsdp", None, None),
        P("fsdp", None, None),
        P("fsdp", None, None),
        P(),
        P(),
    )
    out_specs = (P("fsdp", None, None), P("fsdp", None, None), P("fsdp", None, None))
    return jax.shard_map(body, mesh=mesh, in_specs=in_specs, out_specs=out_specs, check_vma=False)
```

```python
import functools

import jax
import jax.numpy as jnp
from jax import lax
from jax.experimental import pallas as pl
from jax.experimental.pallas import tpu as pltpu
from jax.sharding import PartitionSpec as P

STEP = 10
BETA_ONE = 0.9
BETA_TWO = 0.95
EPSILON = 1e-08
TOP = 32766.0
ROOM = 40 * 2**20
MESH = pl.DeviceIdType.MESH
F32 = jnp.float32
BF16 = jnp.bfloat16
I16 = jnp.int16


def neighbours(devices):
    me = lax.axis_index("fsdp")
    core = lax.axis_index("dp")
    right = {"fsdp": jnp.minimum(me + 1, devices - 1)}
    left = {"fsdp": jnp.maximum(me - 1, 0)}
    twin = {"dp": 1 - core}
    return me, core, right, left, twin


def greet(me, devices, right, left, twin):
    barrier = pltpu.get_barrier_semaphore()

    def signal(peer):
        pl.semaphore_signal(barrier, inc=1, device_id=peer, device_id_type=MESH)

    signal(twin)
    pl.when(me < devices - 1)(lambda: signal(right))
    pl.when(me > 0)(lambda: signal(left))
    at_end = (me == 0) | (me == devices - 1)
    pl.when(at_end)(lambda: pl.semaphore_wait(barrier, 2))
    pl.when(~at_end)(lambda: pl.semaphore_wait(barrier, 3))


def push(src, dst, send_sem, recv_sem, peer):
    return pltpu.make_async_remote_copy(
        src_ref=src,
        dst_ref=dst,
        send_sem=send_sem,
        recv_sem=recv_sem,
        device_id=peer,
        device_id_type=MESH,
    )


def split(x):
    high = x.astype(BF16)
    return high, (x - high.astype(F32)).astype(BF16)


def dot(a, b, dims):
    return lax.dot_general(a, b, (dims, ((), ())), preferred_element_type=F32)


def dot_three(a, b, dims):
    return dot(a[0], b[0], dims) + (dot(a[0], b[1], dims) + dot(a[1], b[0], dims))


NN = ((1,), (0,))
NT = ((1,), (1,))
WAVE = 2
LATE = 4


def soap_kernel(
    devices, starts_in, owners_in, grad, moment_in, second_in, left_in, right_in, first_out, second_out, out, out_scales,
    starts, owners, table, mine, theirs, other, gathered_a, gathered_b, moment, second, left, right, lt_two, lh_two, r_high, r_low, rt_high, rt_low,
    base, update_a, update_b, scales_a, scales_b, second_late, codes, scales, far_in, far_scales, merged, merged_scales, h_two, s_high, s_low, z_two,
    load_sem, swap_sem, own_send, relay_send, ring_recv, hand_send, hand_recv, far_send, far_recv, near_send, near_recv, give_sem, scale_send, scale_recv
):
    me, core, right_peer, left_peer, twin = neighbours(devices)
    slots = grad.shape[1]
    half = grad.shape[2] // 2
    owned = moment.shape[0]
    blocks = owners.shape[0]
    rows = pl.ds(pl.multiple_of(core * half, half), half)
    other_rows = pl.ds(pl.multiple_of((1 - core) * half, half), half)
    gathered = (gathered_a, gathered_b)

    loads = [
        pltpu.make_async_copy(src, dst, load_sem.at[at])
        for at, (src, dst) in enumerate(
            (
                (grad.at[0, :, other_rows], other),
                (grad.at[0, :, rows], mine),
                (starts_in, starts),
                (owners_in, owners),
                (left_in, left),
                (moment_in, moment),
                (right_in, right),
                (second_in, second),
            )
        )
    ]
    for load in loads:
        load.start()
    greet(me, devices, right_peer, left_peer, twin)

    def swap(s):
        return push(other.at[s], theirs.at[s], swap_sem.at[0, s], swap_sem.at[1, s], twin)

    def own(w, side, t):
        source = gathered[w].at[2, t, rows] if t is not None else gathered[w].at[2, :, rows]
        target = gathered[w].at[side["near"], t, rows] if t is not None else gathered[w].at[side["near"], :, rows]
        arrived = ring_recv.at[side["at"], WAVE * w + (t or 0)]
        return push(source, target, own_send.at[side["at"], w], arrived, side["peer"])

    def relay(w, side, t):
        source = gathered[w].at[side["near"], t, rows] if t is not None else gathered[w].at[side["near"], :, rows]
        target = gathered[w].at[side["far"], t, rows] if t is not None else gathered[w].at[side["far"], :, rows]
        arrived = ring_recv.at[2 + side["at"], WAVE * w + (t or 0)]
        return push(source, target, relay_send.at[side["at"], w], arrived, side["peer"])

    def hand(w, k=None, t=None):
        part = gathered[w].at[:, :, rows] if k is None else gathered[w].at[k, t, rows]
        return push(part, part, hand_send.at[w], hand_recv.at[w], twin)

    to_right = dict(at=0, near=1, far=0, peer=right_peer, has=me >= 1, gives=me >= 2, sends=me < devices - 1, to_far=4, to_near=3)
    to_left = dict(at=1, near=3, far=4, peer=left_peer, has=me < devices - 1, gives=me < devices - 2, sends=me >= 1, to_far=0, to_near=1)
    sides = (to_right, to_left)

    def send_own(w, side, t):
        pl.when(side["sends"])(own(w, side, t).start)

    def send_on(w, side, places=range(WAVE)):
        for t in places:

            @pl.when(side["has"])
            def _():
                own(w, side, t).wait_recv()

            @pl.when(side["has"] & side["sends"])
            def _():
                relay(w, side, t).start()

            hand(w, side["near"], t).start()

    left_edge, right_edge = lax.rem(me, 4) == 0, lax.rem(me, 4) == 3
    z_edge = (lax.rem(me, 16) == 0) | (lax.rem(me, 16) == 15)
    after_edge = (lax.rem(me, 16) == 1) | (lax.rem(me, 16) == 14)
    to_right["late"] = left_edge | (lax.rem(me, 16) == 1)
    to_left["late"] = right_edge | (lax.rem(me, 16) == 14)

    loads[0].wait()
    for s in range(slots):
        swap(s).start()
    loads[1].wait()
    for w in range(2):
        for t in range(WAVE):
            s = WAVE * w + t
            swap(s).wait_recv()
            gathered[w][2, t, rows] = (mine[s].astype(F32) + theirs[s].astype(F32)).astype(BF16)
            for side in sides:
                if w == 0:
                    send_own(w, side, t)
                elif t == 0:
                    pl.when(side["late"] | ~z_edge)(functools.partial(send_own, w, side, t))
                else:
                    pl.when(side["late"])(functools.partial(send_own, w, side, t))
    for w in range(2):
        for t in range(WAVE):
            hand(w, 2, t).start()

    for side in sides:

        @pl.when(~side["has"])
        def _():
            far_in[side["at"]] = jnp.zeros(far_in.shape[1:], I16)
            far_scales[side["at"]] = jnp.zeros(far_scales.shape[1:], F32)
            out_scales[side["at"], core] = jnp.zeros(out_scales.shape[2:], F32)
            for s in range(slots):
                out[side["at"], s, rows] = jnp.zeros((half, out.shape[3]), I16)
                gathered[s // WAVE][side["near"], s % WAVE, rows] = jnp.zeros((half, out.shape[3]), BF16)

        @pl.when(~side["gives"])
        def _():
            for s in range(slots):
                gathered[s // WAVE][side["far"], s % WAVE, rows] = jnp.zeros((half, out.shape[3]), BF16)

    loads[2].wait()
    loads[3].wait()

    def start_of(device):
        value = starts[jnp.clip(device, 0, devices - 1)]
        return jnp.where(device < 0, -1, jnp.where(device >= devices, blocks, value))

    first = jnp.maximum(start_of(me - 2), 0)
    below = jnp.int32(0)
    for k in range(5 * slots):
        at = first + k
        owner = owners[jnp.minimum(at, blocks - 1)]
        below += jnp.where((at < blocks) & (owner < me), 1, 0)
    first = first + below
    rank = jnp.int32(0)
    chosen_late = [jnp.int32(0)] * LATE
    for j in range(owned):
        block = first + j
        live = (block < blocks) & (owners[jnp.minimum(block, blocks - 1)] == me)
        place = jnp.int32(0)
        for delta in (-1, 0, 1, 2):
            place += jnp.where(start_of(me + delta) <= block, 1, 0)
        slot = block - starts[jnp.clip(me + place - 2, 0, devices - 1)]
        late = live & (slot >= WAVE)
        table[0, j] = jnp.where(live & ~late, 1, 0)
        table[1, j] = jnp.where(late, 1, 0)
        table[2, j] = jnp.where(live, jnp.clip(place, 0, 4), 0)
        table[3, j] = jnp.where(live, jnp.clip(lax.rem(slot, WAVE), 0, WAVE - 1), 0)
        table[4, j] = rank
        for b in range(LATE):
            chosen_late[b] = jnp.where(late & (rank == b), j, chosen_late[b])
        rank = jnp.minimum(rank + jnp.where(late, 1, 0), LATE - 1)
    for b in range(LATE):
        table[5, b] = chosen_late[b]
    for k in range(5):
        holder = me + k - 2
        begin, end = start_of(holder), start_of(holder + 1)
        for s in range(slots):
            block = begin + s
            valid = (holder >= 0) & (holder < devices) & (block < end) & (owners[jnp.clip(block, 0, blocks - 1)] == me)
            table[6 + 2 * k, s] = jnp.where(valid, 1, 0)
            table[7 + 2 * k, s] = jnp.where(valid, jnp.clip(block - first, 0, owned - 1), 0)

    loads[4].wait()
    loads[5].wait()
    loads[6].wait()

    bias_one = 1.0 - BETA_ONE**STEP
    bias_two = 1.0 - BETA_TWO**STEP
    gain = bias_two**0.5 / bias_one

    def prepare(j):
        whole = left[j]
        l_two = split(whole.T)
        half_l = split(left[j, rows])
        r_two = split(right[j])
        for at in range(2):
            lt_two[j, at * whole.shape[0] : (at + 1) * whole.shape[0]] = l_two[at]
            lh_two[j, at * half : (at + 1) * half] = half_l[at]
        r_high[j], r_low[j] = r_two
        rt_high[j], rt_low[j] = split(right[j].T)
        turned = dot_three(split(dot_three(l_two, split(moment[j]), NN)), r_two, NN)
        base[j] = (BETA_ONE * gain) * turned

    @pl.loop(0, owned // 2)
    def _(j):
        prepare(j)

    for side in sides:

        @pl.when(~side["late"])
        def _():
            send_on(0, side)
            pl.when(z_edge)(functools.partial(send_own, 1, side, 0))
            send_own(1, side, 1)

    @pl.loop(owned // 2, owned)
    def _(j):
        prepare(j)

    for side in sides:

        @pl.when(side["late"])
        def _():
            send_on(0, side)

    def send_on_late_wave(late, places, where):
        for side in sides:

            @pl.when((side["late"] == late) & where)
            def _():
                send_on(1, side, places)

    send_on_late_wave(False, (0,), me >= 0)
    send_on_late_wave(False, (1,), z_edge)
    send_on_late_wave(True, (0, 1), after_edge)

    def pass_far(w):
        for t in range(WAVE):
            for side in sides:
                pl.when(side["gives"])(relay(w, side, t).wait_recv)
                hand(w, side["far"], t).start()

    def stacked(two, b_high, b_low):
        size = two.shape[0] // 2
        full = dot(two, b_high, NN)
        return full[:size] + (full[size:] + dot(two[:size], b_low, NN))

    def stack(two, at, value):
        size = value.shape[0]
        two[at, :size], two[at, size:] = split(value)

    def solve(indices, source, second_to, update_to, scales_to, between):
        size = source.shape[2]
        for at, j in enumerate(indices):
            both = dot(lt_two[j], source[table[2, j], table[3, j]], NN)
            stack(h_two, at, both[:size] + both[size:])
        for at, j in enumerate(indices):
            turned = stacked(h_two[at], r_high[j], r_low[j])
            second_next = BETA_TWO * second[j] + ((1.0 - BETA_TWO) * turned) * turned
            second_to[at] = second_next
            scaled = (base[j] + ((1.0 - BETA_ONE) * gain) * turned) / (second_next * lax.rsqrt(second_next) + EPSILON * bias_two**0.5)
            s_high[at], s_low[at] = split(scaled)
        between()
        for at, j in enumerate(indices):
            stack(z_two, at, stacked(lh_two[j], s_high[at], s_low[at]))
        for at, j in enumerate(indices):
            new = stacked(z_two[at], rt_high[j], rt_low[j])
            largest = jnp.maximum(jnp.max(jnp.abs(new), axis=0, keepdims=True), 1e-30)
            update_to[at] = jnp.round(new * (TOP / largest)).astype(jnp.int32).astype(I16)
            scales_to[at] = largest * (1.0 / TOP)

    loads[7].wait()
    pass_far(0)
    send_on_late_wave(False, (1,), ~z_edge)
    send_on_late_wave(True, (0,), ~after_edge)
    hand(0).wait_recv()
    solve(range(owned), gathered_a, second_out, update_a, scales_a, lambda: send_on_late_wave(True, (1,), ~after_edge))

    def chosen(k, s, absent):
        at = table[7 + 2 * k, s]
        value = update_a[at] if s < WAVE else update_b[table[4, at]]
        return jnp.where(table[6 + 2 * k, s] == 1, value, absent)

    def chosen_scale(k, s, absent):
        at = table[7 + 2 * k, s]
        value = scales_a[at] if s < WAVE else scales_b[table[4, at]]
        return jnp.where(table[6 + 2 * k, s] == 1, value, absent)

    def far(w, side, t):
        at = side["at"]
        part = (at, w, t) if t is not None else (at,)
        return push(codes.at[part], far_in.at[part], far_send.at[at], far_recv.at[at, WAVE * (w or 0) + (t or 0)], side["peer"])

    def far_scale(side):
        at = side["at"]
        return push(scales.at[at], far_scales.at[at], scale_send.at[at], scale_recv.at[at], side["peer"])

    def near(w, side, t):
        at = side["at"]
        part = (at, WAVE * w + t) if t is not None else (at,)
        held = (at, WAVE * w + t, rows) if t is not None else (at, slice(None), rows)
        return push(merged.at[part], out.at[held], near_send.at[at], near_recv.at[at, WAVE * (w or 0) + (t or 0)], side["peer"])

    def near_scale(side):
        at = side["at"]
        return push(merged_scales.at[at], out_scales.at[at, core], scale_send.at[2 + at], scale_recv.at[2 + at], side["peer"])

    def give(k=None, s=None):
        part = out.at[:, :, rows] if k is None else out.at[k, s, rows]
        return push(part, part, give_sem.at[0], give_sem.at[1], twin)

    def give_scale():
        part = out_scales.at[:, core]
        return push(part, part, scale_send.at[4], scale_recv.at[4], twin)

    def send_far(w):
        for t in range(WAVE):
            for side in sides:
                codes[side["at"], w, t] = chosen(side["to_far"], WAVE * w + t, jnp.zeros((), I16))
                pl.when(side["sends"])(far(w, side, t).start)
                scales[side["at"], w, pl.ds(t, 1)] = chosen_scale(side["to_far"], WAVE * w + t, 0.0)
        if w == 1:
            for side in sides:
                pl.when(side["sends"])(far_scale(side).start)
        for t in range(WAVE):
            s = WAVE * w + t
            out[2, s, rows] = chosen(2, s, jnp.zeros((), I16))
            give(2, s).start()
            out_scales[2, core, w, pl.ds(t, 1)] = chosen_scale(2, s, 0.0)

    def send_near(w, side):
        for t in range(WAVE):
            pl.when(side["has"])(far(w, side, t).wait_recv)
            merged[side["at"], WAVE * w + t] = chosen(side["to_near"], WAVE * w + t, far_in[side["at"], w, t])
            pl.when(side["sends"])(near(w, side, t).start)
        if w == 1:
            pl.when(side["has"])(far_scale(side).wait_recv)
            for s in range(slots):
                place = (side["at"], s // WAVE, pl.ds(s % WAVE, 1))
                merged_scales[place] = chosen_scale(side["to_near"], s, far_scales[place])
            pl.when(side["sends"])(near_scale(side).start)

    send_far(0)
    pass_far(1)
    hand(1).wait_recv()

    solve([table[5, b] for b in range(LATE)], gathered_b, second_late, update_b, scales_b, lambda: None)

    send_far(1)
    def each(order):
        for w, side in order:
            send_near(w, side)

    pl.when(left_edge)(lambda: each(((0, to_left), (1, to_left), (0, to_right), (1, to_right))))
    pl.when(right_edge)(lambda: each(((0, to_right), (1, to_right), (0, to_left), (1, to_left))))
    pl.when(~(left_edge | right_edge))(lambda: each(((0, to_right), (0, to_left), (1, to_right), (1, to_left))))

    @pl.loop(0, owned)
    def _(j):
        early, late = table[0, j] == 1, table[1, j] == 1
        gradient = jnp.where(late, gathered_b[table[2, j], table[3, j]].astype(F32), gathered_a[table[2, j], table[3, j]].astype(F32))
        first_out[j] = jnp.where(early | late, BETA_ONE * moment[j] + (1.0 - BETA_ONE) * gradient, 0.0)
        second_out[j] = jnp.where(late, second_late[table[4, j]], jnp.where(early, second_out[j], 0.0))

    for s in range(slots):
        for side in sides:
            pl.when(side["has"])(near(s // WAVE, side, s % WAVE).wait_recv)
            give(side["at"], s).start()
    for side in sides:
        pl.when(side["has"])(near_scale(side).wait_recv)
    give_scale().start()

    for s in range(slots):
        swap(s).wait_send()
    for w in range(2):
        hand(w).wait_send()
    for side in sides:

        @pl.when(side["sends"])
        def _():
            for w in range(2):
                own(w, side, None).wait_send()
            far(None, side, None).wait_send()
            far_scale(side).wait_send()
            near(None, side, None).wait_send()
            near_scale(side).wait_send()

        @pl.when(side["has"] & side["sends"])
        def _():
            for w in range(2):
                relay(w, side, None).wait_send()

    give().wait_send()
    give_scale().wait_send()
    give().wait_recv()
    give_scale().wait_recv()


def finish_kernel(codes, scales, first, second, direction, first_new, second_new, decoded, sem):
    slots = codes.shape[1]
    half = codes.shape[2] // 2
    copies = [pltpu.make_async_copy(first, first_new, sem.at[0]), pltpu.make_async_copy(second, second_new, sem.at[1])]
    for j in range(first.shape[0]):
        pltpu.make_async_copy(first.at[j], first_new.at[j], sem.at[0]).start()
        pltpu.make_async_copy(second.at[j], second_new.at[j], sem.at[1]).start()
    for s in range(slots):
        for core in range(2):
            rows = pl.ds(core * half, half)
            total = 0.0
            for k in range(3):
                total += codes[k, s, rows].astype(jnp.int32).astype(F32) * scales[k, core, s // WAVE, pl.ds(s % WAVE, 1)]
            decoded[s, rows] = total
        copy = pltpu.make_async_copy(decoded.at[s], direction.at[s], sem.at[2 + s])
        copy.start()
        copies.append(copy)
    for copy in copies:
        copy.wait()


def body(gradients, first_moment, second_moment, left_basis, right_basis, shard_starts, block_owners):
    devices = lax.axis_size("fsdp")
    slots = gradients.shape[1]
    owned, width = first_moment.shape[0], first_moment.shape[1]
    half = width // 2
    any_space = pl.BlockSpec(memory_space=pl.ANY)
    in_vmem = pl.BlockSpec(memory_space=pltpu.VMEM)
    dma = pltpu.SemaphoreType.DMA
    keep = functools.partial(pltpu.with_memory_space_constraint, memory_space=pltpu.VMEM)
    stay = functools.partial(pltpu.with_memory_space_constraint, memory_space=pltpu.HBM)
    matrices = (owned, width, width)
    halves = (owned, half, width)
    first_new, second_new, out, out_scales = pl.pallas_call(
        functools.partial(soap_kernel, devices),
        out_shape=[
            pltpu.VMEM(matrices, F32),
            pltpu.VMEM(matrices, F32),
            pltpu.VMEM((3, slots, width, width), I16),
            pltpu.VMEM((3, 2, 2, WAVE, width), F32),
        ],
        in_specs=[any_space] * 7,
        out_specs=[in_vmem] * 4,
        scratch_shapes=[
            pltpu.SMEM(shard_starts.shape, jnp.int32),
            pltpu.SMEM(block_owners.shape, jnp.int32),
            pltpu.SMEM((16, 8), jnp.int32),
            *[pltpu.VMEM((slots, half, width), BF16)] * 3,
            *[pltpu.VMEM((5, WAVE, width, width), BF16)] * 2,
            *[pltpu.VMEM(matrices, F32)] * 4,
            pltpu.VMEM((owned, 2 * width, width), BF16),
            pltpu.VMEM((owned, width, width), BF16),
            *[pltpu.VMEM(matrices, BF16)] * 4,
            pltpu.VMEM(matrices, F32),
            pltpu.VMEM(halves, I16),
            pltpu.VMEM((LATE, half, width), I16),
            pltpu.VMEM((owned, 1, width), F32),
            pltpu.VMEM((LATE, 1, width), F32),
            pltpu.VMEM((LATE, width, width), F32),
            *[pltpu.VMEM((2, 2, WAVE, half, width), I16), pltpu.VMEM((2, 2, WAVE, width), F32)] * 2,
            pltpu.VMEM((2, slots, half, width), I16),
            pltpu.VMEM((2, 2, WAVE, width), F32),
            pltpu.VMEM((owned, 2 * width, width), BF16),
            *[pltpu.VMEM(matrices, BF16)] * 2,
            pltpu.VMEM((owned, width, width), BF16),
            dma((8,)), dma((2, slots)), *[dma((2, 2))] * 2, dma((4, slots)), *[dma((2,))] * 2,
            *[dma((2,)), dma((2, slots))] * 2, dma((2,)), *[dma((5,))] * 2,
        ],
        compiler_params=pltpu.CompilerParams(collective_id=0, has_side_effects=True, vmem_limit_bytes=ROOM),
        name="soap",
    )(*map(stay, (shard_starts, block_owners, gradients, first_moment, second_moment, left_basis, right_basis)))

    return tuple(
        pl.pallas_call(
            finish_kernel,
            out_shape=[
                jax.ShapeDtypeStruct((slots, width, width), F32),
                jax.ShapeDtypeStruct(matrices, F32),
                jax.ShapeDtypeStruct(matrices, F32),
            ],
            in_specs=[in_vmem] * 4,
            out_specs=[any_space] * 3,
            scratch_shapes=[pltpu.VMEM((slots, width, width), F32), dma((2 + slots,))],
            compiler_params=pltpu.CompilerParams(vmem_limit_bytes=8 * 2**20),
            name="finish",
        )(*map(keep, (out, out_scales, first_new, second_new)))
    )


def solution(mesh):
    in_specs = (
        P("dp", "fsdp", None, None),
        P("fsdp", None, None),
        P("fsdp", None, None),
        P("fsdp", None, None),
        P("fsdp", None, None),
        P(),
        P(),
    )
    out_specs = (P("fsdp", None, None), P("fsdp", None, None), P("fsdp", None, None))
    return jax.shard_map(body, mesh=mesh, in_specs=in_specs, out_specs=out_specs, check_vma=False)
```

```python
import functools

import jax
import jax.numpy as jnp
from jax import lax
from jax.experimental import pallas as pl
from jax.experimental.pallas import tpu as pltpu
from jax.sharding import PartitionSpec as P

STEP = 10
BETA_ONE = 0.9
BETA_TWO = 0.95
EPSILON = 1e-08
TOP = 32766.0
ROOM = 40 * 2**20
MESH = pl.DeviceIdType.MESH
F32 = jnp.float32
BF16 = jnp.bfloat16
I16 = jnp.int16


def neighbours(devices):
    me = lax.axis_index("fsdp")
    core = lax.axis_index("dp")
    right = {"fsdp": jnp.minimum(me + 1, devices - 1)}
    left = {"fsdp": jnp.maximum(me - 1, 0)}
    twin = {"dp": 1 - core}
    return me, core, right, left, twin


def greet(me, devices, right, left, twin):
    barrier = pltpu.get_barrier_semaphore()

    def signal(peer):
        pl.semaphore_signal(barrier, inc=1, device_id=peer, device_id_type=MESH)

    signal(twin)
    pl.when(me < devices - 1)(lambda: signal(right))
    pl.when(me > 0)(lambda: signal(left))
    at_end = (me == 0) | (me == devices - 1)
    pl.when(at_end)(lambda: pl.semaphore_wait(barrier, 2))
    pl.when(~at_end)(lambda: pl.semaphore_wait(barrier, 3))


def push(src, dst, send_sem, recv_sem, peer):
    return pltpu.make_async_remote_copy(
        src_ref=src,
        dst_ref=dst,
        send_sem=send_sem,
        recv_sem=recv_sem,
        device_id=peer,
        device_id_type=MESH,
    )


def split(x):
    high = x.astype(BF16)
    return high, (x - high.astype(F32)).astype(BF16)


def dot(a, b, dims):
    return lax.dot_general(a, b, (dims, ((), ())), preferred_element_type=F32)


def dot_three(a, b, dims):
    return dot(a[0], b[0], dims) + (dot(a[0], b[1], dims) + dot(a[1], b[0], dims))


NN = ((1,), (0,))
NT = ((1,), (1,))
WAVE = 2
LATE = 4


def soap_kernel(
    devices, starts_in, owners_in, grad, moment_in, second_in, left_in, right_in, first_out, second_out, out, out_scales,
    starts, owners, table, mine, theirs, other, gathered_a, gathered_b, moment, second, left, right, lt_two, lh_two, r_high, r_low, rt_high, rt_low,
    base, update_a, update_b, scales_a, scales_b, second_late, codes, scales, far_in, far_scales, merged, merged_scales, h_two, s_high, s_low, z_two,
    load_sem, swap_sem, own_send, relay_send, ring_recv, hand_send, hand_recv, far_send, far_recv, near_send, near_recv, give_sem, scale_send, scale_recv
):
    me, core, right_peer, left_peer, twin = neighbours(devices)
    slots = grad.shape[1]
    half = grad.shape[2] // 2
    owned = moment.shape[0]
    blocks = owners.shape[0]
    rows = pl.ds(pl.multiple_of(core * half, half), half)
    other_rows = pl.ds(pl.multiple_of((1 - core) * half, half), half)
    gathered = (gathered_a, gathered_b)

    loads = [
        pltpu.make_async_copy(src, dst, load_sem.at[at])
        for at, (src, dst) in enumerate(
            (
                (grad.at[0, :, other_rows], other),
                (grad.at[0, :, rows], mine),
                (starts_in, starts),
                (owners_in, owners),
                (left_in, left),
                (moment_in, moment),
                (right_in, right),
                (second_in, second),
            )
        )
    ]
    for load in loads:
        load.start()
    greet(me, devices, right_peer, left_peer, twin)

    def swap(s):
        return push(other.at[s], theirs.at[s], swap_sem.at[0, s], swap_sem.at[1, s], twin)

    def own(w, side, t):
        source = gathered[w].at[2, t, rows] if t is not None else gathered[w].at[2, :, rows]
        target = gathered[w].at[side["near"], t, rows] if t is not None else gathered[w].at[side["near"], :, rows]
        arrived = ring_recv.at[side["at"], WAVE * w + (t or 0)]
        return push(source, target, own_send.at[side["at"], w], arrived, side["peer"])

    def relay(w, side, t):
        source = gathered[w].at[side["near"], t, rows] if t is not None else gathered[w].at[side["near"], :, rows]
        target = gathered[w].at[side["far"], t, rows] if t is not None else gathered[w].at[side["far"], :, rows]
        arrived = ring_recv.at[2 + side["at"], WAVE * w + (t or 0)]
        return push(source, target, relay_send.at[side["at"], w], arrived, side["peer"])

    def hand(w, k=None, t=None):
        part = gathered[w].at[:, :, rows] if k is None else gathered[w].at[k, t, rows]
        return push(part, part, hand_send.at[w], hand_recv.at[w], twin)

    to_right = dict(at=0, near=1, far=0, peer=right_peer, has=me >= 1, gives=me >= 2, sends=me < devices - 1, to_far=4, to_near=3)
    to_left = dict(at=1, near=3, far=4, peer=left_peer, has=me < devices - 1, gives=me < devices - 2, sends=me >= 1, to_far=0, to_near=1)
    sides = (to_right, to_left)

    def send_own(w, side, t):
        pl.when(side["sends"])(own(w, side, t).start)

    def send_on(w, side, places=range(WAVE)):
        for t in places:

            @pl.when(side["has"])
            def _():
                own(w, side, t).wait_recv()

            @pl.when(side["has"] & side["sends"])
            def _():
                relay(w, side, t).start()

            hand(w, side["near"], t).start()

    left_edge, right_edge = lax.rem(me, 4) == 0, lax.rem(me, 4) == 3
    z_edge = (lax.rem(me, 16) == 0) | (lax.rem(me, 16) == 15)
    after_edge = (lax.rem(me, 16) == 1) | (lax.rem(me, 16) == 14)
    to_right["late"] = left_edge | (lax.rem(me, 16) == 1)
    to_left["late"] = right_edge | (lax.rem(me, 16) == 14)

    loads[0].wait()
    for s in range(slots):
        swap(s).start()
    loads[1].wait()
    for w in range(2):
        for t in range(WAVE):
            s = WAVE * w + t
            swap(s).wait_recv()
            gathered[w][2, t, rows] = (mine[s].astype(F32) + theirs[s].astype(F32)).astype(BF16)
            for side in sides:
                if w == 0:
                    send_own(w, side, t)
                elif t == 0:
                    pl.when(side["late"] | ~z_edge)(functools.partial(send_own, w, side, t))
                else:
                    pl.when(side["late"])(functools.partial(send_own, w, side, t))
    for w in range(2):
        for t in range(WAVE):
            hand(w, 2, t).start()

    for side in sides:

        @pl.when(~side["has"])
        def _():
            far_in[side["at"]] = jnp.zeros(far_in.shape[1:], I16)
            far_scales[side["at"]] = jnp.zeros(far_scales.shape[1:], F32)
            out_scales[side["at"], core] = jnp.zeros(out_scales.shape[2:], F32)
            for s in range(slots):
                out[side["at"], s, rows] = jnp.zeros((half, out.shape[3]), I16)
                gathered[s // WAVE][side["near"], s % WAVE, rows] = jnp.zeros((half, out.shape[3]), BF16)

        @pl.when(~side["gives"])
        def _():
            for s in range(slots):
                gathered[s // WAVE][side["far"], s % WAVE, rows] = jnp.zeros((half, out.shape[3]), BF16)

    loads[2].wait()
    loads[3].wait()

    def start_of(device):
        value = starts[jnp.clip(device, 0, devices - 1)]
        return jnp.where(device < 0, -1, jnp.where(device >= devices, blocks, value))

    first = jnp.maximum(start_of(me - 2), 0)
    below = jnp.int32(0)
    for k in range(5 * slots):
        at = first + k
        owner = owners[jnp.minimum(at, blocks - 1)]
        below += jnp.where((at < blocks) & (owner < me), 1, 0)
    first = first + below
    rank = jnp.int32(0)
    chosen_late = [jnp.int32(0)] * LATE
    for j in range(owned):
        block = first + j
        live = (block < blocks) & (owners[jnp.minimum(block, blocks - 1)] == me)
        place = jnp.int32(0)
        for delta in (-1, 0, 1, 2):
            place += jnp.where(start_of(me + delta) <= block, 1, 0)
        slot = block - starts[jnp.clip(me + place - 2, 0, devices - 1)]
        late = live & (slot >= WAVE)
        table[0, j] = jnp.where(live & ~late, 1, 0)
        table[1, j] = jnp.where(late, 1, 0)
        table[2, j] = jnp.where(live, jnp.clip(place, 0, 4), 0)
        table[3, j] = jnp.where(live, jnp.clip(lax.rem(slot, WAVE), 0, WAVE - 1), 0)
        table[4, j] = rank
        for b in range(LATE):
            chosen_late[b] = jnp.where(late & (rank == b), j, chosen_late[b])
        rank = jnp.minimum(rank + jnp.where(late, 1, 0), LATE - 1)
    for b in range(LATE):
        table[5, b] = chosen_late[b]
    for k in range(5):
        holder = me + k - 2
        begin, end = start_of(holder), start_of(holder + 1)
        for s in range(slots):
            block = begin + s
            valid = (holder >= 0) & (holder < devices) & (block < end) & (owners[jnp.clip(block, 0, blocks - 1)] == me)
            table[6 + 2 * k, s] = jnp.where(valid, 1, 0)
            table[7 + 2 * k, s] = jnp.where(valid, jnp.clip(block - first, 0, owned - 1), 0)

    loads[4].wait()
    loads[5].wait()
    loads[6].wait()

    bias_one = 1.0 - BETA_ONE**STEP
    bias_two = 1.0 - BETA_TWO**STEP
    gain = bias_two**0.5 / bias_one

    def prepare(j):
        whole = left[j]
        l_two = split(whole.T)
        half_l = split(left[j, rows])
        r_two = split(right[j])
        for at in range(2):
            lt_two[j, at * whole.shape[0] : (at + 1) * whole.shape[0]] = l_two[at]
            lh_two[j, at * half : (at + 1) * half] = half_l[at]
        r_high[j], r_low[j] = r_two
        rt_high[j], rt_low[j] = split(right[j].T)
        turned = dot_three(split(dot_three(l_two, split(moment[j]), NN)), r_two, NN)
        base[j] = (BETA_ONE * gain) * turned

    @pl.loop(0, owned // 2)
    def _(j):
        prepare(j)

    for side in sides:

        @pl.when(~side["late"])
        def _():
            send_on(0, side)
            pl.when(z_edge)(functools.partial(send_own, 1, side, 0))
            send_own(1, side, 1)

    @pl.loop(owned // 2, owned)
    def _(j):
        prepare(j)

    for side in sides:

        @pl.when(side["late"])
        def _():
            send_on(0, side)

    def send_on_late_wave(late, places, where):
        for side in sides:

            @pl.when((side["late"] == late) & where)
            def _():
                send_on(1, side, places)

    send_on_late_wave(False, (0,), me >= 0)
    send_on_late_wave(False, (1,), z_edge)
    send_on_late_wave(True, (0, 1), after_edge)

    def pass_far(w):
        for t in range(WAVE):
            for side in sides:
                pl.when(side["gives"])(relay(w, side, t).wait_recv)
                hand(w, side["far"], t).start()

    def stacked(two, b_high, b_low):
        size = two.shape[0] // 2
        full = dot(two, b_high, NN)
        return full[:size] + (full[size:] + dot(two[:size], b_low, NN))

    def stack(two, at, value):
        size = value.shape[0]
        two[at, :size], two[at, size:] = split(value)

    def solve(indices, source, second_to, update_to, scales_to, between):
        size = source.shape[2]
        for at, j in enumerate(indices):
            both = dot(lt_two[j], source[table[2, j], table[3, j]], NN)
            stack(h_two, at, both[:size] + both[size:])
        for at, j in enumerate(indices):
            turned = stacked(h_two[at], r_high[j], r_low[j])
            second_next = BETA_TWO * second[j] + ((1.0 - BETA_TWO) * turned) * turned
            second_to[at] = second_next
            scaled = (base[j] + ((1.0 - BETA_ONE) * gain) * turned) / (second_next * lax.rsqrt(second_next) + EPSILON * bias_two**0.5)
            s_high[at], s_low[at] = split(scaled)
        between()
        for at, j in enumerate(indices):
            stack(z_two, at, stacked(lh_two[j], s_high[at], s_low[at]))
        for at, j in enumerate(indices):
            new = stacked(z_two[at], rt_high[j], rt_low[j])
            largest = jnp.maximum(jnp.max(jnp.abs(new), axis=0, keepdims=True), 1e-30)
            update_to[at] = jnp.round(new * (TOP / largest)).astype(jnp.int32).astype(I16)
            scales_to[at] = largest * (1.0 / TOP)

    loads[7].wait()
    pass_far(0)
    send_on_late_wave(False, (1,), ~z_edge)
    send_on_late_wave(True, (0,), ~after_edge)
    hand(0).wait_recv()
    solve(range(owned), gathered_a, second_out, update_a, scales_a, lambda: send_on_late_wave(True, (1,), ~after_edge))

    def chosen(k, s, absent):
        at = table[7 + 2 * k, s]
        value = update_a[at] if s < WAVE else update_b[table[4, at]]
        return jnp.where(table[6 + 2 * k, s] == 1, value, absent)

    def chosen_scale(k, s, absent):
        at = table[7 + 2 * k, s]
        value = scales_a[at] if s < WAVE else scales_b[table[4, at]]
        return jnp.where(table[6 + 2 * k, s] == 1, value, absent)

    def far(w, side, t):
        at = side["at"]
        part = (at, w, t) if t is not None else (at,)
        return push(codes.at[part], far_in.at[part], far_send.at[at], far_recv.at[at, WAVE * (w or 0) + (t or 0)], side["peer"])

    def far_scale(side):
        at = side["at"]
        return push(scales.at[at], far_scales.at[at], scale_send.at[at], scale_recv.at[at], side["peer"])

    def near(w, side, t):
        at = side["at"]
        part = (at, WAVE * w + t) if t is not None else (at,)
        held = (at, WAVE * w + t, rows) if t is not None else (at, slice(None), rows)
        return push(merged.at[part], out.at[held], near_send.at[at], near_recv.at[at, WAVE * (w or 0) + (t or 0)], side["peer"])

    def near_scale(side):
        at = side["at"]
        return push(merged_scales.at[at], out_scales.at[at, core], scale_send.at[2 + at], scale_recv.at[2 + at], side["peer"])

    def give(k=None, s=None):
        part = out.at[:, :, rows] if k is None else out.at[k, s, rows]
        return push(part, part, give_sem.at[0], give_sem.at[1], twin)

    def give_scale():
        part = out_scales.at[:, core]
        return push(part, part, scale_send.at[4], scale_recv.at[4], twin)

    def send_far(w):
        for t in range(WAVE):
            for side in sides:
                codes[side["at"], w, t] = chosen(side["to_far"], WAVE * w + t, jnp.zeros((), I16))
                pl.when(side["sends"])(far(w, side, t).start)
                scales[side["at"], w, pl.ds(t, 1)] = chosen_scale(side["to_far"], WAVE * w + t, 0.0)
        if w == 1:
            for side in sides:
                pl.when(side["sends"])(far_scale(side).start)
        for t in range(WAVE):
            s = WAVE * w + t
            out[2, s, rows] = chosen(2, s, jnp.zeros((), I16))
            give(2, s).start()
            out_scales[2, core, w, pl.ds(t, 1)] = chosen_scale(2, s, 0.0)

    def send_near(w, side):
        for t in range(WAVE):
            pl.when(side["has"])(far(w, side, t).wait_recv)
            merged[side["at"], WAVE * w + t] = chosen(side["to_near"], WAVE * w + t, far_in[side["at"], w, t])
            pl.when(side["sends"])(near(w, side, t).start)
        if w == 1:
            pl.when(side["has"])(far_scale(side).wait_recv)
            for s in range(slots):
                place = (side["at"], s // WAVE, pl.ds(s % WAVE, 1))
                merged_scales[place] = chosen_scale(side["to_near"], s, far_scales[place])
            pl.when(side["sends"])(near_scale(side).start)

    send_far(0)
    pass_far(1)
    hand(1).wait_recv()

    solve([table[5, b] for b in range(LATE)], gathered_b, second_late, update_b, scales_b, lambda: None)

    send_far(1)
    def each(order):
        for w, side in order:
            send_near(w, side)

    pl.when(left_edge)(lambda: each(((0, to_left), (0, to_right), (1, to_left), (1, to_right))))
    pl.when(right_edge)(lambda: each(((0, to_right), (0, to_left), (1, to_right), (1, to_left))))
    pl.when(~(left_edge | right_edge))(lambda: each(((0, to_right), (0, to_left), (1, to_right), (1, to_left))))

    @pl.loop(0, owned)
    def _(j):
        early, late = table[0, j] == 1, table[1, j] == 1
        gradient = jnp.where(late, gathered_b[table[2, j], table[3, j]].astype(F32), gathered_a[table[2, j], table[3, j]].astype(F32))
        first_out[j] = jnp.where(early | late, BETA_ONE * moment[j] + (1.0 - BETA_ONE) * gradient, 0.0)
        second_out[j] = jnp.where(late, second_late[table[4, j]], jnp.where(early, second_out[j], 0.0))

    for s in range(slots):
        for side in sides:
            pl.when(side["has"])(near(s // WAVE, side, s % WAVE).wait_recv)
            give(side["at"], s).start()
    for side in sides:
        pl.when(side["has"])(near_scale(side).wait_recv)
    give_scale().start()

    for s in range(slots):
        swap(s).wait_send()
    for w in range(2):
        hand(w).wait_send()
    for side in sides:

        @pl.when(side["sends"])
        def _():
            for w in range(2):
                own(w, side, None).wait_send()
            far(None, side, None).wait_send()
            far_scale(side).wait_send()
            near(None, side, None).wait_send()
            near_scale(side).wait_send()

        @pl.when(side["has"] & side["sends"])
        def _():
            for w in range(2):
                relay(w, side, None).wait_send()

    give().wait_send()
    give_scale().wait_send()
    give().wait_recv()
    give_scale().wait_recv()


def finish_kernel(codes, scales, first, second, direction, first_new, second_new, decoded, sem):
    slots = codes.shape[1]
    half = codes.shape[2] // 2
    copies = [pltpu.make_async_copy(first, first_new, sem.at[0]), pltpu.make_async_copy(second, second_new, sem.at[1])]
    for j in range(first.shape[0]):
        pltpu.make_async_copy(first.at[j], first_new.at[j], sem.at[0]).start()
        pltpu.make_async_copy(second.at[j], second_new.at[j], sem.at[1]).start()
    for s in range(slots):
        for core in range(2):
            rows = pl.ds(core * half, half)
            total = 0.0
            for k in range(3):
                total += codes[k, s, rows].astype(jnp.int32).astype(F32) * scales[k, core, s // WAVE, pl.ds(s % WAVE, 1)]
            decoded[s, rows] = total
        copy = pltpu.make_async_copy(decoded.at[s], direction.at[s], sem.at[2 + s])
        copy.start()
        copies.append(copy)
    for copy in copies:
        copy.wait()


def body(gradients, first_moment, second_moment, left_basis, right_basis, shard_starts, block_owners):
    devices = lax.axis_size("fsdp")
    slots = gradients.shape[1]
    owned, width = first_moment.shape[0], first_moment.shape[1]
    half = width // 2
    any_space = pl.BlockSpec(memory_space=pl.ANY)
    in_vmem = pl.BlockSpec(memory_space=pltpu.VMEM)
    dma = pltpu.SemaphoreType.DMA
    keep = functools.partial(pltpu.with_memory_space_constraint, memory_space=pltpu.VMEM)
    stay = functools.partial(pltpu.with_memory_space_constraint, memory_space=pltpu.HBM)
    matrices = (owned, width, width)
    halves = (owned, half, width)
    first_new, second_new, out, out_scales = pl.pallas_call(
        functools.partial(soap_kernel, devices),
        out_shape=[
            pltpu.VMEM(matrices, F32),
            pltpu.VMEM(matrices, F32),
            pltpu.VMEM((3, slots, width, width), I16),
            pltpu.VMEM((3, 2, 2, WAVE, width), F32),
        ],
        in_specs=[any_space] * 7,
        out_specs=[in_vmem] * 4,
        scratch_shapes=[
            pltpu.SMEM(shard_starts.shape, jnp.int32),
            pltpu.SMEM(block_owners.shape, jnp.int32),
            pltpu.SMEM((16, 8), jnp.int32),
            *[pltpu.VMEM((slots, half, width), BF16)] * 3,
            *[pltpu.VMEM((5, WAVE, width, width), BF16)] * 2,
            *[pltpu.VMEM(matrices, F32)] * 4,
            pltpu.VMEM((owned, 2 * width, width), BF16),
            pltpu.VMEM((owned, width, width), BF16),
            *[pltpu.VMEM(matrices, BF16)] * 4,
            pltpu.VMEM(matrices, F32),
            pltpu.VMEM(halves, I16),
            pltpu.VMEM((LATE, half, width), I16),
            pltpu.VMEM((owned, 1, width), F32),
            pltpu.VMEM((LATE, 1, width), F32),
            pltpu.VMEM((LATE, width, width), F32),
            *[pltpu.VMEM((2, 2, WAVE, half, width), I16), pltpu.VMEM((2, 2, WAVE, width), F32)] * 2,
            pltpu.VMEM((2, slots, half, width), I16),
            pltpu.VMEM((2, 2, WAVE, width), F32),
            pltpu.VMEM((owned, 2 * width, width), BF16),
            *[pltpu.VMEM(matrices, BF16)] * 2,
            pltpu.VMEM((owned, width, width), BF16),
            dma((8,)), dma((2, slots)), *[dma((2, 2))] * 2, dma((4, slots)), *[dma((2,))] * 2,
            *[dma((2,)), dma((2, slots))] * 2, dma((2,)), *[dma((5,))] * 2,
        ],
        compiler_params=pltpu.CompilerParams(collective_id=0, has_side_effects=True, vmem_limit_bytes=ROOM),
        name="soap",
    )(*map(stay, (shard_starts, block_owners, gradients, first_moment, second_moment, left_basis, right_basis)))

    return tuple(
        pl.pallas_call(
            finish_kernel,
            out_shape=[
                jax.ShapeDtypeStruct((slots, width, width), F32),
                jax.ShapeDtypeStruct(matrices, F32),
                jax.ShapeDtypeStruct(matrices, F32),
            ],
            in_specs=[in_vmem] * 4,
            out_specs=[any_space] * 3,
            scratch_shapes=[pltpu.VMEM((slots, width, width), F32), dma((2 + slots,))],
            compiler_params=pltpu.CompilerParams(vmem_limit_bytes=8 * 2**20),
            name="finish",
        )(*map(keep, (out, out_scales, first_new, second_new)))
    )


def solution(mesh):
    in_specs = (
        P("dp", "fsdp", None, None),
        P("fsdp", None, None),
        P("fsdp", None, None),
        P("fsdp", None, None),
        P("fsdp", None, None),
        P(),
        P(),
    )
    out_specs = (P("fsdp", None, None), P("fsdp", None, None), P("fsdp", None, None))
    return jax.shard_map(body, mesh=mesh, in_specs=in_specs, out_specs=out_specs, check_vma=False)
```

```python
import functools

import jax
import jax.numpy as jnp
from jax import lax
from jax.experimental import pallas as pl
from jax.experimental.pallas import tpu as pltpu
from jax.sharding import PartitionSpec as P

STEP = 10
BETA_ONE = 0.9
BETA_TWO = 0.95
EPSILON = 1e-08
TOP = 32766.0
ROOM = 40 * 2**20
MESH = pl.DeviceIdType.MESH
F32 = jnp.float32
BF16 = jnp.bfloat16
I16 = jnp.int16


def neighbours(devices):
    me = lax.axis_index("fsdp")
    core = lax.axis_index("dp")
    right = {"fsdp": jnp.minimum(me + 1, devices - 1)}
    left = {"fsdp": jnp.maximum(me - 1, 0)}
    twin = {"dp": 1 - core}
    return me, core, right, left, twin


def greet(me, devices, right, left, twin):
    barrier = pltpu.get_barrier_semaphore()

    def signal(peer):
        pl.semaphore_signal(barrier, inc=1, device_id=peer, device_id_type=MESH)

    signal(twin)
    pl.when(me < devices - 1)(lambda: signal(right))
    pl.when(me > 0)(lambda: signal(left))
    at_end = (me == 0) | (me == devices - 1)
    pl.when(at_end)(lambda: pl.semaphore_wait(barrier, 2))
    pl.when(~at_end)(lambda: pl.semaphore_wait(barrier, 3))


def push(src, dst, send_sem, recv_sem, peer):
    return pltpu.make_async_remote_copy(
        src_ref=src,
        dst_ref=dst,
        send_sem=send_sem,
        recv_sem=recv_sem,
        device_id=peer,
        device_id_type=MESH,
    )


def split(x):
    high = x.astype(BF16)
    return high, (x - high.astype(F32)).astype(BF16)


def dot(a, b, dims):
    return lax.dot_general(a, b, (dims, ((), ())), preferred_element_type=F32)


def dot_three(a, b, dims):
    return dot(a[0], b[0], dims) + (dot(a[0], b[1], dims) + dot(a[1], b[0], dims))


NN = ((1,), (0,))
NT = ((1,), (1,))
WAVE = 2
LATE = 4


def soap_kernel(
    devices, starts_in, owners_in, grad, moment_in, second_in, left_in, right_in, first_out, second_out, out, out_scales,
    starts, owners, table, mine, theirs, other, gathered_a, gathered_b, moment, second, left, right, lt_two, lh_two, r_high, r_low, rt_high, rt_low,
    base, update_a, update_b, scales_a, scales_b, second_late, codes, scales, far_in, far_scales, merged, merged_scales, h_two, s_high, s_low, z_two,
    load_sem, swap_sem, own_send, relay_send, ring_recv, hand_send, hand_recv, far_send, far_recv, near_send, near_recv, give_sem, scale_send, scale_recv
):
    me, core, right_peer, left_peer, twin = neighbours(devices)
    slots = grad.shape[1]
    half = grad.shape[2] // 2
    owned = moment.shape[0]
    blocks = owners.shape[0]
    rows = pl.ds(pl.multiple_of(core * half, half), half)
    other_rows = pl.ds(pl.multiple_of((1 - core) * half, half), half)
    gathered = (gathered_a, gathered_b)

    loads = [
        pltpu.make_async_copy(src, dst, load_sem.at[at])
        for at, (src, dst) in enumerate(
            (
                (grad.at[0, :, other_rows], other),
                (grad.at[0, :, rows], mine),
                (starts_in, starts),
                (owners_in, owners),
                (left_in, left),
                (moment_in, moment),
                (right_in, right),
                (second_in, second),
            )
        )
    ]
    for load in loads:
        load.start()
    greet(me, devices, right_peer, left_peer, twin)

    def swap(s):
        return push(other.at[s], theirs.at[s], swap_sem.at[0, s], swap_sem.at[1, s], twin)

    def own(w, side, t):
        source = gathered[w].at[2, t, rows] if t is not None else gathered[w].at[2, :, rows]
        target = gathered[w].at[side["near"], t, rows] if t is not None else gathered[w].at[side["near"], :, rows]
        arrived = ring_recv.at[side["at"], WAVE * w + (t or 0)]
        return push(source, target, own_send.at[side["at"], w], arrived, side["peer"])

    def relay(w, side, t):
        source = gathered[w].at[side["near"], t, rows] if t is not None else gathered[w].at[side["near"], :, rows]
        target = gathered[w].at[side["far"], t, rows] if t is not None else gathered[w].at[side["far"], :, rows]
        arrived = ring_recv.at[2 + side["at"], WAVE * w + (t or 0)]
        return push(source, target, relay_send.at[side["at"], w], arrived, side["peer"])

    def hand(w, k=None, t=None):
        part = gathered[w].at[:, :, rows] if k is None else gathered[w].at[k, t, rows]
        return push(part, part, hand_send.at[w], hand_recv.at[w], twin)

    to_right = dict(at=0, near=1, far=0, peer=right_peer, has=me >= 1, gives=me >= 2, sends=me < devices - 1, to_far=4, to_near=3)
    to_left = dict(at=1, near=3, far=4, peer=left_peer, has=me < devices - 1, gives=me < devices - 2, sends=me >= 1, to_far=0, to_near=1)
    sides = (to_right, to_left)

    def send_own(w, side, t):
        pl.when(side["sends"])(own(w, side, t).start)

    def send_on(w, side, places=range(WAVE)):
        for t in places:

            @pl.when(side["has"])
            def _():
                own(w, side, t).wait_recv()

            @pl.when(side["has"] & side["sends"])
            def _():
                relay(w, side, t).start()

            hand(w, side["near"], t).start()

    left_edge, right_edge = lax.rem(me, 4) == 0, lax.rem(me, 4) == 3
    z_edge = (lax.rem(me, 16) == 0) | (lax.rem(me, 16) == 15)
    after_edge = (lax.rem(me, 16) == 1) | (lax.rem(me, 16) == 14)
    to_right["late"] = left_edge | (lax.rem(me, 16) == 1)
    to_left["late"] = right_edge | (lax.rem(me, 16) == 14)

    loads[0].wait()
    for s in range(slots):
        swap(s).start()
    loads[1].wait()
    for w in range(2):
        for t in range(WAVE):
            s = WAVE * w + t
            swap(s).wait_recv()
            gathered[w][2, t, rows] = (mine[s].astype(F32) + theirs[s].astype(F32)).astype(BF16)
            for side in sides:
                if w == 0:
                    send_own(w, side, t)
                elif t == 0:
                    pl.when(side["late"] | ~z_edge)(functools.partial(send_own, w, side, t))
                else:
                    pl.when(side["late"])(functools.partial(send_own, w, side, t))
    for w in range(2):
        for t in range(WAVE):
            hand(w, 2, t).start()

    for side in sides:

        @pl.when(~side["has"])
        def _():
            far_in[side["at"]] = jnp.zeros(far_in.shape[1:], I16)
            far_scales[side["at"]] = jnp.zeros(far_scales.shape[1:], F32)
            out_scales[side["at"], core] = jnp.zeros(out_scales.shape[2:], F32)
            for s in range(slots):
                out[side["at"], s, rows] = jnp.zeros((half, out.shape[3]), I16)
                gathered[s // WAVE][side["near"], s % WAVE, rows] = jnp.zeros((half, out.shape[3]), BF16)

        @pl.when(~side["gives"])
        def _():
            for s in range(slots):
                gathered[s // WAVE][side["far"], s % WAVE, rows] = jnp.zeros((half, out.shape[3]), BF16)

    loads[2].wait()
    loads[3].wait()

    def start_of(device):
        value = starts[jnp.clip(device, 0, devices - 1)]
        return jnp.where(device < 0, -1, jnp.where(device >= devices, blocks, value))

    first = jnp.maximum(start_of(me - 2), 0)
    below = jnp.int32(0)
    for k in range(5 * slots):
        at = first + k
        owner = owners[jnp.minimum(at, blocks - 1)]
        below += jnp.where((at < blocks) & (owner < me), 1, 0)
    first = first + below
    rank = jnp.int32(0)
    chosen_late = [jnp.int32(0)] * LATE
    for j in range(owned):
        block = first + j
        live = (block < blocks) & (owners[jnp.minimum(block, blocks - 1)] == me)
        place = jnp.int32(0)
        for delta in (-1, 0, 1, 2):
            place += jnp.where(start_of(me + delta) <= block, 1, 0)
        slot = block - starts[jnp.clip(me + place - 2, 0, devices - 1)]
        late = live & (slot >= WAVE)
        table[0, j] = jnp.where(live & ~late, 1, 0)
        table[1, j] = jnp.where(late, 1, 0)
        table[2, j] = jnp.where(live, jnp.clip(place, 0, 4), 0)
        table[3, j] = jnp.where(live, jnp.clip(lax.rem(slot, WAVE), 0, WAVE - 1), 0)
        table[4, j] = rank
        for b in range(LATE):
            chosen_late[b] = jnp.where(late & (rank == b), j, chosen_late[b])
        rank = jnp.minimum(rank + jnp.where(late, 1, 0), LATE - 1)
    for b in range(LATE):
        table[5, b] = chosen_late[b]
    for k in range(5):
        holder = me + k - 2
        begin, end = start_of(holder), start_of(holder + 1)
        for s in range(slots):
            block = begin + s
            valid = (holder >= 0) & (holder < devices) & (block < end) & (owners[jnp.clip(block, 0, blocks - 1)] == me)
            table[6 + 2 * k, s] = jnp.where(valid, 1, 0)
            table[7 + 2 * k, s] = jnp.where(valid, jnp.clip(block - first, 0, owned - 1), 0)

    loads[4].wait()
    loads[5].wait()
    loads[6].wait()

    bias_one = 1.0 - BETA_ONE**STEP
    bias_two = 1.0 - BETA_TWO**STEP
    gain = bias_two**0.5 / bias_one

    def prepare(j):
        whole = left[j]
        l_two = split(whole.T)
        half_l = split(left[j, rows])
        r_two = split(right[j])
        for at in range(2):
            lt_two[j, at * whole.shape[0] : (at + 1) * whole.shape[0]] = l_two[at]
            lh_two[j, at * half : (at + 1) * half] = half_l[at]
        r_high[j], r_low[j] = r_two
        rt_high[j], rt_low[j] = split(right[j].T)
        turned = dot_three(split(dot_three(l_two, split(moment[j]), NN)), r_two, NN)
        base[j] = (BETA_ONE * gain) * turned

    @pl.loop(0, owned // 2)
    def _(j):
        prepare(j)

    for side in sides:

        @pl.when(~side["late"])
        def _():
            send_on(0, side)
            pl.when(z_edge)(functools.partial(send_own, 1, side, 0))
            send_own(1, side, 1)

    @pl.loop(owned // 2, owned)
    def _(j):
        prepare(j)

    for side in sides:

        @pl.when(side["late"])
        def _():
            send_on(0, side)

    def send_on_late_wave(late, places, where):
        for side in sides:

            @pl.when((side["late"] == late) & where)
            def _():
                send_on(1, side, places)

    send_on_late_wave(False, (0,), me >= 0)
    send_on_late_wave(False, (1,), z_edge)
    send_on_late_wave(True, (0, 1), after_edge)

    def pass_far(w):
        for t in range(WAVE):
            for side in sides:
                pl.when(side["gives"])(relay(w, side, t).wait_recv)
                hand(w, side["far"], t).start()

    def stacked(two, b_high, b_low):
        size = two.shape[0] // 2
        full = dot(two, b_high, NN)
        return full[:size] + (full[size:] + dot(two[:size], b_low, NN))

    def stack(two, at, value):
        size = value.shape[0]
        two[at, :size], two[at, size:] = split(value)

    def solve(indices, source, second_to, update_to, scales_to, between):
        size = source.shape[2]
        for at, j in enumerate(indices):
            both = dot(lt_two[j], source[table[2, j], table[3, j]], NN)
            stack(h_two, at, both[:size] + both[size:])
        for at, j in enumerate(indices):
            turned = stacked(h_two[at], r_high[j], r_low[j])
            second_next = BETA_TWO * second[j] + ((1.0 - BETA_TWO) * turned) * turned
            second_to[at] = second_next
            scaled = (base[j] + ((1.0 - BETA_ONE) * gain) * turned) / (second_next * lax.rsqrt(second_next) + EPSILON * bias_two**0.5)
            s_high[at], s_low[at] = split(scaled)
        between()
        for at, j in enumerate(indices):
            stack(z_two, at, stacked(lh_two[j], s_high[at], s_low[at]))
        for at, j in enumerate(indices):
            new = stacked(z_two[at], rt_high[j], rt_low[j])
            largest = jnp.maximum(jnp.max(jnp.abs(new), axis=0, keepdims=True), 1e-30)
            update_to[at] = jnp.round(new * (TOP / largest)).astype(jnp.int32).astype(I16)
            scales_to[at] = largest * (1.0 / TOP)

    loads[7].wait()
    pass_far(0)
    send_on_late_wave(False, (1,), ~z_edge)
    send_on_late_wave(True, (0,), ~after_edge)
    hand(0).wait_recv()
    solve(range(owned), gathered_a, second_out, update_a, scales_a, lambda: send_on_late_wave(True, (1,), ~after_edge))

    def chosen(k, s, absent):
        at = table[7 + 2 * k, s]
        value = update_a[at] if s < WAVE else update_b[table[4, at]]
        return jnp.where(table[6 + 2 * k, s] == 1, value, absent)

    def chosen_scale(k, s, absent):
        at = table[7 + 2 * k, s]
        value = scales_a[at] if s < WAVE else scales_b[table[4, at]]
        return jnp.where(table[6 + 2 * k, s] == 1, value, absent)

    def far(w, side, t):
        at = side["at"]
        part = (at, w, t) if t is not None else (at,)
        return push(codes.at[part], far_in.at[part], far_send.at[at], far_recv.at[at, WAVE * (w or 0) + (t or 0)], side["peer"])

    def far_scale(side):
        at = side["at"]
        return push(scales.at[at], far_scales.at[at], scale_send.at[at], scale_recv.at[at], side["peer"])

    def near(w, side, t):
        at = side["at"]
        part = (at, WAVE * w + t) if t is not None else (at,)
        held = (at, WAVE * w + t, rows) if t is not None else (at, slice(None), rows)
        return push(merged.at[part], out.at[held], near_send.at[at], near_recv.at[at, WAVE * (w or 0) + (t or 0)], side["peer"])

    def near_scale(side):
        at = side["at"]
        return push(merged_scales.at[at], out_scales.at[at, core], scale_send.at[2 + at], scale_recv.at[2 + at], side["peer"])

    def give(k=None, s=None):
        part = out.at[:, :, rows] if k is None else out.at[k, s, rows]
        return push(part, part, give_sem.at[0], give_sem.at[1], twin)

    def give_scale():
        part = out_scales.at[:, core]
        return push(part, part, scale_send.at[4], scale_recv.at[4], twin)

    def send_far(w):
        for t in range(WAVE):
            for side in sides:
                scales[side["at"], w, pl.ds(t, 1)] = chosen_scale(side["to_far"], WAVE * w + t, 0.0)
        if w == 1:
            for side in sides:
                pl.when(side["sends"])(far_scale(side).start)
        for t in range(WAVE):
            for side in sides:
                codes[side["at"], w, t] = chosen(side["to_far"], WAVE * w + t, jnp.zeros((), I16))
                pl.when(side["sends"])(far(w, side, t).start)
        for t in range(WAVE):
            s = WAVE * w + t
            out[2, s, rows] = chosen(2, s, jnp.zeros((), I16))
            give(2, s).start()
            out_scales[2, core, w, pl.ds(t, 1)] = chosen_scale(2, s, 0.0)

    def send_near(w, side):
        if w == 1:
            pl.when(side["has"])(far_scale(side).wait_recv)
            for s in range(slots):
                place = (side["at"], s // WAVE, pl.ds(s % WAVE, 1))
                merged_scales[place] = chosen_scale(side["to_near"], s, far_scales[place])
            pl.when(side["sends"])(near_scale(side).start)
        for t in range(WAVE):
            pl.when(side["has"])(far(w, side, t).wait_recv)
            merged[side["at"], WAVE * w + t] = chosen(side["to_near"], WAVE * w + t, far_in[side["at"], w, t])
            pl.when(side["sends"])(near(w, side, t).start)

    send_far(0)
    pass_far(1)
    hand(1).wait_recv()

    solve([table[5, b] for b in range(LATE)], gathered_b, second_late, update_b, scales_b, lambda: None)

    send_far(1)
    def each(order):
        for w, side in order:
            send_near(w, side)

    pl.when(left_edge)(lambda: each(((0, to_left), (0, to_right), (1, to_left), (1, to_right))))
    pl.when(right_edge)(lambda: each(((0, to_right), (0, to_left), (1, to_right), (1, to_left))))
    pl.when(~(left_edge | right_edge))(lambda: each(((0, to_right), (0, to_left), (1, to_right), (1, to_left))))

    @pl.loop(0, owned)
    def _(j):
        early, late = table[0, j] == 1, table[1, j] == 1
        gradient = jnp.where(late, gathered_b[table[2, j], table[3, j]].astype(F32), gathered_a[table[2, j], table[3, j]].astype(F32))
        first_out[j] = jnp.where(early | late, BETA_ONE * moment[j] + (1.0 - BETA_ONE) * gradient, 0.0)
        second_out[j] = jnp.where(late, second_late[table[4, j]], jnp.where(early, second_out[j], 0.0))

    for s in range(slots):
        if s == slots - 1:
            for side in sides:
                pl.when(side["has"])(near_scale(side).wait_recv)
            give_scale().start()
        for side in sides:
            pl.when(side["has"])(near(s // WAVE, side, s % WAVE).wait_recv)
            give(side["at"], s).start()

    for s in range(slots):
        swap(s).wait_send()
    for w in range(2):
        hand(w).wait_send()
    for side in sides:

        @pl.when(side["sends"])
        def _():
            for w in range(2):
                own(w, side, None).wait_send()
            far(None, side, None).wait_send()
            far_scale(side).wait_send()
            near(None, side, None).wait_send()
            near_scale(side).wait_send()

        @pl.when(side["has"] & side["sends"])
        def _():
            for w in range(2):
                relay(w, side, None).wait_send()

    give().wait_send()
    give_scale().wait_send()
    give().wait_recv()
    give_scale().wait_recv()


def finish_kernel(codes, scales, first, second, direction, first_new, second_new, decoded, sem):
    slots = codes.shape[1]
    half = codes.shape[2] // 2
    copies = [pltpu.make_async_copy(first, first_new, sem.at[0]), pltpu.make_async_copy(second, second_new, sem.at[1])]
    for j in range(first.shape[0]):
        pltpu.make_async_copy(first.at[j], first_new.at[j], sem.at[0]).start()
        pltpu.make_async_copy(second.at[j], second_new.at[j], sem.at[1]).start()
    for s in range(slots):
        for core in range(2):
            rows = pl.ds(core * half, half)
            total = 0.0
            for k in range(3):
                total += codes[k, s, rows].astype(jnp.int32).astype(F32) * scales[k, core, s // WAVE, pl.ds(s % WAVE, 1)]
            decoded[s, rows] = total
        copy = pltpu.make_async_copy(decoded.at[s], direction.at[s], sem.at[2 + s])
        copy.start()
        copies.append(copy)
    for copy in copies:
        copy.wait()


def body(gradients, first_moment, second_moment, left_basis, right_basis, shard_starts, block_owners):
    devices = lax.axis_size("fsdp")
    slots = gradients.shape[1]
    owned, width = first_moment.shape[0], first_moment.shape[1]
    half = width // 2
    any_space = pl.BlockSpec(memory_space=pl.ANY)
    in_vmem = pl.BlockSpec(memory_space=pltpu.VMEM)
    dma = pltpu.SemaphoreType.DMA
    keep = functools.partial(pltpu.with_memory_space_constraint, memory_space=pltpu.VMEM)
    stay = functools.partial(pltpu.with_memory_space_constraint, memory_space=pltpu.HBM)
    matrices = (owned, width, width)
    halves = (owned, half, width)
    first_new, second_new, out, out_scales = pl.pallas_call(
        functools.partial(soap_kernel, devices),
        out_shape=[
            pltpu.VMEM(matrices, F32),
            pltpu.VMEM(matrices, F32),
            pltpu.VMEM((3, slots, width, width), I16),
            pltpu.VMEM((3, 2, 2, WAVE, width), F32),
        ],
        in_specs=[any_space] * 7,
        out_specs=[in_vmem] * 4,
        scratch_shapes=[
            pltpu.SMEM(shard_starts.shape, jnp.int32),
            pltpu.SMEM(block_owners.shape, jnp.int32),
            pltpu.SMEM((16, 8), jnp.int32),
            *[pltpu.VMEM((slots, half, width), BF16)] * 3,
            *[pltpu.VMEM((5, WAVE, width, width), BF16)] * 2,
            *[pltpu.VMEM(matrices, F32)] * 4,
            pltpu.VMEM((owned, 2 * width, width), BF16),
            pltpu.VMEM((owned, width, width), BF16),
            *[pltpu.VMEM(matrices, BF16)] * 4,
            pltpu.VMEM(matrices, F32),
            pltpu.VMEM(halves, I16),
            pltpu.VMEM((LATE, half, width), I16),
            pltpu.VMEM((owned, 1, width), F32),
            pltpu.VMEM((LATE, 1, width), F32),
            pltpu.VMEM((LATE, width, width), F32),
            *[pltpu.VMEM((2, 2, WAVE, half, width), I16), pltpu.VMEM((2, 2, WAVE, width), F32)] * 2,
            pltpu.VMEM((2, slots, half, width), I16),
            pltpu.VMEM((2, 2, WAVE, width), F32),
            pltpu.VMEM((owned, 2 * width, width), BF16),
            *[pltpu.VMEM(matrices, BF16)] * 2,
            pltpu.VMEM((owned, width, width), BF16),
            dma((8,)), dma((2, slots)), *[dma((2, 2))] * 2, dma((4, slots)), *[dma((2,))] * 2,
            *[dma((2,)), dma((2, slots))] * 2, dma((2,)), *[dma((5,))] * 2,
        ],
        compiler_params=pltpu.CompilerParams(collective_id=0, has_side_effects=True, vmem_limit_bytes=ROOM),
        name="soap",
    )(*map(stay, (shard_starts, block_owners, gradients, first_moment, second_moment, left_basis, right_basis)))

    return tuple(
        pl.pallas_call(
            finish_kernel,
            out_shape=[
                jax.ShapeDtypeStruct((slots, width, width), F32),
                jax.ShapeDtypeStruct(matrices, F32),
                jax.ShapeDtypeStruct(matrices, F32),
            ],
            in_specs=[in_vmem] * 4,
            out_specs=[any_space] * 3,
            scratch_shapes=[pltpu.VMEM((slots, width, width), F32), dma((2 + slots,))],
            compiler_params=pltpu.CompilerParams(vmem_limit_bytes=8 * 2**20),
            name="finish",
        )(*map(keep, (out, out_scales, first_new, second_new)))
    )


def solution(mesh):
    in_specs = (
        P("dp", "fsdp", None, None),
        P("fsdp", None, None),
        P("fsdp", None, None),
        P("fsdp", None, None),
        P("fsdp", None, None),
        P(),
        P(),
    )
    out_specs = (P("fsdp", None, None), P("fsdp", None, None), P("fsdp", None, None))
    return jax.shard_map(body, mesh=mesh, in_specs=in_specs, out_specs=out_specs, check_vma=False)
```

```python
import functools

import jax
import jax.numpy as jnp
from jax import lax
from jax.experimental import pallas as pl
from jax.experimental.pallas import tpu as pltpu
from jax.sharding import PartitionSpec as P

STEP = 10
BETA_ONE = 0.9
BETA_TWO = 0.95
EPSILON = 1e-08
TOP = 32766.0
ROOM = 40 * 2**20
MESH = pl.DeviceIdType.MESH
F32 = jnp.float32
BF16 = jnp.bfloat16
I16 = jnp.int16


def neighbours(devices):
    me = lax.axis_index("fsdp")
    core = lax.axis_index("dp")
    right = {"fsdp": jnp.minimum(me + 1, devices - 1)}
    left = {"fsdp": jnp.maximum(me - 1, 0)}
    twin = {"dp": 1 - core}
    return me, core, right, left, twin


def greet(me, devices, right, left, twin):
    barrier = pltpu.get_barrier_semaphore()

    def signal(peer):
        pl.semaphore_signal(barrier, inc=1, device_id=peer, device_id_type=MESH)

    signal(twin)
    pl.when(me < devices - 1)(lambda: signal(right))
    pl.when(me > 0)(lambda: signal(left))
    at_end = (me == 0) | (me == devices - 1)
    pl.when(at_end)(lambda: pl.semaphore_wait(barrier, 2))
    pl.when(~at_end)(lambda: pl.semaphore_wait(barrier, 3))


def push(src, dst, send_sem, recv_sem, peer):
    return pltpu.make_async_remote_copy(
        src_ref=src,
        dst_ref=dst,
        send_sem=send_sem,
        recv_sem=recv_sem,
        device_id=peer,
        device_id_type=MESH,
    )


def split(x):
    high = x.astype(BF16)
    return high, (x - high.astype(F32)).astype(BF16)


def dot(a, b, dims):
    return lax.dot_general(a, b, (dims, ((), ())), preferred_element_type=F32)


def dot_three(a, b, dims):
    return dot(a[0], b[0], dims) + (dot(a[0], b[1], dims) + dot(a[1], b[0], dims))


NN = ((1,), (0,))
NT = ((1,), (1,))
WAVE = 2
LATE = 4


def soap_kernel(
    devices, starts_in, owners_in, grad, moment_in, second_in, left_in, right_in, first_out, second_out, out, out_scales,
    starts, owners, table, mine, theirs, other, gathered_a, gathered_b, moment, second, left, right, lt_two, lh_two, r_high, r_low, rt_high, rt_low,
    base, update_a, update_b, scales_a, scales_b, second_late, codes, scales, far_in, far_scales, merged, merged_scales, h_two, s_high, s_low, z_two,
    load_sem, swap_sem, own_send, relay_send, ring_recv, hand_send, hand_recv, far_send, far_recv, near_send, near_recv, give_sem, scale_send, scale_recv
):
    me, core, right_peer, left_peer, twin = neighbours(devices)
    slots = grad.shape[1]
    half = grad.shape[2] // 2
    owned = moment.shape[0]
    blocks = owners.shape[0]
    rows = pl.ds(pl.multiple_of(core * half, half), half)
    other_rows = pl.ds(pl.multiple_of((1 - core) * half, half), half)
    gathered = (gathered_a, gathered_b)

    loads = [
        pltpu.make_async_copy(src, dst, load_sem.at[at])
        for at, (src, dst) in enumerate(
            (
                (grad.at[0, :, other_rows], other),
                (grad.at[0, :, rows], mine),
                (starts_in, starts),
                (owners_in, owners),
                (left_in, left),
                (moment_in, moment),
                (right_in, right),
                (second_in, second),
            )
        )
    ]
    for load in loads:
        load.start()
    greet(me, devices, right_peer, left_peer, twin)

    def swap(s):
        return push(other.at[s], theirs.at[s], swap_sem.at[0, s], swap_sem.at[1, s], twin)

    def own(w, side, t):
        source = gathered[w].at[2, t, rows] if t is not None else gathered[w].at[2, :, rows]
        target = gathered[w].at[side["near"], t, rows] if t is not None else gathered[w].at[side["near"], :, rows]
        arrived = ring_recv.at[side["at"], WAVE * w + (t or 0)]
        return push(source, target, own_send.at[side["at"], w], arrived, side["peer"])

    def relay(w, side, t):
        source = gathered[w].at[side["near"], t, rows] if t is not None else gathered[w].at[side["near"], :, rows]
        target = gathered[w].at[side["far"], t, rows] if t is not None else gathered[w].at[side["far"], :, rows]
        arrived = ring_recv.at[2 + side["at"], WAVE * w + (t or 0)]
        return push(source, target, relay_send.at[side["at"], w], arrived, side["peer"])

    def hand(w, k=None, t=None):
        part = gathered[w].at[:, :, rows] if k is None else gathered[w].at[k, t, rows]
        return push(part, part, hand_send.at[w], hand_recv.at[w], twin)

    to_right = dict(at=0, near=1, far=0, peer=right_peer, has=me >= 1, gives=me >= 2, sends=me < devices - 1, to_far=4, to_near=3)
    to_left = dict(at=1, near=3, far=4, peer=left_peer, has=me < devices - 1, gives=me < devices - 2, sends=me >= 1, to_far=0, to_near=1)
    sides = (to_right, to_left)

    def send_own(w, side, t):
        pl.when(side["sends"])(own(w, side, t).start)

    def send_on(w, side, places=range(WAVE)):
        for t in places:

            @pl.when(side["has"])
            def _():
                own(w, side, t).wait_recv()

            @pl.when(side["has"] & side["sends"])
            def _():
                relay(w, side, t).start()

            hand(w, side["near"], t).start()

    left_edge, right_edge = lax.rem(me, 4) == 0, lax.rem(me, 4) == 3
    z_edge = (lax.rem(me, 16) == 0) | (lax.rem(me, 16) == 15)
    after_edge = (lax.rem(me, 16) == 1) | (lax.rem(me, 16) == 14)
    to_right["late"] = left_edge | (lax.rem(me, 16) == 1)
    to_left["late"] = right_edge | (lax.rem(me, 16) == 14)

    loads[0].wait()
    for s in range(slots):
        swap(s).start()
    loads[1].wait()
    for w in range(2):
        for t in range(WAVE):
            s = WAVE * w + t
            swap(s).wait_recv()
            gathered[w][2, t, rows] = (mine[s].astype(F32) + theirs[s].astype(F32)).astype(BF16)
            for side in sides:
                if w == 0:
                    send_own(w, side, t)
                elif t == 0:
                    pl.when(side["late"] | ~z_edge)(functools.partial(send_own, w, side, t))
                else:
                    pl.when(side["late"])(functools.partial(send_own, w, side, t))
    for w in range(2):
        for t in range(WAVE):
            hand(w, 2, t).start()

    for side in sides:

        @pl.when(~side["has"])
        def _():
            far_in[side["at"]] = jnp.zeros(far_in.shape[1:], I16)
            far_scales[side["at"]] = jnp.zeros(far_scales.shape[1:], F32)
            out_scales[side["at"], core] = jnp.zeros(out_scales.shape[2:], F32)
            for s in range(slots):
                out[side["at"], s, rows] = jnp.zeros((half, out.shape[3]), I16)
                gathered[s // WAVE][side["near"], s % WAVE, rows] = jnp.zeros((half, out.shape[3]), BF16)

        @pl.when(~side["gives"])
        def _():
            for s in range(slots):
                gathered[s // WAVE][side["far"], s % WAVE, rows] = jnp.zeros((half, out.shape[3]), BF16)

    loads[2].wait()
    loads[3].wait()

    def start_of(device):
        value = starts[jnp.clip(device, 0, devices - 1)]
        return jnp.where(device < 0, -1, jnp.where(device >= devices, blocks, value))

    first = jnp.maximum(start_of(me - 2), 0)
    below = jnp.int32(0)
    for k in range(5 * slots):
        at = first + k
        owner = owners[jnp.minimum(at, blocks - 1)]
        below += jnp.where((at < blocks) & (owner < me), 1, 0)
    first = first + below
    rank = jnp.int32(0)
    chosen_late = [jnp.int32(0)] * LATE
    for j in range(owned):
        block = first + j
        live = (block < blocks) & (owners[jnp.minimum(block, blocks - 1)] == me)
        place = jnp.int32(0)
        for delta in (-1, 0, 1, 2):
            place += jnp.where(start_of(me + delta) <= block, 1, 0)
        slot = block - starts[jnp.clip(me + place - 2, 0, devices - 1)]
        late = live & (slot >= WAVE)
        table[0, j] = jnp.where(live & ~late, 1, 0)
        table[1, j] = jnp.where(late, 1, 0)
        table[2, j] = jnp.where(live, jnp.clip(place, 0, 4), 0)
        table[3, j] = jnp.where(live, jnp.clip(lax.rem(slot, WAVE), 0, WAVE - 1), 0)
        table[4, j] = rank
        for b in range(LATE):
            chosen_late[b] = jnp.where(late & (rank == b), j, chosen_late[b])
        rank = jnp.minimum(rank + jnp.where(late, 1, 0), LATE - 1)
    for b in range(LATE):
        table[5, b] = chosen_late[b]
    for k in range(5):
        holder = me + k - 2
        begin, end = start_of(holder), start_of(holder + 1)
        for s in range(slots):
            block = begin + s
            valid = (holder >= 0) & (holder < devices) & (block < end) & (owners[jnp.clip(block, 0, blocks - 1)] == me)
            table[6 + 2 * k, s] = jnp.where(valid, 1, 0)
            table[7 + 2 * k, s] = jnp.where(valid, jnp.clip(block - first, 0, owned - 1), 0)

    loads[4].wait()
    loads[5].wait()
    loads[6].wait()

    bias_one = 1.0 - BETA_ONE**STEP
    bias_two = 1.0 - BETA_TWO**STEP
    gain = bias_two**0.5 / bias_one

    def prepare(j):
        whole = left[j]
        l_two = split(whole.T)
        half_l = split(left[j, rows])
        r_two = split(right[j])
        for at in range(2):
            lt_two[j, at * whole.shape[0] : (at + 1) * whole.shape[0]] = l_two[at]
            lh_two[j, at * half : (at + 1) * half] = half_l[at]
        r_high[j], r_low[j] = r_two
        rt_high[j], rt_low[j] = split(right[j].T)
        turned = dot_three(split(dot_three(l_two, split(moment[j]), NN)), r_two, NN)
        base[j] = (BETA_ONE * gain) * turned

    @pl.loop(0, owned // 2)
    def _(j):
        prepare(j)

    for side in sides:

        @pl.when(~side["late"])
        def _():
            send_on(0, side)
            pl.when(z_edge)(functools.partial(send_own, 1, side, 0))
            send_own(1, side, 1)

    @pl.loop(owned // 2, owned)
    def _(j):
        prepare(j)

    for side in sides:

        @pl.when(side["late"])
        def _():
            send_on(0, side)

    def send_on_late_wave(late, places, where):
        for side in sides:

            @pl.when((side["late"] == late) & where)
            def _():
                send_on(1, side, places)

    send_on_late_wave(False, (0,), me >= 0)
    send_on_late_wave(False, (1,), z_edge)
    send_on_late_wave(True, (0, 1), after_edge)

    def pass_far(w):
        for t in range(WAVE):
            for side in sides:
                pl.when(side["gives"])(relay(w, side, t).wait_recv)
                hand(w, side["far"], t).start()

    def stacked(two, b_high, b_low):
        size = two.shape[0] // 2
        full = dot(two, b_high, NN)
        return full[:size] + (full[size:] + dot(two[:size], b_low, NN))

    def stack(two, at, value):
        size = value.shape[0]
        two[at, :size], two[at, size:] = split(value)

    def solve(indices, source, second_to, update_to, scales_to, between):
        size = source.shape[2]
        for at, j in enumerate(indices):
            both = dot(lt_two[j], source[table[2, j], table[3, j]], NN)
            stack(h_two, at, both[:size] + both[size:])
        for at, j in enumerate(indices):
            turned = stacked(h_two[at], r_high[j], r_low[j])
            second_next = BETA_TWO * second[j] + ((1.0 - BETA_TWO) * turned) * turned
            second_to[at] = second_next
            scaled = (base[j] + ((1.0 - BETA_ONE) * gain) * turned) / (second_next * lax.rsqrt(second_next) + EPSILON * bias_two**0.5)
            s_high[at], s_low[at] = split(scaled)
        between()
        for at, j in enumerate(indices):
            stack(z_two, at, stacked(lh_two[j], s_high[at], s_low[at]))
        for at, j in enumerate(indices):
            new = stacked(z_two[at], rt_high[j], rt_low[j])
            largest = jnp.maximum(jnp.max(jnp.abs(new), axis=0, keepdims=True), 1e-30)
            update_to[at] = jnp.round(new * (TOP / largest)).astype(jnp.int32).astype(I16)
            scales_to[at] = largest * (1.0 / TOP)

    loads[7].wait()
    pass_far(0)
    send_on_late_wave(False, (1,), ~z_edge)
    send_on_late_wave(True, (0,), ~after_edge)
    hand(0).wait_recv()
    solve(range(owned), gathered_a, second_out, update_a, scales_a, lambda: send_on_late_wave(True, (1,), ~after_edge))

    def chosen(k, s, absent):
        at = table[7 + 2 * k, s]
        value = update_a[at] if s < WAVE else update_b[table[4, at]]
        return jnp.where(table[6 + 2 * k, s] == 1, value, absent)

    def chosen_scale(k, s, absent):
        at = table[7 + 2 * k, s]
        value = scales_a[at] if s < WAVE else scales_b[table[4, at]]
        return jnp.where(table[6 + 2 * k, s] == 1, value, absent)

    def far(w, side, t):
        at = side["at"]
        part = (at, w, t) if t is not None else (at,)
        return push(codes.at[part], far_in.at[part], far_send.at[at], far_recv.at[at, WAVE * (w or 0) + (t or 0)], side["peer"])

    def far_scale(side):
        at = side["at"]
        return push(scales.at[at], far_scales.at[at], scale_send.at[at], scale_recv.at[at], side["peer"])

    def near(w, side, t):
        at = side["at"]
        part = (at, WAVE * w + t) if t is not None else (at,)
        held = (at, WAVE * w + t, rows) if t is not None else (at, slice(None), rows)
        return push(merged.at[part], out.at[held], near_send.at[at], near_recv.at[at, WAVE * (w or 0) + (t or 0)], side["peer"])

    def near_scale(side):
        at = side["at"]
        return push(merged_scales.at[at], out_scales.at[at, core], scale_send.at[2 + at], scale_recv.at[2 + at], side["peer"])

    def give(k=None, s=None):
        part = out.at[:, :, rows] if k is None else out.at[k, s, rows]
        return push(part, part, give_sem.at[0], give_sem.at[1], twin)

    def give_scale():
        part = out_scales.at[:, core]
        return push(part, part, scale_send.at[4], scale_recv.at[4], twin)

    def send_far(w):
        for t in range(WAVE):
            for side in sides:
                codes[side["at"], w, t] = chosen(side["to_far"], WAVE * w + t, jnp.zeros((), I16))
                pl.when(side["sends"])(far(w, side, t).start)
                scales[side["at"], w, pl.ds(t, 1)] = chosen_scale(side["to_far"], WAVE * w + t, 0.0)
        if w == 1:
            for side in sides:
                pl.when(side["sends"])(far_scale(side).start)
        for t in range(WAVE):
            s = WAVE * w + t
            out[2, s, rows] = chosen(2, s, jnp.zeros((), I16))
            give(2, s).start()
            out_scales[2, core, w, pl.ds(t, 1)] = chosen_scale(2, s, 0.0)

    def send_near(w, side):
        for t in range(WAVE):
            pl.when(side["has"])(far(w, side, t).wait_recv)
            merged[side["at"], WAVE * w + t] = chosen(side["to_near"], WAVE * w + t, far_in[side["at"], w, t])
            pl.when(side["sends"])(near(w, side, t).start)
        if w == 1:
            pl.when(side["has"])(far_scale(side).wait_recv)
            for s in range(slots):
                place = (side["at"], s // WAVE, pl.ds(s % WAVE, 1))
                merged_scales[place] = chosen_scale(side["to_near"], s, far_scales[place])
            pl.when(side["sends"])(near_scale(side).start)

    send_far(0)
    pass_far(1)
    hand(1).wait_recv()

    solve([table[5, b] for b in range(LATE)], gathered_b, second_late, update_b, scales_b, lambda: None)

    send_far(1)
    def each(order):
        for w, side in order:
            send_near(w, side)

    pl.when(left_edge)(lambda: each(((0, to_left), (0, to_right), (1, to_left), (1, to_right))))
    pl.when(right_edge)(lambda: each(((0, to_right), (0, to_left), (1, to_right), (1, to_left))))
    pl.when(~(left_edge | right_edge))(lambda: each(((0, to_right), (0, to_left), (1, to_right), (1, to_left))))

    @pl.loop(0, owned)
    def _(j):
        early, late = table[0, j] == 1, table[1, j] == 1
        gradient = jnp.where(late, gathered_b[table[2, j], table[3, j]].astype(F32), gathered_a[table[2, j], table[3, j]].astype(F32))
        first_out[j] = jnp.where(early | late, BETA_ONE * moment[j] + (1.0 - BETA_ONE) * gradient, 0.0)
        second_out[j] = jnp.where(late, second_late[table[4, j]], jnp.where(early, second_out[j], 0.0))

    def give_near(order):
        for s, side in order:
            pl.when(side["has"])(near(s // WAVE, side, s % WAVE).wait_recv)
            give(side["at"], s).start()

    pl.when(left_edge)(lambda: give_near([(s, side) for side in (to_left, to_right) for s in range(slots)]))
    pl.when(~left_edge)(lambda: give_near([(s, side) for s in range(slots) for side in sides]))
    for side in sides:
        pl.when(side["has"])(near_scale(side).wait_recv)
    give_scale().start()

    for s in range(slots):
        swap(s).wait_send()
    for w in range(2):
        hand(w).wait_send()
    for side in sides:

        @pl.when(side["sends"])
        def _():
            for w in range(2):
                own(w, side, None).wait_send()
            far(None, side, None).wait_send()
            far_scale(side).wait_send()
            near(None, side, None).wait_send()
            near_scale(side).wait_send()

        @pl.when(side["has"] & side["sends"])
        def _():
            for w in range(2):
                relay(w, side, None).wait_send()

    give().wait_send()
    give_scale().wait_send()
    give().wait_recv()
    give_scale().wait_recv()


def finish_kernel(codes, scales, first, second, direction, first_new, second_new, decoded, sem):
    slots = codes.shape[1]
    half = codes.shape[2] // 2
    copies = [pltpu.make_async_copy(first, first_new, sem.at[0]), pltpu.make_async_copy(second, second_new, sem.at[1])]
    for j in range(first.shape[0]):
        pltpu.make_async_copy(first.at[j], first_new.at[j], sem.at[0]).start()
        pltpu.make_async_copy(second.at[j], second_new.at[j], sem.at[1]).start()
    for s in range(slots):
        for core in range(2):
            rows = pl.ds(core * half, half)
            total = 0.0
            for k in range(3):
                total += codes[k, s, rows].astype(jnp.int32).astype(F32) * scales[k, core, s // WAVE, pl.ds(s % WAVE, 1)]
            decoded[s, rows] = total
        copy = pltpu.make_async_copy(decoded.at[s], direction.at[s], sem.at[2 + s])
        copy.start()
        copies.append(copy)
    for copy in copies:
        copy.wait()


def body(gradients, first_moment, second_moment, left_basis, right_basis, shard_starts, block_owners):
    devices = lax.axis_size("fsdp")
    slots = gradients.shape[1]
    owned, width = first_moment.shape[0], first_moment.shape[1]
    half = width // 2
    any_space = pl.BlockSpec(memory_space=pl.ANY)
    in_vmem = pl.BlockSpec(memory_space=pltpu.VMEM)
    dma = pltpu.SemaphoreType.DMA
    keep = functools.partial(pltpu.with_memory_space_constraint, memory_space=pltpu.VMEM)
    stay = functools.partial(pltpu.with_memory_space_constraint, memory_space=pltpu.HBM)
    matrices = (owned, width, width)
    halves = (owned, half, width)
    first_new, second_new, out, out_scales = pl.pallas_call(
        functools.partial(soap_kernel, devices),
        out_shape=[
            pltpu.VMEM(matrices, F32),
            pltpu.VMEM(matrices, F32),
            pltpu.VMEM((3, slots, width, width), I16),
            pltpu.VMEM((3, 2, 2, WAVE, width), F32),
        ],
        in_specs=[any_space] * 7,
        out_specs=[in_vmem] * 4,
        scratch_shapes=[
            pltpu.SMEM(shard_starts.shape, jnp.int32),
            pltpu.SMEM(block_owners.shape, jnp.int32),
            pltpu.SMEM((16, 8), jnp.int32),
            *[pltpu.VMEM((slots, half, width), BF16)] * 3,
            *[pltpu.VMEM((5, WAVE, width, width), BF16)] * 2,
            *[pltpu.VMEM(matrices, F32)] * 4,
            pltpu.VMEM((owned, 2 * width, width), BF16),
            pltpu.VMEM((owned, width, width), BF16),
            *[pltpu.VMEM(matrices, BF16)] * 4,
            pltpu.VMEM(matrices, F32),
            pltpu.VMEM(halves, I16),
            pltpu.VMEM((LATE, half, width), I16),
            pltpu.VMEM((owned, 1, width), F32),
            pltpu.VMEM((LATE, 1, width), F32),
            pltpu.VMEM((LATE, width, width), F32),
            *[pltpu.VMEM((2, 2, WAVE, half, width), I16), pltpu.VMEM((2, 2, WAVE, width), F32)] * 2,
            pltpu.VMEM((2, slots, half, width), I16),
            pltpu.VMEM((2, 2, WAVE, width), F32),
            pltpu.VMEM((owned, 2 * width, width), BF16),
            *[pltpu.VMEM(matrices, BF16)] * 2,
            pltpu.VMEM((owned, width, width), BF16),
            dma((8,)), dma((2, slots)), *[dma((2, 2))] * 2, dma((4, slots)), *[dma((2,))] * 2,
            *[dma((2,)), dma((2, slots))] * 2, dma((2,)), *[dma((5,))] * 2,
        ],
        compiler_params=pltpu.CompilerParams(collective_id=0, has_side_effects=True, vmem_limit_bytes=ROOM),
        name="soap",
    )(*map(stay, (shard_starts, block_owners, gradients, first_moment, second_moment, left_basis, right_basis)))

    return tuple(
        pl.pallas_call(
            finish_kernel,
            out_shape=[
                jax.ShapeDtypeStruct((slots, width, width), F32),
                jax.ShapeDtypeStruct(matrices, F32),
                jax.ShapeDtypeStruct(matrices, F32),
            ],
            in_specs=[in_vmem] * 4,
            out_specs=[any_space] * 3,
            scratch_shapes=[pltpu.VMEM((slots, width, width), F32), dma((2 + slots,))],
            compiler_params=pltpu.CompilerParams(vmem_limit_bytes=8 * 2**20),
            name="finish",
        )(*map(keep, (out, out_scales, first_new, second_new)))
    )


def solution(mesh):
    in_specs = (
        P("dp", "fsdp", None, None),
        P("fsdp", None, None),
        P("fsdp", None, None),
        P("fsdp", None, None),
        P("fsdp", None, None),
        P(),
        P(),
    )
    out_specs = (P("fsdp", None, None), P("fsdp", None, None), P("fsdp", None, None))
    return jax.shard_map(body, mesh=mesh, in_specs=in_specs, out_specs=out_specs, check_vma=False)
```
